32 devices in a mesh: tensor: 4 (over x, core), dp: 4 (over z), ctx: 2 (over y).
Axes of the slice: x: 2, y: 2, z: 4, core: 2. Of those that a mesh axis runs over, the one named last changes fastest.
Arguments:
- inputs: bfloat16 [4, 1024, 2048], P('dp', 'ctx'), may hold values from -8 to 8
- cotangent: bfloat16 [4, 1024, 2048], P('dp', 'ctx'), may hold values from -6 to 6
- qkv_state: float32 [3, 2, 2048, 3, 2048], P(None, None, ('dp', 'ctx'), None, 'tensor'), may hold values from -1024 to 1024, as said below
- out_state: float32 [3, 2, 2048, 2048], P(None, None, 'tensor', ('dp', 'ctx')), may hold values from -1024 to 1024, as said below
- up_state: float32 [3, 2, 2048, 8192], P(None, None, ('dp', 'ctx'), 'tensor'), may hold values from -1024 to 1024, as said below
- down_state: float32 [3, 2, 8192, 2048], P(None, None, 'tensor', ('dp', 'ctx')), may hold values from -1024 to 1024, as said below
- qkv_bias_state: float32 [3, 2, 3, 2048], P(None, None, None, ('tensor', 'dp', 'ctx')), may hold values from -1024 to 1024, as said below
- up_bias_state: float32 [3, 2, 8192], P(None, None, ('tensor', 'dp', 'ctx')), may hold values from -1024 to 1024, as said below
- norm_state: float32 [3, 2, 5, 2048], P(None, None, None, ('dp', 'ctx')), may hold values from -1024 to 1024, as said below
Outputs:
- outputs: bfloat16 [4, 1024, 2048], P('dp', 'ctx')
- input_grad: float32 [4, 1024, 2048], P('dp', 'ctx')
- qkv_grad: float32 [3, 2, 2048, 3, 2048], P(None, None, ('dp', 'ctx'), None, 'tensor')
- qkv_new: float32 [2, 2048, 3, 2048], P(None, ('dp', 'ctx'), None, 'tensor')
- out_grad: float32 [3, 2, 2048, 2048], P(None, None, 'tensor', ('dp', 'ctx'))
- out_new: float32 [2, 2048, 2048], P(None, 'tensor', ('dp', 'ctx'))
- up_grad: float32 [3, 2, 2048, 8192], P(None, None, ('dp', 'ctx'), 'tensor')
- up_new: float32 [2, 2048, 8192], P(None, ('dp', 'ctx'), 'tensor')
- down_grad: float32 [3, 2, 8192, 2048], P(None, None, 'tensor', ('dp', 'ctx'))
- down_new: float32 [2, 8192, 2048], P(None, 'tensor', ('dp', 'ctx'))
- qkv_bias_grad: float32 [3, 2, 3, 2048], P(None, None, None, ('tensor', 'dp', 'ctx'))
- qkv_bias_new: float32 [2, 3, 2048], P(None, None, ('tensor', 'dp', 'ctx'))
- up_bias_grad: float32 [3, 2, 8192], P(None, None, ('tensor', 'dp', 'ctx'))
- up_bias_new: float32 [2, 8192], P(None, ('tensor', 'dp', 'ctx'))
- norm_grad: float32 [3, 2, 5, 2048], P(None, None, None, ('dp', 'ctx'))
- norm_new: float32 [2, 5, 2048], P(None, None, ('dp', 'ctx'))
The draws below stay inside these ranges and needn't reach their ends.
Inputs may be any that keep to these rules, and one draw needn't show every extreme that they name: `qkv_state`: index 0 of the first dimension holds the weights, 1 the first moments, 2 the roots of the second moments, which are positive. `out_state`: index 0 of the first dimension holds the weights, 1 the first moments, 2 the roots of the second moments, which are positive. `up_state`: index 0 of the first dimension holds the weights, 1 the first moments, 2 the roots of the second moments, which are positive. `down_state`: index 0 of the first dimension holds the weights, 1 the first moments, 2 the roots of the second moments, which are positive. `qkv_bias_state`: index 0 of the first dimension holds the biases, 1 the first moments, 2 the roots of the second moments, which are positive. `up_bias_state`: index 0 of the first dimension holds the biases, 1 the first moments, 2 the roots of the second moments, which are positive. `norm_state`: index 0 of the first dimension holds the gains, shifts and output bias, 1 the first moments, 2 the roots of the second moments, which are positive.
All inputs are finite; a program needn't handle non-finite values.
Results may differ from the reference program's by a relative error of at most 0.015.
Values may be sent and summed in bfloat16 or wider, within the bound.
A program may use at most 384 MiB of HBM per device.

```python
import math
import jax
import jax.numpy as jnp
from jax import lax

D = 2048
HEADS = 8
HEAD_DIM = 256
ROT = 64
FF = 8192
LAYERS = 2
LEN = 1024
STEP = 4
BATCH = 4
TOKENS = 4096


def with_moments(key, weight, per_token):
    full_shape = weight.shape
    grad_scale = per_token * math.sqrt(TOKENS)
    first_moment = 0.4 * grad_scale * jnp.clip(jax.random.normal(jax.random.fold_in(key, 21), full_shape, jnp.float32), -5.0, 5.0)
    root_moment = grad_scale * jnp.exp(jax.random.uniform(jax.random.fold_in(key, 22), full_shape, jnp.float32, minval=math.log(0.25), maxval=0.0))
    limit = float(TOKENS // 4)
    return jnp.clip(jnp.stack([weight, first_moment, root_moment]), -limit, limit)


def draw_inputs(key, part):
    full_shape = (BATCH, LEN, D)
    noise_draw = jax.random.normal(jax.random.fold_in(key, 1), full_shape, jnp.float32)
    values = noise_draw
    return jnp.clip(values, -8.0, 8.0).astype(jnp.bfloat16)


def draw_qkv_state(key, part):
    full_shape = (LAYERS, D, 3, HEADS, HEAD_DIM)
    base_draw = jax.random.normal(jax.random.fold_in(key, 1), full_shape, jnp.float32) * D ** (-0.5)
    return with_moments(key, base_draw.reshape(LAYERS, D, 3, D), 2.0)


def draw_out_state(key, part):
    weight = jax.random.normal(jax.random.fold_in(key, 1), (LAYERS, D, D), jnp.float32) * (4.0 * D ** (-0.5))
    return with_moments(key, weight, 0.4)


def draw_up_state(key, part):
    weight = jax.random.normal(jax.random.fold_in(key, 1), (LAYERS, D, FF), jnp.float32) * D ** (-0.5)
    return with_moments(key, weight, 0.3)


def draw_down_state(key, part):
    weight = jax.random.normal(jax.random.fold_in(key, 1), (LAYERS, FF, D), jnp.float32) * FF ** (-0.5)
    return with_moments(key, weight, 0.7)


def draw_qkv_bias_state(key, part):
    weight = 0.3 * jax.random.normal(jax.random.fold_in(key, 1), (LAYERS, 3, D), jnp.float32)
    return with_moments(key, weight, 3.0)


def draw_up_bias_state(key, part):
    weight = 0.3 * jax.random.normal(jax.random.fold_in(key, 1), (LAYERS, FF), jnp.float32)
    return with_moments(key, weight, 0.4)


def draw_norm_state(key, part):
    gain_rows = 1.0 + 0.1 * jax.random.uniform(jax.random.fold_in(key, 1), (LAYERS, 2, D), jnp.float32, minval=-3.0, maxval=3.0)
    shifts = 0.3 * jax.random.normal(jax.random.fold_in(key, 2), (LAYERS, 3, D), jnp.float32)
    weight = jnp.stack([gain_rows[:, 0], shifts[:, 0], gain_rows[:, 1], shifts[:, 1], shifts[:, 2]], axis=1)
    return with_moments(key, weight, 3.0)


def levels(rng, dims, split, smallest, high):
    def one(dim, blocks):
        heights = jax.random.uniform(jax.random.fold_in(jax.random.fold_in(rng, 6), dim), (blocks,), jnp.float32, smallest / len(split), high / len(split))
        return jnp.repeat(jnp.exp(heights), dims[dim] // blocks).reshape((-1,) + (1,) * (len(dims) - dim - 1))

    gain = one(*split[0])
    for cut in split[1:]:
        gain = gain * one(*cut)
    return gain


def scatter_about(rng, extent, deviation, most, cuts=(), kind=jnp.bfloat16):
    values = jax.random.normal(rng, extent, jnp.float32) * deviation
    if len(cuts) > 0:
        values = levels(rng, extent, cuts, -0.22, 0.18) * values
    return jnp.clip(values, min=-most, max=most).astype(kind)


def setup_inputs(seed: int = 0) -> dict:
    splits = jax.random.split(jax.random.key(seed), 10)
    inputs = draw_inputs(jax.random.fold_in(splits[9], 71), 0)
    cotangent = scatter_about(splits[1], (BATCH, LEN, D), 1.0, 6.0, ((0, 4), (1, 2)))
    qkv_state = draw_qkv_state(jax.random.fold_in(splits[9], 71), 0)
    out_state = draw_out_state(jax.random.fold_in(splits[9], 71), 0)
    up_state = draw_up_state(jax.random.fold_in(splits[9], 71), 0)
    down_state = draw_down_state(jax.random.fold_in(splits[9], 71), 0)
    qkv_bias_state = draw_qkv_bias_state(jax.random.fold_in(splits[9], 71), 0)
    up_bias_state = draw_up_bias_state(jax.random.fold_in(splits[9], 71), 0)
    norm_state = draw_norm_state(jax.random.fold_in(splits[9], 71), 0)
    return {"inputs": inputs, "cotangent": cotangent, "qkv_state": qkv_state, "out_state": out_state, "up_state": up_state, "down_state": down_state, "qkv_bias_state": qkv_bias_state, "up_bias_state": up_bias_state, "norm_state": norm_state}


@jax.custom_vjp
def low(v):
    return lax.optimization_barrier(v.astype(jnp.bfloat16)).astype(jnp.float32)

@jax.custom_vjp
def low_back(v):
    return v

def low_keep(v):
    return (low(v), None)

def low_pass(kept, grad):
    return (grad,)

def back_keep(v):
    return (v, None)

def back_low(kept, grad):
    return (low(grad),)
low.defvjp(low_keep, low_pass)
low_back.defvjp(back_keep, back_low)
highest = lax.Precision.HIGHEST
beta_one = 0.9
beta_two = 0.95
adam_eps = 1e-08
norm_eps = 1e-05
rate_matrix = 0.008
rate_vector = 0.2
weight_decay = 0.01

def layer_norm(values, norm_gain, norm_shift):
    centered = values - lax.optimization_barrier(jnp.mean(values, axis=-1, keepdims=True))
    spread = lax.optimization_barrier(jnp.mean(centered * centered, axis=-1, keepdims=True))
    return centered * lax.rsqrt(spread + norm_eps) * norm_gain + norm_shift

def angle_tables(positions, rotated):
    halfway = rotated // 2
    frequency = 10000.0 ** (-2.0 * jnp.arange(halfway, dtype=jnp.float32) / rotated)
    angles = positions[:, None] * frequency[None, :]
    return (jnp.cos(angles)[:, None, :], jnp.sin(angles)[:, None, :])

def rotate(features_in, cosine_table, sine_table):
    halfway = cosine_table.shape[-1]
    lower_half = features_in[..., :halfway]
    upper_half = features_in[..., halfway:2 * halfway]
    return jnp.concatenate([lower_half * cosine_table - upper_half * sine_table, upper_half * cosine_table + lower_half * sine_table, features_in[..., 2 * halfway:]], axis=-1)

def attend_sequence(triple):
    queries, key_block, value_block = triple
    length = queries.shape[0]
    raw_scores = jnp.einsum('qhd,khd->hqk', queries, key_block, precision=highest) * HEAD_DIM ** (-0.5)
    scores = low_back(raw_scores)
    causal = jnp.arange(length)[None, :] <= jnp.arange(length)[:, None]
    scores = jnp.where(causal[None], scores, -1e+30)
    attention = jax.nn.softmax(scores, axis=-1)
    return jnp.einsum('hqk,khd->qhd', low(attention), value_block, precision=highest)

def forward(hidden, qkv_weight, out_weight, up_weight, down_weight, qkv_bias, up_bias, vectors):
    batch_size, length, features = hidden.shape
    positions = jnp.arange(length, dtype=jnp.float32)
    cosine_table, sine_table = angle_tables(positions, ROT)
    for layer_index in range(LAYERS):
        norm_rows = low(vectors[layer_index])
        normed_one = low(layer_norm(hidden, norm_rows[0], norm_rows[1]))
        normed_two = low(layer_norm(hidden, norm_rows[2], norm_rows[3]))
        bias_full = low(qkv_bias[layer_index])
        projected = jnp.einsum('bld,dkj->blkj', normed_one, low(qkv_weight[layer_index]), precision=highest)
        projected = low_back(projected + bias_full)
        projected = projected.reshape(batch_size, length, 3, HEADS, HEAD_DIM)
        queries = low(rotate(projected[:, :, 0], cosine_table, sine_table))
        key_block = low(rotate(projected[:, :, 1], cosine_table, sine_table))
        value_block = low(projected[:, :, 2])
        mixture = lax.map(jax.checkpoint(attend_sequence), (queries, key_block, value_block))
        mixture = low(low_back(mixture.reshape(batch_size, length, features)))
        pre_act = jnp.einsum('bld,df->blf', normed_two, low(up_weight[layer_index]), precision=highest)
        pre_act = low_back(pre_act + low(up_bias[layer_index]))
        activation = low(jax.nn.gelu(pre_act, approximate=False))
        branch = jnp.einsum('blj,jd->bld', mixture, low(out_weight[layer_index]), precision=highest)
        branch = branch + jnp.einsum('blf,fd->bld', activation, low(down_weight[layer_index]), precision=highest)
        hidden = hidden + low_back(branch) + norm_rows[4]
    return hidden

def adam_step(packed, gradient, learn_rate, decay_rate):
    moment = beta_one * packed[1] + (1.0 - beta_one) * gradient
    root_second = jnp.sqrt(beta_two * packed[2] * packed[2] + (1.0 - beta_two) * gradient * gradient)
    update = learn_rate * (moment / (1.0 - beta_one ** STEP)) / (root_second / (1.0 - beta_two ** STEP) ** 0.5 + adam_eps)
    weight = packed[0] - update - learn_rate * decay_rate * packed[0]
    return (jnp.stack([gradient, moment, root_second]), weight)

def reference(inputs, cotangent, qkv_state, out_state, up_state, down_state, qkv_bias_state, up_bias_state, norm_state):
    final, pullback = jax.vjp(forward, inputs.astype(jnp.float32), qkv_state[0], out_state[0], up_state[0], down_state[0], qkv_bias_state[0], up_bias_state[0], norm_state[0])
    gradients = pullback(cotangent.astype(jnp.float32))
    qkv_pack, qkv_new = adam_step(qkv_state, gradients[1], rate_matrix, weight_decay)
    out_pack, out_new = adam_step(out_state, gradients[2], rate_matrix, weight_decay)
    up_pack, up_new = adam_step(up_state, gradients[3], rate_matrix, weight_decay)
    down_pack, down_new = adam_step(down_state, gradients[4], rate_matrix, weight_decay)
    qkv_bias_pack, qkv_bias_new = adam_step(qkv_bias_state, gradients[5], rate_vector, 0.0)
    up_bias_pack, up_bias_new = adam_step(up_bias_state, gradients[6], rate_vector, 0.0)
    norm_pack, norm_new = adam_step(norm_state, gradients[7], rate_vector, 0.0)
    return (final.astype(jnp.bfloat16), gradients[0], qkv_pack, qkv_new, out_pack, out_new, up_pack, up_new, down_pack, down_new, qkv_bias_pack, qkv_bias_new, up_bias_pack, up_bias_new, norm_pack, norm_new)
```

```python
import jax
import jax.numpy as jnp
from jax import lax
from jax.experimental import pallas as pl
from jax.experimental.pallas import tpu as pltpu
from jax.sharding import PartitionSpec as P

HEAD_DIM = 256
ROT = 64
STEP = 4

beta_one = 0.9
beta_two = 0.95
adam_eps = 1e-08
norm_eps = 1e-05
rate_matrix = 0.008
rate_vector = 0.2
weight_decay = 0.01

BF = jnp.bfloat16
F32 = jnp.float32
AXES = ("tensor", "dp", "ctx")
PAD = 16


def angle_tables(positions, rotated):
    halfway = rotated // 2
    frequency = 10000.0 ** (-2.0 * jnp.arange(halfway, dtype=F32) / rotated)
    angles = positions[:, None] * frequency[None, :]
    return jnp.cos(angles), jnp.sin(angles)


def rotate(x, cosine, sine):
    half = cosine.shape[-1]
    a, b = x[:, :half], x[:, half : 2 * half]
    return jnp.concatenate([a * cosine - b * sine, b * cosine + a * sine, x[:, 2 * half :]], axis=-1)


def rotate_back(x, cosine, sine):
    half = cosine.shape[-1]
    a, b = x[:, :half], x[:, half : 2 * half]
    return jnp.concatenate([a * cosine + b * sine, b * cosine - a * sine, x[:, 2 * half :]], axis=-1)


def adam_step(packed, gradient, learn_rate, decay_rate):
    moment = beta_one * packed[1] + (1.0 - beta_one) * gradient
    root_second = jnp.sqrt(
        beta_two * packed[2] * packed[2] + (1.0 - beta_two) * gradient * gradient
    )
    update = (
        learn_rate
        * (moment / (1.0 - beta_one**STEP))
        / (root_second / (1.0 - beta_two**STEP) ** 0.5 + adam_eps)
    )
    weight = packed[0] - update - learn_rate * decay_rate * packed[0]
    return (jnp.stack([gradient, moment, root_second]), weight)


def normalized(values):
    centered = values - jnp.mean(values, axis=-1, keepdims=True)
    spread = jnp.mean(centered * centered, axis=-1, keepdims=True)
    inverse = lax.rsqrt(spread + norm_eps)
    return centered * inverse, inverse


def dot(a, b, dims):
    return lax.dot_general(a, b, (dims, ((), ())), preferred_element_type=F32)


NN = ((1,), (0,))
NT = ((1,), (1,))
TN = ((0,), (0,))


def causal_block(start, width):
    rows = start + lax.broadcasted_iota(jnp.int32, (width, start + width), 0)
    return lax.broadcasted_iota(jnp.int32, (width, start + width), 1) <= rows


def attend_kernel(tile, q_ref, k_ref, v_ref, o_ref, l_ref):
    length = q_ref.shape[0]
    for start in range(0, length, tile):
        rows, seen = pl.ds(start, tile), pl.ds(0, start + tile)
        scores = dot(q_ref[rows, :], k_ref[seen, :], NT)
        scores = jnp.where(causal_block(start, tile), scores, -1e30)
        peak = jnp.max(scores, axis=-1, keepdims=True)
        weights = jnp.exp(scores - peak)
        total = jnp.sum(weights, axis=-1, keepdims=True)
        weights = (weights * (1.0 / total)).astype(BF)
        o_ref[rows, :] = dot(weights, v_ref[seen, :], NN).astype(BF)
        l_ref[rows, :] = jnp.broadcast_to(peak + jnp.log(total), (tile, 128))


def attend_back_kernel(tile, q_ref, k_ref, v_ref, g_ref, l_ref, dq_ref, dk_ref, dv_ref):
    length = q_ref.shape[0]
    scale = HEAD_DIM ** (-0.5)
    dk_ref[...] = jnp.zeros_like(dk_ref)
    dv_ref[...] = jnp.zeros_like(dv_ref)
    for start in range(0, length, tile):
        rows, seen = pl.ds(start, tile), pl.ds(0, start + tile)
        q, g = q_ref[rows, :], g_ref[rows, :]
        scores = dot(q, k_ref[seen, :], NT)
        weights = jnp.where(
            causal_block(start, tile), jnp.exp(scores - l_ref[rows, 0:1]), 0.0
        )
        slope = dot(g, v_ref[seen, :], NT)
        delta = jnp.sum(weights * slope, axis=-1, keepdims=True)
        ds = (weights * (slope - delta)).astype(BF)
        dq_ref[rows, :] = dot(ds, k_ref[seen, :], NN) * scale
        dk_ref[seen, :] += dot(ds, q, TN)
        dv_ref[seen, :] += dot(weights.astype(BF), g, TN)


def vmem_call(kernel, outs, flops, name):
    return pl.pallas_call(
        kernel,
        out_shape=outs,
        compiler_params=pltpu.CompilerParams(vmem_limit_bytes=48 << 20),
        cost_estimate=pl.CostEstimate(flops=flops, bytes_accessed=4 << 20, transcendentals=1 << 20),
        name=name,
    )


def attend(q, k, v):
    length, width = q.shape
    tile = min(256, length)
    outs = [
        jax.ShapeDtypeStruct((length, width), BF),
        jax.ShapeDtypeStruct((length, 128), F32),
    ]
    kernel = lambda *refs: attend_kernel(tile, *refs)
    return vmem_call(kernel, outs, 3 * length * length * width, "attend")(q, k, v)


def attend_back(q, k, v, g, log_total):
    length, width = q.shape
    tile = min(256, length)
    outs = [jax.ShapeDtypeStruct((length, width), F32)] * 3
    kernel = lambda *refs: attend_back_kernel(tile, *refs)
    return vmem_call(kernel, outs, 7 * length * length * width, "attend_back")(q, k, v, g, log_total)


def split_hi_lo(vector):
    high = vector.astype(BF)
    low = (vector - high.astype(F32)).astype(BF)
    return high, low


def build(mesh):
    tensor, Z, C = (mesh.shape[name] for name in AXES)
    assert tensor == 4 and Z == 4

    def flat(th, tl, z, y):
        return ((th * 2 + tl) * Z + z) * C + y

    def permute(x, move):
        pairs = []
        for th in range(2):
            for tl in range(2):
                for z in range(Z):
                    for y in range(C):
                        target = move(th, tl, z, y)
                        if target is not None:
                            pairs.append((flat(th, tl, z, y), flat(*target)))
        return lax.ppermute(x, AXES, pairs)

    def over_x(x):
        return permute(x, lambda th, tl, z, y: (1 - th, tl, z, y))

    def over_core(x):
        return permute(x, lambda th, tl, z, y: (th, 1 - tl, z, y))

    def over_z(x, k):
        return permute(x, lambda th, tl, z, y: (th, tl, z ^ k, y))

    def over_y(x, j):
        return permute(x, lambda th, tl, z, y: (th, tl, z, y ^ j))

    def fetch_move(turn):
        def move(th, tl, z, y):
            part = (z + turn) % 2
            goal = 2 * tl + part
            core = {0: 0, 2: 1, 3: 0, 1: 1}[goal ^ z]
            return (th, core, goal, y)

        return move

    def give_move(turn):
        def move(th, tl, z, y):
            k = 2 * tl if turn == 0 else 3 - 2 * tl
            return (th, z // 2, z ^ k, y)

        return move

    def local(
        inputs,
        cotangent,
        qkv_state,
        out_state,
        up_state,
        down_state,
        qkv_bias_state,
        up_bias_state,
        norm_state,
    ):
        layers = qkv_state.shape[1]
        S, part_rows, D = inputs.shape
        L = part_rows * C
        rows_b = L // 8
        DB = D // (Z * C)
        F4 = up_state.shape[3]
        F8 = F4 // 2
        HW = qkv_state.shape[4] // 2
        W1C = 3 * HW + F8
        W2R = HW + F8
        t = lax.axis_index("tensor")
        th, tl = t // 2, t % 2
        z = lax.axis_index("dp")
        y = lax.axis_index("ctx")
        odd = (z % 2) == 1
        mine_z = (z ^ (2 * tl), z ^ (3 - 2 * tl))
        other_z = (z ^ (2 - 2 * tl), z ^ (1 + 2 * tl))

        def block_of(dx, k):
            return (th ^ dx) * 4 + (z ^ k)

        def pack(l):
            rows = norm_state[0, l].astype(BF).astype(F32)
            wq = qkv_state[0, l].astype(BF).astype(F32)
            wu = up_state[0, l].astype(BF).astype(F32)
            wo = out_state[0, l].astype(BF)
            wd = down_state[0, l].astype(BF)
            vq = jnp.einsum("d,djk->jk", rows[1], wq, precision=lax.Precision.HIGHEST)
            vu = jnp.einsum("d,dk->k", rows[3], wu, precision=lax.Precision.HIGHEST)
            bq = qkv_bias_state[0, l].astype(BF).astype(F32)
            bu = up_bias_state[0, l].astype(BF).astype(F32)
            place = z * C + y
            vq = vq + lax.dynamic_update_slice(jnp.zeros_like(vq), bq, (0, place * bq.shape[1]))
            vu = vu + lax.dynamic_update_slice(jnp.zeros_like(vu), bu, (place * bu.shape[0],))
            gq = (rows[0][:, None, None] * wq).astype(BF)
            gu = (rows[2][:, None] * wu).astype(BF)
            ones, twos = [], []
            for part in range(2):
                small = jnp.concatenate(
                    [
                        vq[:, part * HW : (part + 1) * HW].reshape(-1),
                        vu[part * F8 : (part + 1) * F8],
                    ]
                )
                high, low = split_hi_lo(small)
                extra = jnp.concatenate(
                    [high[None], low[None], jnp.zeros((PAD - 2, W1C), BF)], axis=0
                )
                body = jnp.concatenate(
                    [
                        gq[:, :, part * HW : (part + 1) * HW].reshape(DB, 3 * HW),
                        gu[:, part * F8 : (part + 1) * F8],
                    ],
                    axis=1,
                )
                ones.append(jnp.concatenate([body, extra], axis=0))
                twos.append(
                    jnp.concatenate(
                        [
                            wo[part * HW : (part + 1) * HW],
                            wd[part * F8 : (part + 1) * F8],
                            rows[4].astype(BF)[None],
                            jnp.zeros((PAD - 1, DB), BF),
                        ],
                        axis=0,
                    )
                )
            pick = lambda pair: (
                jnp.where(odd, pair[1], pair[0]),
                jnp.where(odd, pair[0], pair[1]),
            )
            return pick(ones), pick(twos)

        def gather_blocks(pair):
            first = [permute(block, fetch_move(turn)) for turn, block in enumerate(pair)]
            columns = [(y, first)]
            for j in range(1, C):
                columns.append((y ^ j, [over_y(block, j) for block in first]))
            found = []
            for place, blocks in columns:
                for zs, block in zip(mine_z, blocks):
                    found.append((zs, place, block))
            for place, blocks in columns:
                for zs, block in zip(other_z, blocks):
                    found.append((zs, place, over_core(block)))
            return found

        def fetch_one(pair):
            whole = jnp.zeros((D, W1C), BF)
            small = 0.0
            for zs, ys, block in gather_blocks(pair):
                whole = lax.dynamic_update_slice(whole, block[:DB], ((zs * C + ys) * DB, 0))
                small = small + block[DB].astype(F32) + block[DB + 1].astype(F32)
            return whole, small

        def fetch_two(pair):
            whole = jnp.zeros((W2R, D), BF)
            small = jnp.zeros((1, D), BF)
            for zs, ys, block in gather_blocks(pair):
                at = (zs * C + ys) * DB
                whole = lax.dynamic_update_slice(whole, block[:W2R], (0, at))
                small = lax.dynamic_update_slice(small, block[W2R : W2R + 1], (0, at))
            return whole, small.astype(F32)

        def spread_sequence(natural):
            quarter = part_rows // 4
            own = lax.dynamic_slice_in_dim(natural, t * quarter, quarter, axis=1)
            held = jnp.stack([own] + [over_z(own, k) for k in range(1, Z)])
            whole = jnp.zeros((L, D), BF)
            for j in range(C):
                for d in range(2):
                    goal = 2 * (y ^ j) + (tl ^ d)
                    block = held[z ^ (goal // S), goal % S]
                    if j or d:
                        block = permute(
                            block, lambda th, tl, z, y, j=j, d=d: (th, tl ^ d, z, y ^ j)
                        )
                    base = (y ^ j) * part_rows + (tl ^ d) * quarter
                    far = over_x(block)
                    whole = lax.dynamic_update_slice(whole, block, (base + th * 2 * quarter, 0))
                    whole = lax.dynamic_update_slice(
                        whole, far, (base + (1 - th) * 2 * quarter, 0)
                    )
            return whole

        def my_rows(whole):
            return lax.dynamic_slice_in_dim(whole, block_of(0, 0) * rows_b, rows_b, axis=0)

        def gather_tokens(block):
            whole = jnp.zeros((L, D), block.dtype)
            for k in (3, 2, 1, 0):
                near = over_z(block, k) if k else block
                whole = lax.dynamic_update_slice(whole, near, (block_of(0, k) * rows_b, 0))
                whole = lax.dynamic_update_slice(
                    whole, over_x(near), (block_of(1, k) * rows_b, 0)
                )
            return whole

        def scatter_tokens(near, far):
            cut = lambda half, k: lax.dynamic_slice_in_dim(half, (z ^ k) * rows_b, rows_b, axis=0)
            got = {k: over_x(cut(far, k)) for k in (3, 2, 1, 0)}
            total = 0.0
            for k in (3, 2, 1, 0):
                term = cut(near, k).astype(F32) + got[k].astype(F32)
                if k:
                    term = over_z(term.astype(BF), k).astype(F32)
                total = total + term
            return total

        def halves(fn, act):
            half = L // 2
            pick = lambda dx: tuple(
                lax.dynamic_slice_in_dim(a, (th ^ dx) * half, half, axis=0) for a in act
            )
            far = fn(*pick(1)).astype(BF)
            near = fn(*pick(0)).astype(BF)
            return near, far

        def return_natural(block):
            kind = block.dtype
            if C == 2 and S == 1:
                rows = jnp.zeros((4 * rows_b, D), kind)
                rows = lax.dynamic_update_slice(rows, block, (z * rows_b, 0))
                for k in range(1, Z):
                    came = permute(
                        block,
                        lambda th, tl, z, y: (th, tl, z ^ k, y) if (z ^ k) == 2 * y + tl else None,
                    )
                    rows = lax.dynamic_update_slice(rows, came, ((z ^ k) * rows_b, 0))
                moved = permute(
                    rows,
                    lambda th, tl, z, y: (th, tl, z, th) if z == 2 * y + tl and y != th else None,
                )
                rows = jnp.where(z // 2 == y, rows, moved)
                other = permute(
                    rows,
                    lambda th, tl, z, y: (th, 1 - tl, z, y) if y == th and tl == z % 2 else None,
                )
                rows = jnp.where(tl == z % 2, rows, other)
                other = permute(
                    rows, lambda th, tl, z, y: (1 - th, tl, z, y) if y == th else None
                )
                return jnp.where(th == y, rows, other)[None]
            every = lax.all_gather(block, AXES, axis=0)
            every = every.reshape(2, 2, Z, C, rows_b, D)
            every = jnp.transpose(every, (3, 1, 0, 2, 4, 5)).reshape(2 * C, L, D)
            return lax.dynamic_slice(every, (z * S, y * part_rows, 0), (S, part_rows, D))

        def hand_out(cut_z, cut_y):
            sums = []
            for turn in range(2):
                came = over_core(cut_z(other_z[turn]))
                sums.append(cut_z(mine_z[turn]).astype(F32) + came.astype(F32))
            result = []
            for turn in range(2):
                low = sums[turn].astype(BF)
                total = cut_y(sums[turn], y)
                for j in range(1, C):
                    total = total + over_y(cut_y(low, y ^ j), j).astype(F32)
                result.append(permute(total.astype(BF), give_move(turn)))
            r0, r1 = result
            return jnp.where(odd, r1, r0), jnp.where(odd, r0, r1)

        def give_one(m1, small):
            high, low = split_hi_lo(small)
            extra = jnp.concatenate([high[None], low[None], jnp.zeros((PAD - 2, W1C), BF)], axis=0)

            def cut_z(zs):
                rows = lax.dynamic_slice_in_dim(m1, zs * C * DB, C * DB, axis=0)
                return jnp.concatenate([rows, extra], axis=0)

            def cut_y(block, ys):
                rows = lax.dynamic_slice_in_dim(block, ys * DB, DB, axis=0)
                return jnp.concatenate([rows, block[C * DB :]], axis=0)

            return hand_out(cut_z, cut_y)

        def give_two(m2, small):
            high, low = split_hi_lo(small)
            extra = jnp.concatenate([high[None], low[None], jnp.zeros((PAD - 2, D), BF)], axis=0)

            def cut_z(zs):
                piece = lambda a: lax.dynamic_slice_in_dim(a, zs * C * DB, C * DB, axis=1)
                return jnp.concatenate([piece(m2), piece(extra)], axis=0)

            def cut_y(block, ys):
                return lax.dynamic_slice_in_dim(block, ys * DB, DB, axis=1)

            return hand_out(cut_z, cut_y)

        cosine, sine = angle_tables(jnp.arange(L, dtype=F32), ROT)
        whole_in = spread_sequence(inputs)
        packed = [pack(l) for l in range(layers)]
        params = []
        for l in range(layers):
            ones, twos = packed[l]
            w1, small1 = fetch_one(ones)
            w2, bias_out = fetch_two(twos)
            params.append((w1, small1, w2, bias_out))
        whole_cot = spread_sequence(cotangent)

        h = my_rows(whole_in).astype(F32)
        saved = []
        for l in range(layers):
            w1, small1, w2, bias_out = params[l]
            if l == 0:
                xh = normalized(whole_in.astype(F32))[0].astype(BF)
            else:
                xh = gather_tokens(normalized(h)[0].astype(BF))
            proj = dot(xh, w1, NN) + small1[None]
            q = (rotate(proj[:, :HW], cosine, sine) * HEAD_DIM ** (-0.5)).astype(BF)
            k = rotate(proj[:, HW : 2 * HW], cosine, sine).astype(BF)
            v = proj[:, 2 * HW : 3 * HW].astype(BF)
            u = proj[:, 3 * HW :]
            cumulative = 0.5 * lax.erfc(-u * 0.5**0.5)
            a = (u * cumulative).astype(BF)
            slope = (cumulative + u * jnp.exp(-0.5 * u * u) * 0.3989422804014327).astype(BF)
            o, log_total = attend(q, k, v)
            act = jnp.concatenate([o, a], axis=1)
            near, far = halves(lambda r: dot(r, w2, NN), (act,))
            saved.append((h, xh, q, k, v, log_total, act, slope))
            h = h + scatter_tokens(near, far) + bias_out
        outputs = return_natural(h.astype(BF))

        gb = whole_cot
        g = my_rows(whole_cot).astype(F32)
        got = [None] * layers
        for l in reversed(range(layers)):
            h_in, xh, q, k, v, log_total, act, slope = saved[l]
            w1, small1, w2, bias_out = params[l]
            if l < layers - 1:
                gb = gather_tokens(g.astype(BF))
            back = dot(gb, w2, NT)
            go = back[:, :HW].astype(BF)
            du = (back[:, HW:] * slope.astype(F32)).astype(BF)
            dq, dk, dv = attend_back(q, k, v, go, log_total)
            dy = jnp.concatenate(
                [
                    rotate_back(dq, cosine, sine).astype(BF),
                    rotate_back(dk, cosine, sine).astype(BF),
                    dv.astype(BF),
                    du,
                ],
                axis=1,
            )
            near, far = halves(lambda r: dot(r, w1, NT), (dy,))
            e = scatter_tokens(near, far)
            m2 = dot(act, gb, TN).astype(BF)
            dbo = jnp.sum(gb.astype(F32), axis=0)
            m1 = dot(xh, dy, TN).astype(BF)
            db = jnp.sum(dy.astype(F32), axis=0)
            got[l] = (give_one(m1, db), give_two(m2, dbo))
            xn, inverse = normalized(h_in)
            g = g + inverse * (
                e
                - jnp.mean(e, axis=-1, keepdims=True)
                - xn * jnp.mean(e * xn, axis=-1, keepdims=True)
            )
        input_grad = return_natural(g)

        grads = [[] for _ in range(7)]
        for l in range(layers):
            rows = norm_state[0, l].astype(BF).astype(F32)
            wq = qkv_state[0, l].astype(BF).astype(F32)
            wu = up_state[0, l].astype(BF).astype(F32)
            (one_a, one_b), (two_a, two_b) = got[l]
            pair = lambda f: (f(one_a).astype(F32), f(one_b).astype(F32))
            mq = jnp.concatenate(
                [x.reshape(DB, 3, HW) for x in pair(lambda b: b[:DB, : 3 * HW])], axis=2
            )
            mu = jnp.concatenate(pair(lambda b: b[:DB, 3 * HW :]), axis=1)
            small = [
                b[DB].astype(F32) + b[DB + 1].astype(F32) for b in (one_a, one_b)
            ]
            bq = jnp.concatenate([s[: 3 * HW].reshape(3, HW) for s in small], axis=1)
            bu = jnp.concatenate([s[3 * HW :] for s in small], axis=0)
            grads[0].append(rows[0][:, None, None] * mq + rows[1][:, None, None] * bq[None])
            grads[1].append(
                jnp.concatenate([b[:HW].astype(F32) for b in (two_a, two_b)], axis=0)
            )
            grads[2].append(rows[2][:, None] * mu + rows[3][:, None] * bu[None])
            grads[3].append(
                jnp.concatenate([b[HW:W2R].astype(F32) for b in (two_a, two_b)], axis=0)
            )
            place = z * C + y
            nq, nu = qkv_bias_state.shape[3], up_bias_state.shape[2]
            grads[4].append(lax.dynamic_slice_in_dim(bq, place * nq, nq, axis=1))
            grads[5].append(lax.dynamic_slice_in_dim(bu, place * nu, nu, axis=0))
            terms = jnp.stack(
                [
                    jnp.sum(wq * mq, axis=(1, 2)),
                    jnp.sum(wq * bq[None], axis=(1, 2)),
                    jnp.sum(wu * mu, axis=1),
                    jnp.sum(wu * bu[None], axis=1),
                ]
            )
            terms = terms + over_core(terms)
            terms = terms + over_x(terms)
            dbo = two_a[W2R].astype(F32) + two_a[W2R + 1].astype(F32)
            grads[6].append(jnp.concatenate([terms, dbo[None]], axis=0))
        totals = [jnp.stack(parts) for parts in grads]
        qkv_pack, qkv_new = adam_step(qkv_state, totals[0], rate_matrix, weight_decay)
        out_pack, out_new = adam_step(out_state, totals[1], rate_matrix, weight_decay)
        up_pack, up_new = adam_step(up_state, totals[2], rate_matrix, weight_decay)
        down_pack, down_new = adam_step(down_state, totals[3], rate_matrix, weight_decay)
        qkv_bias_pack, qkv_bias_new = adam_step(qkv_bias_state, totals[4], rate_vector, 0.0)
        up_bias_pack, up_bias_new = adam_step(up_bias_state, totals[5], rate_vector, 0.0)
        norm_pack, norm_new = adam_step(norm_state, totals[6], rate_vector, 0.0)
        return (
            outputs,
            input_grad,
            qkv_pack,
            qkv_new,
            out_pack,
            out_new,
            up_pack,
            up_new,
            down_pack,
            down_new,
            qkv_bias_pack,
            qkv_bias_new,
            up_bias_pack,
            up_bias_new,
            norm_pack,
            norm_new,
        )

    return local


def solution(mesh):
    return jax.shard_map(
        build(mesh),
        mesh=mesh,
        in_specs=(
            P("dp", "ctx", None),
            P("dp", "ctx", None),
            P(None, None, ("dp", "ctx"), None, "tensor"),
            P(None, None, "tensor", ("dp", "ctx")),
            P(None, None, ("dp", "ctx"), "tensor"),
            P(None, None, "tensor", ("dp", "ctx")),
            P(None, None, None, ("tensor", "dp", "ctx")),
            P(None, None, ("tensor", "dp", "ctx")),
            P(None, None, None, ("dp", "ctx")),
        ),
        out_specs=(
            P("dp", "ctx", None),
            P("dp", "ctx", None),
            P(None, None, ("dp", "ctx"), None, "tensor"),
            P(None, ("dp", "ctx"), None, "tensor"),
            P(None, None, "tensor", ("dp", "ctx")),
            P(None, "tensor", ("dp", "ctx")),
            P(None, None, ("dp", "ctx"), "tensor"),
            P(None, ("dp", "ctx"), "tensor"),
            P(None, None, "tensor", ("dp", "ctx")),
            P(None, "tensor", ("dp", "ctx")),
            P(None, None, None, ("tensor", "dp", "ctx")),
            P(None, None, ("tensor", "dp", "ctx")),
            P(None, None, ("tensor", "dp", "ctx")),
            P(None, ("tensor", "dp", "ctx")),
            P(None, None, None, ("dp", "ctx")),
            P(None, None, ("dp", "ctx")),
        ),
        check_vma=False,
    )
```

```python
import jax
import jax.numpy as jnp
from jax import lax
from jax.experimental import pallas as pl
from jax.experimental.pallas import tpu as pltpu
from jax.sharding import PartitionSpec as P

HEAD_DIM = 256
ROT = 64
STEP = 4

beta_one = 0.9
beta_two = 0.95
adam_eps = 1e-08
norm_eps = 1e-05
rate_matrix = 0.008
rate_vector = 0.2
weight_decay = 0.01

BF = jnp.bfloat16
F32 = jnp.float32
AXES = ("tensor", "dp", "ctx")
MESH = pl.DeviceIdType.MESH
ANY, VMEM = pl.ANY, pltpu.VMEM


NN = ((1,), (0,))
NT = ((1,), (1,))
TN = ((0,), (0,))


def dot(a, b, dims):
    return lax.dot_general(a, b, (dims, ((), ())), preferred_element_type=F32)


def adam_step(packed, gradient, learn_rate, decay_rate):
    moment = beta_one * packed[1] + (1.0 - beta_one) * gradient
    root_second = jnp.sqrt(
        beta_two * packed[2] * packed[2] + (1.0 - beta_two) * gradient * gradient
    )
    update = (
        learn_rate
        * (moment / (1.0 - beta_one**STEP))
        / (root_second / (1.0 - beta_two**STEP) ** 0.5 + adam_eps)
    )
    weight = packed[0] - update - learn_rate * decay_rate * packed[0]
    return (jnp.stack([gradient, moment, root_second]), weight)


def normalized(values):
    centered = values - jnp.mean(values, axis=-1, keepdims=True)
    spread = jnp.mean(centered * centered, axis=-1, keepdims=True)
    inverse = lax.rsqrt(spread + norm_eps)
    return centered * inverse, inverse


def here():
    t = lax.axis_index("tensor")
    return t // 2, t % 2, lax.axis_index("dp"), lax.axis_index("ctx")


def flip(v, k):
    out = v
    for bit in (1, 2, 4, 8):
        if k & bit:
            out = out + bit - 2 * bit * ((v // bit) % 2)
    return out


def device(th, tl, z, y):
    return {"tensor": th * 2 + tl, "dp": z, "ctx": y}


def side_of(tl, z):
    half = z // 2
    return tl + half - 2 * tl * half


def planes(side, z):
    return (
        side * z + (1 - side) * flip(z, 2),
        side * (3 - z) + (1 - side) * flip(z, 1),
    )


def fetch_goal(turn):
    th, tl, z, y = here()
    goal = 2 * tl + (z + turn) % 2
    far = goal // 2 + z // 2 - 2 * (goal // 2) * (z // 2)
    side = 1 - far if turn == 0 else far
    half = goal // 2
    core = side + half - 2 * side * half
    return th, core, goal, y


def fetch_source(turn):
    th, tl, z, y = here()
    return th, z // 2, planes(side_of(tl, z), z)[turn], y


class Task:
    def __init__(self, inputs, outs, scratch, pushes, greets, body, copies=0):
        self.inputs, self.outs, self.scratch = inputs, outs, scratch
        self.pushes, self.greets, self.body, self.copies = pushes, greets, body, copies


class Lines:
    def __init__(self, send, recv, local):
        self.send, self.recv, self.local = send, recv, local
        self.used, self.used_local, self.sent, self.closing = 0, 0, [], []

    def push(self, src, dst, to):
        copy = pltpu.make_async_remote_copy(
            src_ref=src,
            dst_ref=dst,
            send_sem=self.send.at[self.used],
            recv_sem=self.recv.at[self.used],
            device_id=device(*to),
            device_id_type=MESH,
        )
        self.used += 1
        copy.start()
        self.sent.append(copy)
        return copy

    def slots(self, n):
        at = self.used
        self.used += n
        return at

    places = slots

    def made(self, src, dst, send, recv, to):
        return pltpu.make_async_remote_copy(
            src_ref=src,
            dst_ref=dst,
            send_sem=send,
            recv_sem=recv,
            device_id=device(*to),
            device_id_type=MESH,
        )

    def copy(self, src, dst):
        copy = pltpu.make_async_copy(src, dst, self.local.at[self.used_local])
        self.used_local += 1
        copy.start()
        return copy


def run_tasks(tasks, number, name, vmem_mib):
    ins = [x for task in tasks for x, _ in task.inputs]
    in_specs = [pl.BlockSpec(memory_space=s) for task in tasks for _, s in task.inputs]
    outs = [x for task in tasks for x, _ in task.outs]
    out_specs = [pl.BlockSpec(memory_space=s) for task in tasks for _, s in task.outs]
    scratch = [x for task in tasks for x in task.scratch]
    pushes = sum(task.pushes for task in tasks)
    copies = max(1, sum(task.copies for task in tasks))
    n_in, n_out = len(ins), len(outs)

    def kernel(*refs):
        lines = Lines(*refs[-3:])
        greets = [place for task in tasks for place in task.greets()]
        barrier = pltpu.get_barrier_semaphore()
        for place in greets:
            pl.semaphore_signal(barrier, inc=1, device_id=device(*place), device_id_type=MESH)
        pl.semaphore_wait(barrier, len(greets))
        i, o, s = 0, n_in, n_in + n_out
        running = []
        for task in tasks:
            running.append(
                task.body(
                    lines,
                    refs[i : i + len(task.inputs)],
                    refs[o : o + len(task.outs)],
                    refs[s : s + len(task.scratch)],
                )
            )
            i, o, s = i + len(task.inputs), o + len(task.outs), s + len(task.scratch)
        while running:
            for body in list(running):
                try:
                    next(body)
                except StopIteration:
                    running.remove(body)
        assert lines.used == pushes, (lines.used, pushes)
        for copy in lines.sent:
            copy.wait_send()
        for close in lines.closing:
            close()

    out = pl.pallas_call(
        kernel,
        out_shape=outs,
        in_specs=in_specs,
        out_specs=out_specs,
        scratch_shapes=scratch
        + [
            pltpu.SemaphoreType.DMA((pushes,)),
            pltpu.SemaphoreType.DMA((pushes,)),
            pltpu.SemaphoreType.DMA((copies,)),
        ],
        compiler_params=pltpu.CompilerParams(
            collective_id=number, has_side_effects=True, vmem_limit_bytes=vmem_mib << 20
        ),
        name=name,
    )(*ins)
    split, at = [], 0
    for task in tasks:
        split.append(out[at : at + len(task.outs)])
        at += len(task.outs)
    return split


def shape(dims, kind):
    return jax.ShapeDtypeStruct(dims, kind)


def rows_at(start, size):
    return pl.ds(pl.multiple_of(start, size), size)


def greet_z():
    th, tl, z, y = here()
    return [(th, tl, flip(z, k), y) for k in (1, 2, 3)]


def greet_x():
    th, tl, z, y = here()
    return [(1 - th, tl, z, y)]


def spread_task(natural, C):
    S, part_rows, D = natural.shape
    quarter = part_rows // 4

    def greets():
        th, tl, z, y = here()
        plane = [
            (th, flip(tl, d), z, flip(y, j)) for j in range(C) for d in range(2) if j or d
        ]
        return greet_z() + plane + greet_x()

    def body(lines, ins, outs, scratch):
        (nat,), (whole,), (held,) = ins, outs, scratch
        th, tl, z, y = here()
        t = th * 2 + tl
        own = nat.at[:, rows_at(t * quarter, quarter), :]
        far = [lines.push(own, held.at[z], (th, tl, flip(z, k), y)) for k in (1, 2, 3)]
        lines.copy(own, held.at[z]).wait()
        yield
        for copy in far:
            copy.wait_recv()
        spots, sent = [], []
        for j in range(C):
            for d in range(2):
                yy, cc = flip(y, j), flip(tl, d)
                goal = 2 * yy + cc
                block = held.at[goal // S, goal % S]
                if j or d:
                    spot = whole.at[rows_at(y * part_rows + t * quarter, quarter), :]
                    sent.append(lines.push(block, spot, (th, cc, z, yy)))
                else:
                    spot = whole.at[rows_at(y * part_rows + t * quarter, quarter), :]
                    cross = [lines.push(block, spot, (1 - th, tl, z, y))]
                    lines.copy(block, spot).wait()
                    sent.append(None)
                spots.append(whole.at[rows_at(yy * part_rows + (th * 2 + cc) * quarter, quarter), :])
        yield
        for copy, spot in zip(sent, spots):
            if copy is not None:
                copy.wait_recv()
                cross.append(lines.push(spot, spot, (1 - th, tl, z, y)))
        yield
        yield
        for copy in cross:
            copy.wait_recv()

    pushes = 3 + 2 * (2 * C - 1) + 1
    return Task(
        [(natural, VMEM)],
        [(shape((part_rows * C, D), natural.dtype), VMEM)],
        [pltpu.VMEM((4, S, quarter, D), natural.dtype)],
        pushes,
        greets,
        body,
        2,
    )


def fetch_task(shards, aux, C):
    _, DB, width = shards.shape

    def greets():
        th, tl, z, y = here()
        across = [(th, tl, z, flip(y, j)) for j in range(1, C)] + [(th, 1 - tl, z, y)]
        return [f(turn) for turn in range(2) for f in (fetch_goal, fetch_source)] + across

    def body(lines, ins, outs, scratch):
        th, tl, z, y = here()
        mine = planes(side_of(tl, z), z)
        whole = outs[0]
        items = [(lambda turn: ins[0].at[turn], lambda a, n: whole.at[rows_at(a * DB, n * DB), :])]
        if aux is not None:
            gathered = outs[1]
            items.append((lambda turn: ins[1].at[turn], lambda a, n: gathered.at[pl.ds(a, n)]))
        first = []
        for turn in range(2):
            for source, spot in items:
                src = source(turn)
                if spot is not items[0][1]:
                    src = ins[1].at[pl.ds(turn, 1)]
                first.append(lines.push(src, spot(z * C + y, 1), fetch_goal(turn)))
        yield
        yield
        second = []
        n = 0
        for turn in range(2):
            second.append([])
            for _, spot in items:
                first[n].wait_recv()
                n += 1
                piece = spot(mine[turn] * C + y, 1)
                for j in range(1, C):
                    second[turn].append(lines.push(piece, piece, (th, tl, z, flip(y, j))))
            yield
        third = []
        for turn in range(2):
            for copy in second[turn]:
                copy.wait_recv()
            for _, spot in items:
                piece = spot(mine[turn] * C, C)
                third.append(lines.push(piece, piece, (th, 1 - tl, z, y)))
            yield
        for copy in third:
            copy.wait_recv()

    kinds = 1 if aux is None else 2
    inputs = [(shards, ANY)]
    outs = [(shape((4 * C * DB, width), shards.dtype), ANY)]
    if aux is not None:
        inputs.append((aux, ANY))
        outs.append((shape((4 * C,) + aux.shape[1:], aux.dtype), ANY))
    return Task(inputs, outs, [], kinds * (2 + 2 * (C - 1) + 2), greets, body)


def gather_task(block):
    rows, D = block.shape

    def greets():
        return greet_z() + greet_x()

    def body(lines, ins, outs, scratch):
        (src,), (whole,) = ins, outs
        th, tl, z, y = here()
        spot = lambda a, b: whole.at[rows_at((a * 4 + b) * rows, rows), :]
        cross = [lines.push(src, spot(th, z), (1 - th, tl, z, y))]
        near = [lines.push(src, spot(th, z), (th, tl, flip(z, k), y)) for k in (1, 2, 3)]
        lines.copy(src, spot(th, z)).wait()
        yield
        for k, copy in zip((1, 2, 3), near):
            copy.wait_recv()
            piece = spot(th, flip(z, k))
            cross.append(lines.push(piece, piece, (1 - th, tl, z, y)))
            yield
        for copy in cross:
            copy.wait_recv()

    return Task(
        [(block, VMEM)],
        [(shape((8 * rows, D), block.dtype), VMEM)],
        [],
        7,
        greets,
        body,
        1,
    )


def scatter_task(near, far):
    half, D = near.shape
    rows = half // 4

    def greets():
        return greet_z() + greet_x()

    def body(lines, ins, outs, scratch):
        near_ref, far_ref = ins
        (out,) = outs
        came, ready, last = scratch
        th, tl, z, y = here()
        spot = lambda ref, k: ref.at[rows_at(flip(z, k) * rows, rows), :]
        cross = {
            k: lines.push(spot(far_ref, k), came.at[k], (1 - th, tl, z, y)) for k in (3, 2, 1, 0)
        }
        yield
        along = []
        for k in (3, 2, 1):
            cross[k].wait_recv()
            term = spot(near_ref, k)[...].astype(F32) + came[k].astype(F32)
            ready[k - 1] = term.astype(BF)
            along.append(
                (k, lines.push(ready.at[k - 1], last.at[k - 1], (th, tl, flip(z, k), y)))
            )
            yield
        cross[0].wait_recv()
        total = spot(near_ref, 0)[...].astype(F32) + came[0].astype(F32)
        yield
        for k, copy in along:
            copy.wait_recv()
            total = total + last[k - 1].astype(F32)
        out[...] = total

    return Task(
        [(near, VMEM), (far, VMEM)],
        [(shape((rows, D), F32), VMEM)],
        [
            pltpu.VMEM((4, rows, D), BF),
            pltpu.VMEM((3, rows, D), BF),
            pltpu.VMEM((3, rows, D), BF),
        ],
        7,
        greets,
        body,
    )


def collect_task(m1, m2, aux, C):
    D, wide = m1.shape
    deep = m2.shape[1]
    DB = D // (4 * C)
    CB = C * DB
    tall = aux.shape

    def greets():
        th, tl, z, y = here()
        return [(th, 1 - tl, z, y)] + [(th, tl, z, flip(y, j)) for j in range(1, C)]

    def add(into, other):
        step = min(64, into.shape[0])

        def some(i, carry):
            at = pl.ds(pl.multiple_of(i * step, step), step)
            into[at, :] = (into[at, :].astype(F32) + other[at, :].astype(F32)).astype(into.dtype)
            return carry

        lax.fori_loop(0, into.shape[0] // step, some, 0)

    def body(lines, ins, outs, scratch):
        own = (scratch[0], scratch[1])
        came = (scratch[2], scratch[3])
        small_own, small_came, small_y = scratch[4:7]
        came_y = (scratch[7], scratch[8])
        th, tl, z, y = here()
        side = side_of(tl, z)
        mine, other = planes(side, z), planes(1 - side, z)
        over = (th, 1 - tl, z, y)
        sent_small = lines.push(ins[2], small_came, over)
        sent, held = [], []
        for turn in range(2):
            for n in range(2):
                at = rows_at(other[turn] * CB, CB)
                sent.append(lines.push(ins[n].at[at, :], came[n].at[turn], over))
                at = rows_at(mine[turn] * CB, CB)
                held.append(lines.copy(ins[n].at[at, :], own[n].at[turn]))
        yield
        sent_small.wait_recv()
        small_own[...] = ins[2][...] + small_came[...]
        small = [
            lines.push(small_own, small_y.at[j - 1], (th, tl, z, flip(y, j)))
            for j in range(1, C)
        ]
        across = []
        i = 0
        for turn in range(2):
            for n in range(2):
                sent[i].wait_recv()
                held[i].wait()
                i += 1
                add(own[n].at[turn], came[n].at[turn])
                for j in range(1, C):
                    at = rows_at(flip(y, j) * DB, DB)
                    across.append(
                        (
                            turn,
                            n,
                            j,
                            lines.push(
                                own[n].at[turn, at, :],
                                came_y[n].at[j - 1, turn],
                                (th, tl, z, flip(y, j)),
                            ),
                        )
                    )
            yield
        yield
        yield
        for copy in small:
            copy.wait_recv()
        total = small_own[...]
        for j in range(1, C):
            total = total + small_y[j - 1]
        outs[2][...] = total
        yield
        for turn, n, j, copy in across:
            copy.wait_recv()
            at = rows_at(y * DB, DB)
            outs_at = outs[n].at[turn]
            if j == 1:
                outs_at[...] = (
                    own[n][turn, at, :].astype(F32) + came_y[n][0, turn].astype(F32)
                ).astype(BF)
            else:
                add(outs_at, came_y[n].at[j - 1, turn])
            yield

    return Task(
        [(m1, ANY), (m2, ANY), (aux, VMEM)],
        [
            (shape((2, DB, wide), BF), VMEM),
            (shape((2, DB, deep), BF), VMEM),
            (shape(tall, F32), VMEM),
        ],
        [
            pltpu.VMEM((2, CB, wide), BF),
            pltpu.VMEM((2, CB, deep), BF),
            pltpu.VMEM((2, CB, wide), BF),
            pltpu.VMEM((2, CB, deep), BF),
            pltpu.VMEM(tall, F32),
            pltpu.VMEM(tall, F32),
            pltpu.VMEM((C - 1,) + tall, F32),
            pltpu.VMEM((C - 1, 2, DB, wide), BF),
            pltpu.VMEM((C - 1, 2, DB, deep), BF),
        ],
        5 + (C - 1) * 5,
        greets,
        body,
        4,
    )


def return_task(f1, f2, aux):
    def greets():
        return [f(turn) for turn in range(2) for f in (fetch_goal, fetch_source)]

    def body(lines, ins, outs, scratch):
        copies = []
        for turn in range(2):
            for n in range(2):
                copies.append(lines.push(ins[n].at[turn], outs[n].at[turn], fetch_source(turn)))
            copies.append(lines.push(ins[2], outs[2].at[turn], fetch_source(turn)))
        for _ in range(8):
            yield
        for copy in copies:
            copy.wait_recv()

    outs = [(shape(x.shape, x.dtype), VMEM) for x in (f1, f2)]
    outs.append((shape((2,) + aux.shape, aux.dtype), VMEM))
    return Task([(f1, VMEM), (f2, VMEM), (aux, VMEM)], outs, [], 6, greets, body)


def natural_task(block, C):
    rows, D = block.shape

    def greets():
        th, tl, z, y = here()
        return greet_z() + greet_x() + [(th, 1 - tl, z, y), (th, tl, z, 1 - y)]

    def body(lines, ins, outs, scratch):
        (src,), (out,), (stage,) = ins, outs, scratch
        th, tl, z, y = here()
        home = z == 2 * y + tl
        line = tl == z % 2
        root = jnp.logical_and(line, y == th)
        side = jnp.logical_and(line, y != th)
        leaf = tl != z % 2
        both = jnp.logical_and
        spot = lambda ref, p: ref.at[rows_at(p * rows, rows), :]
        to_home = lines.slots(1)
        at_home = lines.places(4)
        goal = 2 * y + tl
        send = lines.made(
            src, spot(stage, z), lines.send.at[to_home], lines.recv.at[at_home + z], (th, tl, goal, y)
        )
        pl.when(z != goal)(lambda: send.start())
        lines.closing.append(lambda: pl.when(z != goal)(lambda: send.wait_send()))
        base = lines.slots(12)
        own = lines.local.at[lines.used_local]
        lines.used_local += 2
        local = lines.local.at[lines.used_local - 1]
        yield
        for k in range(4):
            p = flip(z, k)
            hop = lines.made(
                spot(stage, p), spot(out, p), lines.send.at[base + k], lines.recv.at[base + k],
                (th, tl, z, 1 - y),
            )
            core = lines.made(
                spot(out, p), spot(out, p), lines.send.at[base + 4 + k],
                lines.recv.at[base + 4 + k], (th, 1 - tl, z, y),
            )
            cross = lines.made(
                spot(out, p), spot(out, p), lines.send.at[base + 8 + k],
                lines.recv.at[base + 8 + k], (1 - th, tl, z, y),
            )

            @pl.when(home)
            def _():
                if k == 0:
                    keep = pltpu.make_async_copy(src, spot(stage, p), own)
                    keep.start()
                    keep.wait()
                else:
                    lines.made(
                        src, spot(stage, p), lines.send.at[to_home],
                        lines.recv.at[at_home + p], (th, tl, goal, y),
                    ).wait_recv()

            @pl.when(both(home, y == th))
            def _():
                keep = pltpu.make_async_copy(spot(stage, p), spot(out, p), local)
                keep.start()
                keep.wait()

            pl.when(both(home, y != th))(lambda: hop.start())
            lines.closing.append(
                lambda hop=hop: pl.when(both(home, y != th))(lambda: hop.wait_send())
            )
            pl.when(both(root, jnp.logical_not(home)))(lambda: hop.wait_recv())

            @pl.when(root)
            def _():
                core.start()
                cross.start()

            lines.closing.append(
                lambda core=core: pl.when(line)(lambda: core.wait_send())
            )
            lines.closing.append(
                lambda cross=cross: pl.when(root)(lambda: cross.wait_send())
            )
            yield
        for k in range(4):
            p = flip(z, k)
            core = lines.made(
                spot(out, p), spot(out, p), lines.send.at[base + 4 + k],
                lines.recv.at[base + 4 + k], (th, 1 - tl, z, y),
            )
            cross = lines.made(
                spot(out, p), spot(out, p), lines.send.at[base + 8 + k],
                lines.recv.at[base + 8 + k], (1 - th, tl, z, y),
            )

            @pl.when(side)
            def _():
                cross.wait_recv()
                core.start()

            yield
        for k in range(4):
            p = flip(z, k)
            core = lines.made(
                spot(out, p), spot(out, p), lines.send.at[base + 4 + k],
                lines.recv.at[base + 4 + k], (th, 1 - tl, z, y),
            )
            pl.when(leaf)(lambda: core.wait_recv())

    return Task(
        [(block, VMEM)],
        [(shape((4 * rows, D), block.dtype), VMEM)],
        [pltpu.VMEM((4 * rows, D), block.dtype)],
        17,
        greets,
        body,
        2,
    )


def pack_block(l, norm_columns, bias_row, out_bias, qkv, up, out, down):
    DB, HW = qkv.shape[3], qkv.shape[4] // 2
    F8 = up.shape[3] // 2
    W1C, W2R = 3 * HW + F8, HW + F8

    def kernel(n_ref, b_ref, o_ref, qkv_ref, up_ref, out_ref, down_ref, one_ref, two_ref, aux_ref):
        z = lax.axis_index("dp")
        g1, s1 = n_ref[:, 0:1], n_ref[:, 1:2]
        g2, s2 = n_ref[:, 2:3], n_ref[:, 3:4]
        for part in range(2):
            turn = (part + z) % 2
            aux_ref[turn] = jnp.zeros(aux_ref.shape[1:], F32)
            for n in range(4):
                if n < 3:
                    w = qkv_ref[0, 0, n, :, part * HW : (part + 1) * HW]
                    at = slice(n * HW, (n + 1) * HW)
                    g, s = g1, s1
                else:
                    w = up_ref[0, 0, :, part * F8 : (part + 1) * F8]
                    at = slice(3 * HW, W1C)
                    g, s = g2, s2
                w = w.astype(BF).astype(F32)
                one_ref[turn, :, at] = (g * w).astype(BF)
                aux_ref[turn, 0:1, at] = (
                    jnp.sum(s * w, axis=0, keepdims=True) + b_ref[part : part + 1, at]
                )
            aux_ref[turn, 1:2, 0:DB] = o_ref[...]
            two_ref[turn, :, 0:HW] = out_ref[0, 0, part * HW : (part + 1) * HW, :].T.astype(BF)
            two_ref[turn, :, HW:W2R] = down_ref[0, 0, part * F8 : (part + 1) * F8, :].T.astype(BF)

    whole = lambda x: pl.BlockSpec(x.shape, lambda i: (0,) * x.ndim)
    layer = lambda x: pl.BlockSpec(
        (1, 1) + x.shape[2:], lambda i: (0, l) + (0,) * (x.ndim - 2)
    )
    return pl.pallas_call(
        kernel,
        grid=(1,),
        out_shape=[
            shape((2, DB, W1C), BF),
            shape((2, DB, W2R), BF),
            shape((2, 8, W1C), F32),
        ],
        in_specs=[whole(norm_columns), whole(bias_row), whole(out_bias)]
        + [layer(x) for x in (qkv, up, out, down)],
        out_specs=[
            pl.BlockSpec((2, DB, W1C), lambda i: (0, 0, 0)),
            pl.BlockSpec((2, DB, W2R), lambda i: (0, 0, 0)),
            pl.BlockSpec((2, 8, W1C), lambda i: (0, 0, 0)),
        ],
        compiler_params=pltpu.CompilerParams(vmem_limit_bytes=40 << 20),
        cost_estimate=pl.CostEstimate(flops=0, bytes_accessed=10 << 20, transcendentals=0),
        name="pack",
    )(norm_columns, bias_row, out_bias, qkv, up, out, down)


def turned(x, turn_ref, sign):
    half = ROT // 2
    lane = lax.broadcasted_iota(jnp.int32, x.shape, 1)
    width = x.shape[1]
    other = jnp.where(lane < half, pltpu.roll(x, width - half, 1), pltpu.roll(x, half, 1))
    return x * turn_ref[0] + other * (turn_ref[1] * sign)


def causal_block(start, width):
    rows = start + lax.broadcasted_iota(jnp.int32, (width, start + width), 0)
    return lax.broadcasted_iota(jnp.int32, (width, start + width), 1) <= rows


def forward_compute(x, w1, aux, turns, raw):
    L, D = x.shape
    W1C = w1.shape[1]
    HW = turns.shape[2]
    F8 = W1C - 3 * HW
    R = 256 if L % 256 == 0 else L
    steps = L // R

    def kernel(x_ref, w_ref, aux_ref, t_ref, *outs):
        if raw:
            xh_ref, outs = outs[0], outs[1:]
        q_ref, k_ref, v_ref, act_ref, slope_ref, lse_ref, bias_ref = outs
        i = pl.program_id(0)

        @pl.when(i == 0)
        def _():
            total = aux_ref[0, 0:1, :]
            for n in range(1, aux_ref.shape[0]):
                total = total + aux_ref[n, 0:1, :]
            bias_ref[0:1, :] = total

        rows = pl.ds(pl.multiple_of(i * R, R), R)
        if raw:
            xh = normalized(x_ref[...].astype(F32))[0].astype(BF)
            xh_ref[...] = xh
        else:
            xh = x_ref[...]
        table = t_ref.at[:, rows, :]
        for n in range(3):
            at = slice(n * HW, (n + 1) * HW)
            p = dot(xh, w_ref[:, at], NN) + bias_ref[0:1, at]
            if n == 0:
                q_ref[rows, :] = (turned(p, table, 1.0) * HEAD_DIM ** (-0.5)).astype(BF)
            elif n == 1:
                k_ref[rows, :] = turned(p, table, 1.0).astype(BF)
            else:
                v_ref[rows, :] = p.astype(BF)
        piece = min(512, F8)
        for c in range(0, F8, piece):
            at = slice(3 * HW + c, 3 * HW + c + piece)
            u = dot(xh, w_ref[:, at], NN) + bias_ref[0:1, at]
            phi = 0.5 + 0.5 * lax.erf(u * 0.5**0.5)
            act_ref[rows, HW + c : HW + c + piece] = (u * phi).astype(BF)
            slope_ref[:, c : c + piece] = (
                phi + u * (jnp.exp(-0.5 * u * u) * 0.3989422804014327)
            ).astype(BF)

        @pl.when(i == steps - 1)
        def _():
            for start in range(0, L, R):
                here_rows, seen = pl.ds(start, R), pl.ds(0, start + R)
                scores = dot(q_ref[here_rows, :], k_ref[seen, :], NT)
                scores = jnp.where(causal_block(start, R), scores, -1e30)
                peak = jnp.max(scores, axis=-1, keepdims=True)
                weights = jnp.exp(scores - peak)
                total = jnp.sum(weights, axis=-1, keepdims=True)
                weights = (weights * (1.0 / total)).astype(BF)
                act_ref[here_rows, 0:HW] = dot(weights, v_ref[seen, :], NN).astype(BF)
                lse_ref[here_rows, :] = jnp.broadcast_to(peak + jnp.log(total), (R, 128))

    fixed = lambda dims: pl.BlockSpec(dims, lambda i: (0,) * len(dims))
    moving = lambda dims: pl.BlockSpec(dims, lambda i: (i, 0))
    out_shape = [
        shape((L, HW), BF),
        shape((L, HW), BF),
        shape((L, HW), BF),
        shape((L, HW + F8), BF),
        shape((L, F8), BF),
        shape((L, 128), F32),
    ]
    out_specs = [
        fixed((L, HW)),
        fixed((L, HW)),
        fixed((L, HW)),
        fixed((L, HW + F8)),
        moving((R, F8)),
        fixed((L, 128)),
    ]
    if raw:
        out_shape.insert(0, shape((L, D), BF))
        out_specs.insert(0, moving((R, D)))
    out = pl.pallas_call(
        kernel,
        grid=(steps,),
        out_shape=out_shape,
        in_specs=[moving((R, D)), fixed(w1.shape), fixed(aux.shape), fixed(turns.shape)],
        out_specs=out_specs,
        scratch_shapes=[pltpu.VMEM((8, W1C), F32)],
        compiler_params=pltpu.CompilerParams(vmem_limit_bytes=56 << 20),
        cost_estimate=pl.CostEstimate(
            flops=2 * L * D * W1C, bytes_accessed=24 << 20, transcendentals=4 << 20
        ),
        name="forward_raw" if raw else "forward",
    )(x, w1, aux, turns)
    return out if raw else [x] + list(out)


def backward_compute(gb, w2, slope, q, k, v, lse, turns):
    L, D = gb.shape
    W2R = w2.shape[1]
    HW = q.shape[1]
    F8 = W2R - HW
    W1C = 3 * HW + F8
    R = 256 if L % 256 == 0 else L
    steps = L // R
    scale = HEAD_DIM ** (-0.5)

    def kernel(
        g_ref, w_ref, s_ref, q_ref, k_ref, v_ref, l_ref, t_ref, dy_ref, small_ref, go, dq, dk, dv
    ):
        i = pl.program_id(0)

        @pl.when(i == 0)
        def _():
            small_ref[...] = jnp.zeros_like(small_ref)
            dk[...] = jnp.zeros_like(dk)
            dv[...] = jnp.zeros_like(dv)

        rows = pl.ds(pl.multiple_of(i * R, R), R)
        g = g_ref[...]
        small_ref[1:2, 0:D] += jnp.sum(g.astype(F32), axis=0, keepdims=True)
        go[rows, :] = dot(g, w_ref[:, 0:HW], NN).astype(BF)
        piece = min(512, F8)
        for c in range(0, F8, piece):
            du = dot(g, w_ref[:, HW + c : HW + c + piece], NN)
            du = (du * s_ref[:, c : c + piece].astype(F32)).astype(BF)
            dy_ref[rows, 3 * HW + c : 3 * HW + c + piece] = du
            small_ref[0:1, 3 * HW + c : 3 * HW + c + piece] += jnp.sum(
                du.astype(F32), axis=0, keepdims=True
            )

        @pl.when(i == steps - 1)
        def _():
            for start in range(0, L, R):
                here_rows, seen = pl.ds(start, R), pl.ds(0, start + R)
                qq, gg = q_ref[here_rows, :], go[here_rows, :]
                scores = dot(qq, k_ref[seen, :], NT)
                weights = jnp.where(
                    causal_block(start, R), jnp.exp(scores - l_ref[here_rows, 0:1]), 0.0
                )
                inner = dot(gg, v_ref[seen, :], NT)
                delta = jnp.sum(weights * inner, axis=-1, keepdims=True)
                ds = (weights * (inner - delta)).astype(BF)
                dq[here_rows, :] = dot(ds, k_ref[seen, :], NN) * scale
                dk[seen, :] += dot(ds, qq, TN)
                dv[seen, :] += dot(weights.astype(BF), gg, TN)
            for n, grad in enumerate((dq, dk, dv)):
                at = slice(n * HW, (n + 1) * HW)
                value = grad[...] if n == 2 else turned(grad[...], t_ref, -1.0)
                value = value.astype(BF)
                dy_ref[:, at] = value
                small_ref[0:1, at] = jnp.sum(value.astype(F32), axis=0, keepdims=True)

    fixed = lambda dims: pl.BlockSpec(dims, lambda i: (0,) * len(dims))
    moving = lambda dims: pl.BlockSpec(dims, lambda i: (i, 0))
    return pl.pallas_call(
        kernel,
        grid=(steps,),
        out_shape=[shape((L, W1C), BF), shape((8, max(W1C, D)), F32)],
        in_specs=[moving((R, D)), fixed(w2.shape), moving((R, F8))]
        + [fixed(x.shape) for x in (q, k, v, lse, turns)],
        out_specs=[fixed((L, W1C)), fixed((8, max(W1C, D)))],
        scratch_shapes=[
            pltpu.VMEM((L, HW), BF),
            pltpu.VMEM((L, HW), F32),
            pltpu.VMEM((L, HW), F32),
            pltpu.VMEM((L, HW), F32),
        ],
        compiler_params=pltpu.CompilerParams(vmem_limit_bytes=56 << 20),
        cost_estimate=pl.CostEstimate(
            flops=2 * L * D * W2R, bytes_accessed=20 << 20, transcendentals=1 << 20
        ),
        name="backward",
    )(gb, w2, slope, q, k, v, lse, turns)


def adam_values(w, m, q, gradient, learn_rate, decay_rate):
    moment = beta_one * m + (1.0 - beta_one) * gradient
    root_second = jnp.sqrt(beta_two * q * q + (1.0 - beta_two) * gradient * gradient)
    update = (
        (learn_rate / (1.0 - beta_one**STEP))
        * moment
        / (root_second * (1.0 / (1.0 - beta_two**STEP) ** 0.5) + adam_eps)
    )
    return moment, root_second, w - update - learn_rate * decay_rate * w


def adam_block(state_ref, at, gradient, pack_ref, new_ref):
    moment, root_second, weight = adam_values(
        state_ref[(0, 0) + at],
        state_ref[(1, 0) + at],
        state_ref[(2, 0) + at],
        gradient,
        rate_matrix,
        weight_decay,
    )
    pack_ref[(0, 0) + at] = gradient
    pack_ref[(1, 0) + at] = moment
    pack_ref[(2, 0) + at] = root_second
    new_ref[(0,) + at] = weight


def adam_inner(qkv, up, r1, ra, columns):
    _, layers, _, DB, wide = qkv.shape
    HW = wide // 2
    F8 = up.shape[3] // 2
    assert layers == 2

    def qkv_kernel(*refs):
        s_ref, ra0, ra1, rb0, rb1, c0, c1, pack_ref, new_ref, term_ref = refs
        l, n = pl.program_id(0), pl.program_id(1)
        z = lax.axis_index("dp")
        first = l == 0
        col = jnp.where(first, c0[...], c1[...])
        at = pl.ds(pl.multiple_of(n * HW, HW), HW)

        @pl.when(n == 0)
        def _():
            term_ref[...] = jnp.zeros_like(term_ref)

        for part in range(2):
            turn = (part + z) % 2
            m = jnp.where(first, ra0[turn, :, at], ra1[turn, :, at]).astype(F32)
            b = jnp.where(first, rb0[turn, 0:1, at], rb1[turn, 0:1, at])
            spot = (0, slice(None), slice(part * HW, (part + 1) * HW))
            w = s_ref[(0, 0) + spot].astype(BF).astype(F32)
            term_ref[0, :, 0:1] += jnp.sum(w * m, axis=1, keepdims=True)
            term_ref[0, :, 1:2] += jnp.sum(w * b, axis=1, keepdims=True)
            adam_block(s_ref, spot, col[:, 0:1] * m + col[:, 1:2] * b, pack_ref, new_ref)

    def up_kernel(*refs):
        s_ref, ra0, ra1, rb0, rb1, c0, c1, pack_ref, new_ref, term_ref = refs
        l, part = pl.program_id(0), pl.program_id(1)
        turn = (part + lax.axis_index("dp")) % 2
        first = l == 0
        col = jnp.where(first, c0[...], c1[...])

        @pl.when(part == 0)
        def _():
            term_ref[...] = jnp.zeros_like(term_ref)

        piece = min(512, F8)
        for c in range(0, F8, piece):
            at = slice(3 * HW + c, 3 * HW + c + piece)
            m = jnp.where(first, ra0[turn, :, at], ra1[turn, :, at]).astype(F32)
            b = jnp.where(first, rb0[turn, 0:1, at], rb1[turn, 0:1, at])
            spot = (slice(None), slice(c, c + piece))
            w = s_ref[(0, 0) + spot].astype(BF).astype(F32)
            term_ref[0, :, 0:1] += jnp.sum(w * m, axis=1, keepdims=True)
            term_ref[0, :, 1:2] += jnp.sum(w * b, axis=1, keepdims=True)
            adam_block(s_ref, spot, col[:, 2:3] * m + col[:, 3:4] * b, pack_ref, new_ref)

    fixed = lambda x: pl.BlockSpec(x.shape, lambda l, n: (0,) * x.ndim)
    params = pltpu.CompilerParams(vmem_limit_bytes=48 << 20)
    small = list(r1) + list(ra) + list(columns)
    term_spec = pl.BlockSpec((1, DB, 128), lambda l, n: (l, 0, 0))
    term_shape = shape((2, DB, 128), F32)
    cost = lambda x: pl.CostEstimate(flops=0, bytes_accessed=x.size * 10, transcendentals=0)
    qkv_out = pl.pallas_call(
        qkv_kernel,
        grid=(2, 3),
        out_shape=[shape(qkv.shape, F32), shape(qkv.shape[1:], F32), term_shape],
        in_specs=[pl.BlockSpec((3, 1, 1, DB, wide), lambda l, n: (0, l, n, 0, 0))]
        + [fixed(x) for x in small],
        out_specs=[
            pl.BlockSpec((3, 1, 1, DB, wide), lambda l, n: (0, l, n, 0, 0)),
            pl.BlockSpec((1, 1, DB, wide), lambda l, n: (l, n, 0, 0)),
            term_spec,
        ],
        compiler_params=params,
        cost_estimate=cost(qkv),
        name="adam_qkv",
    )(qkv, *small)
    up_out = pl.pallas_call(
        up_kernel,
        grid=(2, 2),
        out_shape=[shape(up.shape, F32), shape(up.shape[1:], F32), term_shape],
        in_specs=[pl.BlockSpec((3, 1, DB, F8), lambda l, n: (0, l, 0, n))]
        + [fixed(x) for x in small],
        out_specs=[
            pl.BlockSpec((3, 1, DB, F8), lambda l, n: (0, l, 0, n)),
            pl.BlockSpec((1, DB, F8), lambda l, n: (l, 0, n)),
            term_spec,
        ],
        compiler_params=params,
        cost_estimate=cost(up),
        name="adam_up",
    )(up, *small)
    return qkv_out, up_out


def adam_outer(state, r2, begin, name):
    _, layers, rows, DB = state.shape
    half = rows // 2

    def kernel(s_ref, r0, r1, pack_ref, new_ref):
        l, part = pl.program_id(0), pl.program_id(1)
        turn = (part + lax.axis_index("dp")) % 2
        piece = min(256, half)
        for c in range(0, half, piece):
            at = slice(begin + c, begin + c + piece)
            m = jnp.where(l == 0, r0[turn, :, at], r1[turn, :, at]).astype(F32).T
            adam_block(s_ref, (slice(c, c + piece), slice(None)), m, pack_ref, new_ref)

    fixed = lambda x: pl.BlockSpec(x.shape, lambda l, n: (0,) * x.ndim)
    return pl.pallas_call(
        kernel,
        grid=(2, 2),
        out_shape=[shape(state.shape, F32), shape(state.shape[1:], F32)],
        in_specs=[pl.BlockSpec((3, 1, half, DB), lambda l, n: (0, l, n, 0))]
        + [fixed(x) for x in r2],
        out_specs=[
            pl.BlockSpec((3, 1, half, DB), lambda l, n: (0, l, n, 0)),
            pl.BlockSpec((1, half, DB), lambda l, n: (l, n, 0)),
        ],
        compiler_params=pltpu.CompilerParams(vmem_limit_bytes=48 << 20),
        cost_estimate=pl.CostEstimate(
            flops=0, bytes_accessed=state.size * 10, transcendentals=0
        ),
        name=name,
    )(state, *r2)


def build(mesh):
    tensor, Z, C = (mesh.shape[name] for name in AXES)
    assert tensor == 4 and Z == 4

    def flat(th, tl, z, y):
        return ((th * 2 + tl) * Z + z) * C + y

    def permute(x, move):
        pairs = []
        for th in range(2):
            for tl in range(2):
                for z in range(Z):
                    for y in range(C):
                        target = move(th, tl, z, y)
                        if target is not None:
                            pairs.append((flat(th, tl, z, y), flat(*target)))
        return lax.ppermute(x, AXES, pairs)

    def over_x(x):
        return permute(x, lambda th, tl, z, y: (1 - th, tl, z, y))

    def over_core(x):
        return permute(x, lambda th, tl, z, y: (th, 1 - tl, z, y))

    def local(
        inputs,
        cotangent,
        qkv_state,
        out_state,
        up_state,
        down_state,
        qkv_bias_state,
        up_bias_state,
        norm_state,
    ):
        layers = qkv_state.shape[1]
        S, part_rows, D = inputs.shape
        L = part_rows * C
        rows_b = L // 8
        DB = D // (Z * C)
        F8 = up_state.shape[3] // 2
        HW = qkv_state.shape[4] // 2
        W1C, W2R = 3 * HW + F8, HW + F8
        th, tl, z, y = here()
        odd = (z % 2) == 1
        place = z * C + y
        qkv_planes = jnp.transpose(qkv_state, (0, 1, 3, 2, 4))

        norm_rows = norm_state[0].astype(BF).astype(F32)
        columns = [jnp.pad(norm_rows[l].T, ((0, 0), (0, 3))) for l in range(layers)]

        def pack(l):
            rows = norm_rows[l]
            bq = qkv_bias_state[0, l].astype(BF).astype(F32)
            bu = up_bias_state[0, l].astype(BF).astype(F32)
            n = bq.shape[1]
            vq = lax.dynamic_update_slice(jnp.zeros((3, 2 * HW), F32), bq, (0, place * n))
            vu = lax.dynamic_update_slice(jnp.zeros((2 * F8,), F32), bu, (place * bu.shape[0],))
            vq = jnp.transpose(vq.reshape(3, 2, HW), (1, 0, 2)).reshape(2, 3 * HW)
            row = jnp.concatenate([vq, vu.reshape(2, F8)], axis=1)
            return pack_block(
                l, columns[l], row, rows[4:5], qkv_planes, up_state, out_state, down_state
            )

        def my_rows(whole):
            return lax.dynamic_slice_in_dim(whole, (th * 4 + z) * rows_b, rows_b, axis=0)

        def halves(act, w, dims):
            half = L // 2
            pick = lambda at: lax.dynamic_slice_in_dim(act, at * half, half, axis=0)
            far = dot(pick(1 - th), w, dims).astype(BF)
            near = dot(pick(th), w, dims).astype(BF)
            return near, far

        near_home = C == 2 and S == 1

        def return_natural(block):
            every = lax.all_gather(block, AXES, axis=0)
            every = every.reshape(2, 2, Z, C, rows_b, D)
            every = jnp.transpose(every, (3, 1, 0, 2, 4, 5)).reshape(2 * C, L, D)
            return lax.dynamic_slice(every, (z * S, y * part_rows, 0), (S, part_rows, D))

        positions = jnp.arange(L, dtype=F32)
        frequency = 10000.0 ** (-2.0 * jnp.arange(ROT // 2, dtype=F32) / ROT)
        angles = positions[:, None] * frequency[None, :]
        cosine, sine = jnp.cos(angles), jnp.sin(angles)
        rest = HEAD_DIM - ROT
        turns = jnp.stack(
            [
                jnp.concatenate([cosine, cosine, jnp.ones((L, rest), F32)], axis=1),
                jnp.concatenate([-sine, sine, jnp.zeros((L, rest), F32)], axis=1),
            ]
        )

        packs = [pack(l) for l in range(layers)]
        one, two, aux = packs[0]
        (whole_in,), (w1, aux1), (w2,) = run_tasks(
            [spread_task(inputs, C), fetch_task(one, aux, C), fetch_task(two, None, C)],
            0,
            "start",
            40,
        )
        h = my_rows(whole_in).astype(F32)
        params, saved = [], []
        x = whole_in
        number = 1
        for l in range(layers):
            xh, q, k, v, act, slope, lse = forward_compute(x, w1, aux1, turns, l == 0)
            bias_out = aux1[:, 1, :DB].reshape(1, D)
            near, far = halves(act, w2, NT)
            saved.append((h, xh, q, k, v, act, slope, lse))
            params.append((w1, w2))
            tasks = [scatter_task(near, far)]
            if l + 1 < layers:
                one, two, aux = packs[l + 1]
                tasks.append(fetch_task(one, aux, C))
            else:
                tasks.append(spread_task(cotangent, C))
            done = run_tasks(tasks, number, "scatter_f%d" % l, 48)
            h = h + done[0][0] + bias_out
            number += 1
            if l + 1 < layers:
                w1, aux1 = done[1]
                block = normalized(h)[0].astype(BF)
                (x,), (w2,) = run_tasks(
                    [gather_task(block), fetch_task(two, None, C)], number, "gather_f%d" % l, 48
                )
                number += 1
            else:
                (gb,) = done[1]
        outputs = None if near_home else return_natural(h.astype(BF))

        g = my_rows(gb).astype(F32)
        got = [None] * layers
        for l in reversed(range(layers)):
            h_in, xh, q, k, v, act, slope, lse = saved[l]
            w1, w2 = params[l]
            dy, small = backward_compute(gb, w2, slope, q, k, v, lse, turns)
            near, far = halves(dy, w1, NT)
            m1 = dot(xh, dy, TN).astype(BF)
            m2 = dot(gb, act, TN).astype(BF)
            tasks = [scatter_task(near, far), collect_task(m1, m2, small, C)]
            if outputs is None:
                tasks.append(natural_task(h.astype(BF), C))
            done = run_tasks(tasks, number, "scatter_b%d" % l, 60)
            (e,), (f1, f2, fa) = done[:2]
            if outputs is None:
                outputs = done[2][0][None]
            number += 1
            xn, inverse = normalized(h_in)
            g = g + inverse * (
                e
                - jnp.mean(e, axis=-1, keepdims=True)
                - xn * jnp.mean(e * xn, axis=-1, keepdims=True)
            )
            tasks = [return_task(f1, f2, fa)]
            if l > 0:
                tasks.insert(0, gather_task(g.astype(BF)))
            elif near_home:
                tasks.insert(0, natural_task(g.astype(BF), C))
            done = run_tasks(tasks, number, "gather_b%d" % l, 48)
            number += 1
            got[l] = done[-1]
            if l > 0:
                (gb,) = done[0]
        if near_home:
            input_grad = done[0][0][None].astype(F32)
        else:
            input_grad = return_natural(g.astype(BF)).astype(F32)

        r1, r2, ra = zip(*got)
        (qkv_pack, qkv_new, term_q), (up_pack, up_new, term_u) = adam_inner(
            qkv_planes, up_state, r1, ra, columns
        )
        terms = jnp.stack(
            [term_q[:, :, 0], term_q[:, :, 1], term_u[:, :, 0], term_u[:, :, 1]], axis=1
        )
        terms = terms + over_core(terms)
        terms = terms + over_x(terms)
        out_pack, out_new = adam_outer(out_state, r2, 0, "adam_out")
        down_pack, down_new = adam_outer(down_state, r2, HW, "adam_down")
        qkv_pack = jnp.transpose(qkv_pack, (0, 1, 3, 2, 4))
        qkv_new = jnp.transpose(qkv_new, (0, 2, 1, 3))
        small = jnp.stack(ra)
        small = jnp.where(odd, small[:, ::-1], small)
        bias_q = jnp.transpose(
            small[:, :, 0, : 3 * HW].reshape(layers, 2, 3, HW), (0, 2, 1, 3)
        ).reshape(layers, 3, 2 * HW)
        bias_u = small[:, :, 0, 3 * HW : W1C].reshape(layers, 2 * F8)
        nq, nu = qkv_bias_state.shape[3], up_bias_state.shape[2]
        bias_q = lax.dynamic_slice_in_dim(bias_q, place * nq, nq, axis=2)
        bias_u = lax.dynamic_slice_in_dim(bias_u, place * nu, nu, axis=1)
        dbo = lax.dynamic_slice_in_dim(small[:, 0, 1], place * DB, DB, axis=1)
        norm_total = jnp.concatenate([terms, dbo[:, None]], axis=1)
        qkv_bias_pack, qkv_bias_new = adam_step(qkv_bias_state, bias_q, rate_vector, 0.0)
        up_bias_pack, up_bias_new = adam_step(up_bias_state, bias_u, rate_vector, 0.0)
        norm_pack, norm_new = adam_step(norm_state, norm_total, rate_vector, 0.0)
        return (
            outputs,
            input_grad,
            qkv_pack,
            qkv_new,
            out_pack,
            out_new,
            up_pack,
            up_new,
            down_pack,
            down_new,
            qkv_bias_pack,
            qkv_bias_new,
            up_bias_pack,
            up_bias_new,
            norm_pack,
            norm_new,
        )

    return local


def solution(mesh):
    return jax.shard_map(
        build(mesh),
        mesh=mesh,
        in_specs=(
            P("dp", "ctx", None),
            P("dp", "ctx", None),
            P(None, None, ("dp", "ctx"), None, "tensor"),
            P(None, None, "tensor", ("dp", "ctx")),
            P(None, None, ("dp", "ctx"), "tensor"),
            P(None, None, "tensor", ("dp", "ctx")),
            P(None, None, None, ("tensor", "dp", "ctx")),
            P(None, None, ("tensor", "dp", "ctx")),
            P(None, None, None, ("dp", "ctx")),
        ),
        out_specs=(
            P("dp", "ctx", None),
            P("dp", "ctx", None),
            P(None, None, ("dp", "ctx"), None, "tensor"),
            P(None, ("dp", "ctx"), None, "tensor"),
            P(None, None, "tensor", ("dp", "ctx")),
            P(None, "tensor", ("dp", "ctx")),
            P(None, None, ("dp", "ctx"), "tensor"),
            P(None, ("dp", "ctx"), "tensor"),
            P(None, None, "tensor", ("dp", "ctx")),
            P(None, "tensor", ("dp", "ctx")),
            P(None, None, None, ("tensor", "dp", "ctx")),
            P(None, None, ("tensor", "dp", "ctx")),
            P(None, None, ("tensor", "dp", "ctx")),
            P(None, ("tensor", "dp", "ctx")),
            P(None, None, None, ("dp", "ctx")),
            P(None, None, ("dp", "ctx")),
        ),
        check_vma=False,
    )
```

```python
import jax
import jax.numpy as jnp
from jax import lax
from jax.experimental import pallas as pl
from jax.experimental.pallas import tpu as pltpu
from jax.sharding import PartitionSpec as P

HEAD_DIM = 256
ROT = 64
STEP = 4

beta_one = 0.9
beta_two = 0.95
adam_eps = 1e-08
norm_eps = 1e-05
rate_matrix = 0.008
rate_vector = 0.2
weight_decay = 0.01

BF = jnp.bfloat16
F32 = jnp.float32
AXES = ("tensor", "dp", "ctx")
MESH = pl.DeviceIdType.MESH
ANY, VMEM = pl.ANY, pltpu.VMEM


NN = ((1,), (0,))
NT = ((1,), (1,))
TN = ((0,), (0,))


def dot(a, b, dims):
    return lax.dot_general(a, b, (dims, ((), ())), preferred_element_type=F32)


def adam_step(packed, gradient, learn_rate, decay_rate):
    moment = beta_one * packed[1] + (1.0 - beta_one) * gradient
    root_second = jnp.sqrt(
        beta_two * packed[2] * packed[2] + (1.0 - beta_two) * gradient * gradient
    )
    update = (
        learn_rate
        * (moment / (1.0 - beta_one**STEP))
        / (root_second / (1.0 - beta_two**STEP) ** 0.5 + adam_eps)
    )
    weight = packed[0] - update - learn_rate * decay_rate * packed[0]
    return (jnp.stack([gradient, moment, root_second]), weight)


def normalized(values):
    centered = values - jnp.mean(values, axis=-1, keepdims=True)
    spread = jnp.mean(centered * centered, axis=-1, keepdims=True)
    inverse = lax.rsqrt(spread + norm_eps)
    return centered * inverse, inverse


def here():
    t = lax.axis_index("tensor")
    return t // 2, t % 2, lax.axis_index("dp"), lax.axis_index("ctx")


def flip(v, k):
    out = v
    for bit in (1, 2, 4, 8):
        if k & bit:
            out = out + bit - 2 * bit * ((v // bit) % 2)
    return out


def device(th, tl, z, y):
    return {"tensor": th * 2 + tl, "dp": z, "ctx": y}


def side_of(tl, z):
    half = z // 2
    return tl + half - 2 * tl * half


def planes(side, z):
    return (
        side * z + (1 - side) * flip(z, 2),
        side * (3 - z) + (1 - side) * flip(z, 1),
    )


def fetch_goal(turn):
    th, tl, z, y = here()
    goal = 2 * tl + (z + turn) % 2
    far = goal // 2 + z // 2 - 2 * (goal // 2) * (z // 2)
    side = 1 - far if turn == 0 else far
    half = goal // 2
    core = side + half - 2 * side * half
    return th, core, goal, y


def fetch_source(turn):
    th, tl, z, y = here()
    return th, z // 2, planes(side_of(tl, z), z)[turn], y


class Task:
    def __init__(self, inputs, outs, scratch, pushes, greets, body, copies=0):
        self.inputs, self.outs, self.scratch = inputs, outs, scratch
        self.pushes, self.greets, self.body, self.copies = pushes, greets, body, copies


class Lines:
    def __init__(self, send, recv, local):
        self.send, self.recv, self.local = send, recv, local
        self.used, self.used_local, self.sent, self.closing = 0, 0, [], []

    def push(self, src, dst, to):
        copy = pltpu.make_async_remote_copy(
            src_ref=src,
            dst_ref=dst,
            send_sem=self.send.at[self.used],
            recv_sem=self.recv.at[self.used],
            device_id=device(*to),
            device_id_type=MESH,
        )
        self.used += 1
        copy.start()
        self.sent.append(copy)
        return copy

    def slots(self, n):
        at = self.used
        self.used += n
        return at

    places = slots

    def made(self, src, dst, send, recv, to):
        return pltpu.make_async_remote_copy(
            src_ref=src,
            dst_ref=dst,
            send_sem=send,
            recv_sem=recv,
            device_id=device(*to),
            device_id_type=MESH,
        )

    def copy(self, src, dst):
        copy = pltpu.make_async_copy(src, dst, self.local.at[self.used_local])
        self.used_local += 1
        copy.start()
        return copy


def run_tasks(tasks, number, name, vmem_mib):
    ins = [x for task in tasks for x, _ in task.inputs]
    in_specs = [pl.BlockSpec(memory_space=s) for task in tasks for _, s in task.inputs]
    outs = [x for task in tasks for x, _ in task.outs]
    out_specs = [pl.BlockSpec(memory_space=s) for task in tasks for _, s in task.outs]
    scratch = [x for task in tasks for x in task.scratch]
    pushes = sum(task.pushes for task in tasks)
    copies = max(1, sum(task.copies for task in tasks))
    n_in, n_out = len(ins), len(outs)

    def kernel(*refs):
        lines = Lines(*refs[-3:])
        greets = [place for task in tasks for place in task.greets()]
        barrier = pltpu.get_barrier_semaphore()
        for place in greets:
            pl.semaphore_signal(barrier, inc=1, device_id=device(*place), device_id_type=MESH)
        pl.semaphore_wait(barrier, len(greets))
        i, o, s = 0, n_in, n_in + n_out
        running = []
        for task in tasks:
            running.append(
                task.body(
                    lines,
                    refs[i : i + len(task.inputs)],
                    refs[o : o + len(task.outs)],
                    refs[s : s + len(task.scratch)],
                )
            )
            i, o, s = i + len(task.inputs), o + len(task.outs), s + len(task.scratch)
        while running:
            for body in list(running):
                try:
                    next(body)
                except StopIteration:
                    running.remove(body)
        assert lines.used == pushes, (lines.used, pushes)
        for copy in lines.sent:
            copy.wait_send()
        for close in lines.closing:
            close()

    out = pl.pallas_call(
        kernel,
        out_shape=outs,
        in_specs=in_specs,
        out_specs=out_specs,
        scratch_shapes=scratch
        + [
            pltpu.SemaphoreType.DMA((pushes,)),
            pltpu.SemaphoreType.DMA((pushes,)),
            pltpu.SemaphoreType.DMA((copies,)),
        ],
        compiler_params=pltpu.CompilerParams(
            collective_id=number, has_side_effects=True, vmem_limit_bytes=vmem_mib << 20
        ),
        name=name,
    )(*ins)
    split, at = [], 0
    for task in tasks:
        split.append(out[at : at + len(task.outs)])
        at += len(task.outs)
    return split


def shape(dims, kind):
    return jax.ShapeDtypeStruct(dims, kind)


def rows_at(start, size):
    return pl.ds(pl.multiple_of(start, size), size)


def greet_z(steps=(1, 2)):
    th, tl, z, y = here()
    return [(th, tl, flip(z, k), y) for k in steps]


def greet_x():
    th, tl, z, y = here()
    return [(1 - th, tl, z, y)]


def spread_task(natural, C, waits=(0, 1, 1, 3)):
    S, part_rows, D = natural.shape
    quarter = part_rows // 4

    def greets():
        th, tl, z, y = here()
        plane = [
            (th, flip(tl, d), z, flip(y, j)) for j in range(C) for d in range(2) if j or d
        ]
        return greet_z() + plane + greet_x()

    def body(lines, ins, outs, scratch):
        (nat,), (whole,), (held,) = ins, outs, scratch
        th, tl, z, y = here()
        t = th * 2 + tl
        own = nat.at[:, rows_at(t * quarter, quarter), :]
        for _ in range(waits[0]):
            yield
        far = [lines.push(own, held.at[z], (th, tl, flip(z, k), y)) for k in (1, 2)]
        lines.copy(own, held.at[z]).wait()
        for _ in range(waits[1]):
            yield
        far[1].wait_recv()
        piece = held.at[flip(z, 2)]
        far.append(lines.push(piece, piece, (th, tl, flip(z, 1), y)))
        yield
        far[0].wait_recv()
        far[2].wait_recv()
        spots, sent = [], []
        for j in range(C):
            for d in range(2):
                yy, cc = flip(y, j), flip(tl, d)
                goal = 2 * yy + cc
                block = held.at[goal // S, goal % S]
                if j or d:
                    spot = whole.at[rows_at(y * part_rows + t * quarter, quarter), :]
                    sent.append(lines.push(block, spot, (th, cc, z, yy)))
                else:
                    spot = whole.at[rows_at(y * part_rows + t * quarter, quarter), :]
                    cross = [lines.push(block, spot, (1 - th, tl, z, y))]
                    lines.copy(block, spot).wait()
                    sent.append(None)
                spots.append(whole.at[rows_at(yy * part_rows + (th * 2 + cc) * quarter, quarter), :])
        for _ in range(waits[2]):
            yield
        for copy, spot in zip(sent, spots):
            if copy is not None:
                copy.wait_recv()
                cross.append(lines.push(spot, spot, (1 - th, tl, z, y)))
        for _ in range(waits[3]):
            yield
        for copy in cross:
            copy.wait_recv()

    pushes = 3 + 2 * (2 * C - 1) + 1
    return Task(
        [(natural, VMEM)],
        [(shape((part_rows * C, D), natural.dtype), VMEM)],
        [pltpu.VMEM((4, S, quarter, D), natural.dtype)],
        pushes,
        greets,
        body,
        2,
    )


def fetch_task(shards, aux, C, waits=(0, 2, 0)):
    _, DB, width = shards.shape

    def greets():
        th, tl, z, y = here()
        across = [(th, tl, z, flip(y, j)) for j in range(1, C)] + [(th, 1 - tl, z, y)]
        return [f(turn) for turn in range(2) for f in (fetch_goal, fetch_source)] + across

    def body(lines, ins, outs, scratch):
        th, tl, z, y = here()
        mine = planes(side_of(tl, z), z)
        whole = outs[0]
        items = [(lambda turn: ins[0].at[turn], lambda a, n: whole.at[rows_at(a * DB, n * DB), :])]
        if aux is not None:
            gathered = outs[1]
            items.append((lambda turn: ins[1].at[turn], lambda a, n: gathered.at[pl.ds(a, n)]))
        for _ in range(waits[0]):
            yield
        first = []
        for turn in range(2):
            for source, spot in items:
                src = source(turn)
                if spot is not items[0][1]:
                    src = ins[1].at[pl.ds(turn, 1)]
                first.append(lines.push(src, spot(z * C + y, 1), fetch_goal(turn)))
        for _ in range(waits[1]):
            yield
        second = []
        n = 0
        for turn in range(2):
            second.append([])
            for _, spot in items:
                first[n].wait_recv()
                n += 1
                piece = spot(mine[turn] * C + y, 1)
                for j in range(1, C):
                    second[turn].append(lines.push(piece, piece, (th, tl, z, flip(y, j))))
            yield
        third = []
        for _ in range(waits[2]):
            yield
        for turn in range(2):
            for copy in second[turn]:
                copy.wait_recv()
            for _, spot in items:
                piece = spot(mine[turn] * C, C)
                third.append(lines.push(piece, piece, (th, 1 - tl, z, y)))
            yield
        for copy in third:
            copy.wait_recv()

    kinds = 1 if aux is None else 2
    inputs = [(shards, ANY)]
    outs = [(shape((4 * C * DB, width), shards.dtype), ANY)]
    if aux is not None:
        inputs.append((aux, ANY))
        outs.append((shape((4 * C,) + aux.shape[1:], aux.dtype), ANY))
    return Task(inputs, outs, [], kinds * (2 + 2 * (C - 1) + 2), greets, body)


def gather_task(box, rows, D):
    def greets():
        return greet_z() + greet_x()

    def body(lines, ins, outs, scratch):
        while "block" not in box:
            yield
        yield from gather_steps(lines, box["block"], outs[0])
        box["gathered"] = True

    return Task([], [(shape((8 * rows, D), BF), VMEM)], [], 7, greets, body, 1)


def scatter_task(near, far, h, g, box):
    half, D = near.shape
    rows = half // 4

    def greets():
        return greet_z() + greet_x()

    def body(lines, ins, outs, scratch):
        near_ref, far_ref, h_ref, g_ref = ins
        (out,) = outs
        came, ready, last, block = scratch
        th, tl, z, y = here()
        spot = lambda ref, k: ref.at[rows_at(flip(z, k) * rows, rows), :]
        cross = {
            k: lines.push(spot(far_ref, k), came.at[k], (1 - th, tl, z, y)) for k in (3, 2, 1, 0)
        }
        yield
        along = {}
        for k in (3, 2, 1):
            cross[k].wait_recv()
            term = spot(near_ref, k)[...].astype(F32) + came[k].astype(F32)
            if k == 2:
                along[3].wait_recv()
                term = term + last[2].astype(F32)
            ready[k - 1] = term.astype(BF)
            goal = flip(z, 2) if k == 2 else flip(z, 1)
            along[k] = lines.push(ready.at[k - 1], last.at[k - 1], (th, tl, goal, y))
            yield
        cross[0].wait_recv()
        total = spot(near_ref, 0)[...].astype(F32) + came[0].astype(F32)
        yield
        for k in (1, 2):
            along[k].wait_recv()
            total = total + last[k - 1].astype(F32)
        xn, inverse = normalized(h_ref[...])
        value = g_ref[...] + inverse * (
            total
            - jnp.mean(total, axis=-1, keepdims=True)
            - xn * jnp.mean(total * xn, axis=-1, keepdims=True)
        )
        out[...] = value
        block[...] = value.astype(BF)
        box["block"] = block

    return Task(
        [(near, VMEM), (far, VMEM), (h, VMEM), (g, VMEM)],
        [(shape((rows, D), F32), VMEM)],
        [
            pltpu.VMEM((4, rows, D), BF),
            pltpu.VMEM((3, rows, D), BF),
            pltpu.VMEM((3, rows, D), BF),
            pltpu.VMEM((rows, D), BF),
        ],
        7,
        greets,
        body,
    )


def collect_task(m1, m2, aux, C, box):
    D, wide = m1.shape
    deep = m2.shape[1]
    DB = D // (4 * C)
    CB = C * DB
    tall = aux.shape

    def greets():
        th, tl, z, y = here()
        return [(th, 1 - tl, z, y)] + [(th, tl, z, flip(y, j)) for j in range(1, C)]

    def add(into, other):
        step = min(64, into.shape[0])

        def some(i, carry):
            at = pl.ds(pl.multiple_of(i * step, step), step)
            into[at, :] = (into[at, :].astype(F32) + other[at, :].astype(F32)).astype(into.dtype)
            return carry

        lax.fori_loop(0, into.shape[0] // step, some, 0)

    def body(lines, ins, outs, scratch):
        own = (scratch[0], scratch[1])
        came = (scratch[2], scratch[3])
        small_own, small_came, small_y = scratch[4:7]
        came_y = (scratch[7], scratch[8])
        th, tl, z, y = here()
        side = side_of(tl, z)
        mine, other = planes(side, z), planes(1 - side, z)
        over = (th, 1 - tl, z, y)
        sent_small = lines.push(ins[2], small_came, over)
        sent, held = [], []
        for turn in range(2):
            for n in range(2):
                at = rows_at(other[turn] * CB, CB)
                sent.append(lines.push(ins[n].at[at, :], came[n].at[turn], over))
                at = rows_at(mine[turn] * CB, CB)
                held.append(lines.copy(ins[n].at[at, :], own[n].at[turn]))
        yield
        sent_small.wait_recv()
        small_own[...] = ins[2][...] + small_came[...]
        small = [
            lines.push(small_own, small_y.at[j - 1], (th, tl, z, flip(y, j)))
            for j in range(1, C)
        ]
        across = []
        i = 0
        for turn in range(2):
            for n in range(2):
                sent[i].wait_recv()
                held[i].wait()
                i += 1
                add(own[n].at[turn], came[n].at[turn])
                for j in range(1, C):
                    at = rows_at(flip(y, j) * DB, DB)
                    across.append(
                        (
                            turn,
                            n,
                            j,
                            lines.push(
                                own[n].at[turn, at, :],
                                came_y[n].at[j - 1, turn],
                                (th, tl, z, flip(y, j)),
                            ),
                        )
                    )
            yield
        yield
        yield
        for copy in small:
            copy.wait_recv()
        total = small_own[...]
        for j in range(1, C):
            total = total + small_y[j - 1]
        outs[1][...] = total
        box["sums"] = outs
        yield
        for turn, n, j, copy in across:
            copy.wait_recv()
            at = rows_at(y * DB, DB)
            outs_at = outs[0].at[turn, :, 0:wide] if n == 0 else outs[0].at[turn, :, wide:]
            if j == 1:
                outs_at[...] = (
                    own[n][turn, at, :].astype(F32) + came_y[n][0, turn].astype(F32)
                ).astype(BF)
            else:
                add(outs_at, came_y[n].at[j - 1, turn])
            if n == 1 and j == C - 1:
                box["turn", turn] = True
            yield

    return Task(
        [(m1, ANY), (m2, ANY), (aux, VMEM)],
        [
            (shape((2, DB, wide + deep), BF), VMEM),
            (shape(tall, F32), VMEM),
        ],
        [
            pltpu.VMEM((2, CB, wide), BF),
            pltpu.VMEM((2, CB, deep), BF),
            pltpu.VMEM((2, CB, wide), BF),
            pltpu.VMEM((2, CB, deep), BF),
            pltpu.VMEM(tall, F32),
            pltpu.VMEM(tall, F32),
            pltpu.VMEM((C - 1,) + tall, F32),
            pltpu.VMEM((C - 1, 2, DB, wide), BF),
            pltpu.VMEM((C - 1, 2, DB, deep), BF),
        ],
        5 + (C - 1) * 5,
        greets,
        body,
        4,
    )


def return_task(f_shape, aux_shape, box):
    def greets():
        return [g(turn) for turn in range(2) for g in (fetch_goal, fetch_source)]

    def body(lines, ins, outs, scratch):
        copies = []
        for turn in range(2):
            while ("turn", turn) not in box:
                yield
            f, aux = box["sums"]
            copies.append(lines.push(f.at[turn], outs[turn], fetch_source(turn)))
            copies.append(lines.push(aux, outs[2 + turn], fetch_source(turn)))
        while "placed" not in box:
            yield
        for copy in copies:
            copy.wait_recv()

    outs = [(shape(f_shape, BF), VMEM)] * 2 + [(shape(aux_shape, F32), VMEM)] * 2
    return Task([], outs, [], 4, greets, body)


def natural_task(rows, D, box, block=None, wait=None):
    def greets():
        th, tl, z, y = here()
        return greet_z((1, 2, 3)) + greet_x() + [(th, 1 - tl, z, y), (th, tl, z, 1 - y)]

    def body(lines, ins, outs, scratch):
        (out,), (stage,) = outs, scratch
        if block is None:
            while "block" not in box:
                yield
            src = box["block"]
        else:
            src = ins[0]
        th, tl, z, y = here()
        home = z == 2 * y + tl
        line = tl == z % 2
        root = jnp.logical_and(line, y == th)
        side = jnp.logical_and(line, y != th)
        leaf = tl != z % 2
        both = jnp.logical_and
        spot = lambda ref, p: ref.at[rows_at(p * rows, rows), :]
        to_home = lines.slots(1)
        at_home = lines.places(4)
        goal = 2 * y + tl
        send = lines.made(
            src, spot(stage, z), lines.send.at[to_home], lines.recv.at[at_home + z], (th, tl, goal, y)
        )
        pl.when(z != goal)(lambda: send.start())
        lines.closing.append(lambda: pl.when(z != goal)(lambda: send.wait_send()))
        base = lines.slots(12)
        own = lines.local.at[lines.used_local]
        lines.used_local += 2
        local = lines.local.at[lines.used_local - 1]
        yield
        for k in range(4):
            p = flip(z, k)
            hop = lines.made(
                spot(stage, p), spot(out, p), lines.send.at[base + k], lines.recv.at[base + k],
                (th, tl, z, 1 - y),
            )
            @pl.when(home)
            def _():
                if k == 0:
                    keep = pltpu.make_async_copy(src, spot(stage, p), own)
                    keep.start()
                    keep.wait()
                else:
                    lines.made(
                        src, spot(stage, p), lines.send.at[to_home],
                        lines.recv.at[at_home + p], (th, tl, goal, y),
                    ).wait_recv()

            @pl.when(both(home, y == th))
            def _():
                keep = pltpu.make_async_copy(spot(stage, p), spot(out, p), local)
                keep.start()
                keep.wait()

            pl.when(both(home, y != th))(lambda: hop.start())
            lines.closing.append(
                lambda hop=hop: pl.when(both(home, y != th))(lambda: hop.wait_send())
            )
            yield
        while wait is not None and wait not in box:
            yield
        for k in range(4):
            p = flip(z, k)
            hop = lines.made(
                spot(stage, p), spot(out, p), lines.send.at[base + k], lines.recv.at[base + k],
                (th, tl, z, 1 - y),
            )
            core = lines.made(
                spot(out, p), spot(out, p), lines.send.at[base + 4 + k],
                lines.recv.at[base + 4 + k], (th, 1 - tl, z, y),
            )
            cross = lines.made(
                spot(out, p), spot(out, p), lines.send.at[base + 8 + k],
                lines.recv.at[base + 8 + k], (1 - th, tl, z, y),
            )
            pl.when(both(root, jnp.logical_not(home)))(lambda: hop.wait_recv())

            @pl.when(root)
            def _():
                core.start()
                cross.start()

            lines.closing.append(
                lambda core=core: pl.when(line)(lambda: core.wait_send())
            )
            lines.closing.append(
                lambda cross=cross: pl.when(root)(lambda: cross.wait_send())
            )
            yield
        for k in range(4):
            p = flip(z, k)
            core = lines.made(
                spot(out, p), spot(out, p), lines.send.at[base + 4 + k],
                lines.recv.at[base + 4 + k], (th, 1 - tl, z, y),
            )
            cross = lines.made(
                spot(out, p), spot(out, p), lines.send.at[base + 8 + k],
                lines.recv.at[base + 8 + k], (1 - th, tl, z, y),
            )

            @pl.when(side)
            def _():
                cross.wait_recv()
                core.start()

            yield
        for k in range(4):
            p = flip(z, k)
            core = lines.made(
                spot(out, p), spot(out, p), lines.send.at[base + 4 + k],
                lines.recv.at[base + 4 + k], (th, 1 - tl, z, y),
            )
            pl.when(leaf)(lambda: core.wait_recv())
        box["placed"] = True

    return Task(
        [] if block is None else [(block, VMEM)],
        [(shape((4 * rows, D), BF), VMEM)],
        [pltpu.VMEM((4 * rows, D), BF)],
        17,
        greets,
        body,
        2,
    )


def pack_block(l, norm_columns, bias_row, out_bias, qkv, up, out, down):
    DB, HW = qkv.shape[3], qkv.shape[4] // 2
    F8 = up.shape[3] // 2
    W1C, W2R = 3 * HW + F8, HW + F8

    def kernel(n_ref, b_ref, o_ref, qkv_ref, up_ref, out_ref, down_ref, one_ref, two_ref, aux_ref):
        z = lax.axis_index("dp")
        g1, s1 = n_ref[:, 0:1], n_ref[:, 1:2]
        g2, s2 = n_ref[:, 2:3], n_ref[:, 3:4]
        for part in range(2):
            turn = (part + z) % 2
            aux_ref[turn] = jnp.zeros(aux_ref.shape[1:], F32)
            for n in range(4):
                if n < 3:
                    w = qkv_ref[0, 0, n, :, part * HW : (part + 1) * HW]
                    at = slice(n * HW, (n + 1) * HW)
                    g, s = g1, s1
                else:
                    w = up_ref[0, 0, :, part * F8 : (part + 1) * F8]
                    at = slice(3 * HW, W1C)
                    g, s = g2, s2
                w = w.astype(BF).astype(F32)
                one_ref[turn, :, at] = (g * w).astype(BF)
                aux_ref[turn, 0:1, at] = (
                    jnp.sum(s * w, axis=0, keepdims=True) + b_ref[part : part + 1, at]
                )
            aux_ref[turn, 1:2, 0:DB] = o_ref[...]
            two_ref[turn, :, 0:HW] = out_ref[0, 0, part * HW : (part + 1) * HW, :].T.astype(BF)
            two_ref[turn, :, HW:W2R] = down_ref[0, 0, part * F8 : (part + 1) * F8, :].T.astype(BF)

    whole = lambda x: pl.BlockSpec(x.shape, lambda i: (0,) * x.ndim)
    layer = lambda x: pl.BlockSpec(
        (1, 1) + x.shape[2:], lambda i: (0, l) + (0,) * (x.ndim - 2)
    )
    return pl.pallas_call(
        kernel,
        grid=(1,),
        out_shape=[
            shape((2, DB, W1C), BF),
            shape((2, DB, W2R), BF),
            shape((2, 8, W1C), F32),
        ],
        in_specs=[whole(norm_columns), whole(bias_row), whole(out_bias)]
        + [layer(x) for x in (qkv, up, out, down)],
        out_specs=[
            pl.BlockSpec((2, DB, W1C), lambda i: (0, 0, 0)),
            pl.BlockSpec((2, DB, W2R), lambda i: (0, 0, 0)),
            pl.BlockSpec((2, 8, W1C), lambda i: (0, 0, 0)),
        ],
        compiler_params=pltpu.CompilerParams(vmem_limit_bytes=40 << 20),
        cost_estimate=pl.CostEstimate(flops=0, bytes_accessed=10 << 20, transcendentals=0),
        name="pack",
    )(norm_columns, bias_row, out_bias, qkv, up, out, down)


def turned(x, turn_ref, sign):
    half = ROT // 2
    lane = lax.broadcasted_iota(jnp.int32, x.shape, 1)
    width = x.shape[1]
    other = jnp.where(lane < half, pltpu.roll(x, width - half, 1), pltpu.roll(x, half, 1))
    return x * turn_ref[0] + other * (turn_ref[1] * sign)


def causal_block(start, width):
    rows = start + lax.broadcasted_iota(jnp.int32, (width, start + width), 0)
    return lax.broadcasted_iota(jnp.int32, (width, start + width), 1) <= rows


def forward_compute(x, w1, aux, turns, raw):
    L, D = x.shape
    W1C = w1.shape[1]
    HW = turns.shape[2]
    F8 = W1C - 3 * HW
    R = 256 if L % 256 == 0 else L
    steps = L // R

    def kernel(x_ref, w_ref, aux_ref, t_ref, *outs):
        if raw:
            xh_ref, outs = outs[0], outs[1:]
        q_ref, k_ref, v_ref, act_ref, slope_ref, lse_ref, bias_ref = outs
        i = pl.program_id(0)

        @pl.when(i == 0)
        def _():
            total = aux_ref[0, 0:1, :]
            for n in range(1, aux_ref.shape[0]):
                total = total + aux_ref[n, 0:1, :]
            bias_ref[0:1, :] = total

        rows = pl.ds(pl.multiple_of(i * R, R), R)
        if raw:
            xh = normalized(x_ref[...].astype(F32))[0].astype(BF)
            xh_ref[...] = xh
        else:
            xh = x_ref[...]
        table = t_ref.at[:, rows, :]
        for n in range(3):
            at = slice(n * HW, (n + 1) * HW)
            p = dot(xh, w_ref[:, at], NN) + bias_ref[0:1, at]
            if n == 0:
                q_ref[rows, :] = (turned(p, table, 1.0) * HEAD_DIM ** (-0.5)).astype(BF)
            elif n == 1:
                k_ref[rows, :] = turned(p, table, 1.0).astype(BF)
            else:
                v_ref[rows, :] = p.astype(BF)
        piece = min(512, F8)
        for c in range(0, F8, piece):
            at = slice(3 * HW + c, 3 * HW + c + piece)
            u = dot(xh, w_ref[:, at], NN) + bias_ref[0:1, at]
            phi = 0.5 + 0.5 * lax.erf(u * 0.5**0.5)
            act_ref[rows, HW + c : HW + c + piece] = (u * phi).astype(BF)
            slope_ref[:, c : c + piece] = (
                phi + u * (jnp.exp(-0.5 * u * u) * 0.3989422804014327)
            ).astype(BF)

        @pl.when(i == steps - 1)
        def _():
            for start in range(0, L, R):
                here_rows, seen = pl.ds(start, R), pl.ds(0, start + R)
                scores = dot(q_ref[here_rows, :], k_ref[seen, :], NT)
                scores = jnp.where(causal_block(start, R), scores, -1e30)
                peak = jnp.max(scores, axis=-1, keepdims=True)
                weights = jnp.exp(scores - peak)
                total = jnp.sum(weights, axis=-1, keepdims=True)
                weights = (weights * (1.0 / total)).astype(BF)
                act_ref[here_rows, 0:HW] = dot(weights, v_ref[seen, :], NN).astype(BF)
                lse_ref[here_rows, :] = jnp.broadcast_to(peak + jnp.log(total), (R, 128))

    fixed = lambda dims: pl.BlockSpec(dims, lambda i: (0,) * len(dims))
    moving = lambda dims: pl.BlockSpec(dims, lambda i: (i, 0))
    out_shape = [
        shape((L, HW), BF),
        shape((L, HW), BF),
        shape((L, HW), BF),
        shape((L, HW + F8), BF),
        shape((L, F8), BF),
        shape((L, 128), F32),
    ]
    out_specs = [
        fixed((L, HW)),
        fixed((L, HW)),
        fixed((L, HW)),
        fixed((L, HW + F8)),
        moving((R, F8)),
        fixed((L, 128)),
    ]
    if raw:
        out_shape.insert(0, shape((L, D), BF))
        out_specs.insert(0, moving((R, D)))
    out = pl.pallas_call(
        kernel,
        grid=(steps,),
        out_shape=out_shape,
        in_specs=[moving((R, D)), fixed(w1.shape), fixed(aux.shape), fixed(turns.shape)],
        out_specs=out_specs,
        scratch_shapes=[pltpu.VMEM((8, W1C), F32)],
        compiler_params=pltpu.CompilerParams(vmem_limit_bytes=56 << 20),
        cost_estimate=pl.CostEstimate(
            flops=2 * L * D * W1C, bytes_accessed=24 << 20, transcendentals=4 << 20
        ),
        name="forward_raw" if raw else "forward",
    )(x, w1, aux, turns)
    return out if raw else [x] + list(out)


def backward_compute(gb, w2, slope, q, k, v, lse, turns):
    L, D = gb.shape
    W2R = w2.shape[1]
    HW = q.shape[1]
    F8 = W2R - HW
    W1C = 3 * HW + F8
    R = 256 if L % 256 == 0 else L
    steps = L // R
    scale = HEAD_DIM ** (-0.5)

    def kernel(
        g_ref, w_ref, s_ref, q_ref, k_ref, v_ref, l_ref, t_ref, dy_ref, small_ref, go, dq, dk, dv
    ):
        i = pl.program_id(0)

        @pl.when(i == 0)
        def _():
            small_ref[...] = jnp.zeros_like(small_ref)
            dk[...] = jnp.zeros_like(dk)
            dv[...] = jnp.zeros_like(dv)

        rows = pl.ds(pl.multiple_of(i * R, R), R)
        g = g_ref[...]
        small_ref[1:2, 0:D] += jnp.sum(g.astype(F32), axis=0, keepdims=True)
        go[rows, :] = dot(g, w_ref[:, 0:HW], NN).astype(BF)
        piece = min(512, F8)
        for c in range(0, F8, piece):
            du = dot(g, w_ref[:, HW + c : HW + c + piece], NN)
            du = (du * s_ref[:, c : c + piece].astype(F32)).astype(BF)
            dy_ref[rows, 3 * HW + c : 3 * HW + c + piece] = du
            small_ref[0:1, 3 * HW + c : 3 * HW + c + piece] += jnp.sum(
                du.astype(F32), axis=0, keepdims=True
            )

        @pl.when(i == steps - 1)
        def _():
            for start in range(0, L, R):
                here_rows, seen = pl.ds(start, R), pl.ds(0, start + R)
                qq, gg = q_ref[here_rows, :], go[here_rows, :]
                scores = dot(qq, k_ref[seen, :], NT)
                weights = jnp.where(
                    causal_block(start, R), jnp.exp(scores - l_ref[here_rows, 0:1]), 0.0
                )
                inner = dot(gg, v_ref[seen, :], NT)
                delta = jnp.sum(weights * inner, axis=-1, keepdims=True)
                ds = (weights * (inner - delta)).astype(BF)
                dq[here_rows, :] = dot(ds, k_ref[seen, :], NN) * scale
                dk[seen, :] += dot(ds, qq, TN)
                dv[seen, :] += dot(weights.astype(BF), gg, TN)
            for n, grad in enumerate((dq, dk, dv)):
                at = slice(n * HW, (n + 1) * HW)
                value = grad[...] if n == 2 else turned(grad[...], t_ref, -1.0)
                value = value.astype(BF)
                dy_ref[:, at] = value
                small_ref[0:1, at] = jnp.sum(value.astype(F32), axis=0, keepdims=True)

    fixed = lambda dims: pl.BlockSpec(dims, lambda i: (0,) * len(dims))
    moving = lambda dims: pl.BlockSpec(dims, lambda i: (i, 0))
    return pl.pallas_call(
        kernel,
        grid=(steps,),
        out_shape=[shape((L, W1C), BF), shape((8, max(W1C, D)), F32)],
        in_specs=[moving((R, D)), fixed(w2.shape), moving((R, F8))]
        + [fixed(x.shape) for x in (q, k, v, lse, turns)],
        out_specs=[fixed((L, W1C)), fixed((8, max(W1C, D)))],
        scratch_shapes=[
            pltpu.VMEM((L, HW), BF),
            pltpu.VMEM((L, HW), F32),
            pltpu.VMEM((L, HW), F32),
            pltpu.VMEM((L, HW), F32),
        ],
        compiler_params=pltpu.CompilerParams(vmem_limit_bytes=56 << 20),
        cost_estimate=pl.CostEstimate(
            flops=2 * L * D * W2R, bytes_accessed=20 << 20, transcendentals=1 << 20
        ),
        name="backward",
    )(gb, w2, slope, q, k, v, lse, turns)


def adam_values(w, m, q, gradient, learn_rate, decay_rate):
    moment = beta_one * m + (1.0 - beta_one) * gradient
    root_second = jnp.sqrt(beta_two * q * q + (1.0 - beta_two) * gradient * gradient)
    update = (
        (learn_rate / (1.0 - beta_one**STEP))
        * moment
        / (root_second * (1.0 / (1.0 - beta_two**STEP) ** 0.5) + adam_eps)
    )
    return moment, root_second, w - update - learn_rate * decay_rate * w


def adam_block(state_ref, at, gradient, pack_ref, new_ref):
    moment, root_second, weight = adam_values(
        state_ref[(0, 0) + at],
        state_ref[(1, 0) + at],
        state_ref[(2, 0) + at],
        gradient,
        rate_matrix,
        weight_decay,
    )
    pack_ref[(0, 0) + at] = gradient
    pack_ref[(1, 0) + at] = moment
    pack_ref[(2, 0) + at] = root_second
    new_ref[(0,) + at] = weight


def chosen(first, turn, values):
    even = turn == 0
    return jnp.where(
        first, jnp.where(even, values[0], values[1]), jnp.where(even, values[2], values[3])
    )


def adam_inner(qkv, up, grads, smalls, columns):
    _, layers, _, DB, wide = qkv.shape
    HW = wide // 2
    F8 = up.shape[3] // 2
    assert layers == 2

    def qkv_kernel(*refs):
        s_ref, grads, smalls, (c0, c1) = refs[0], refs[1:5], refs[5:9], refs[9:11]
        pack_ref, new_ref, term_ref = refs[11:]
        l, n = pl.program_id(0), pl.program_id(1)
        z = lax.axis_index("dp")
        first = l == 0
        col = jnp.where(first, c0[...], c1[...])
        at = pl.ds(pl.multiple_of(n * HW, HW), HW)

        @pl.when(n == 0)
        def _():
            term_ref[...] = jnp.zeros_like(term_ref)

        for part in range(2):
            turn = (part + z) % 2
            m = chosen(first, turn, [g[:, at] for g in grads]).astype(F32)
            b = chosen(first, turn, [g[0:1, at] for g in smalls])
            spot = (0, slice(None), slice(part * HW, (part + 1) * HW))
            w = s_ref[(0, 0) + spot].astype(BF).astype(F32)
            term_ref[0, :, 0:1] += jnp.sum(w * m, axis=1, keepdims=True)
            term_ref[0, :, 1:2] += jnp.sum(w * b, axis=1, keepdims=True)
            adam_block(s_ref, spot, col[:, 0:1] * m + col[:, 1:2] * b, pack_ref, new_ref)

    def up_kernel(*refs):
        s_ref, grads, smalls, (c0, c1) = refs[0], refs[1:5], refs[5:9], refs[9:11]
        pack_ref, new_ref, term_ref = refs[11:]
        l, part = pl.program_id(0), pl.program_id(1)
        turn = (part + lax.axis_index("dp")) % 2
        first = l == 0
        col = jnp.where(first, c0[...], c1[...])

        @pl.when(part == 0)
        def _():
            term_ref[...] = jnp.zeros_like(term_ref)

        piece = min(512, F8)
        for c in range(0, F8, piece):
            at = slice(3 * HW + c, 3 * HW + c + piece)
            m = chosen(first, turn, [g[:, at] for g in grads]).astype(F32)
            b = chosen(first, turn, [g[0:1, at] for g in smalls])
            spot = (slice(None), slice(c, c + piece))
            w = s_ref[(0, 0) + spot].astype(BF).astype(F32)
            term_ref[0, :, 0:1] += jnp.sum(w * m, axis=1, keepdims=True)
            term_ref[0, :, 1:2] += jnp.sum(w * b, axis=1, keepdims=True)
            adam_block(s_ref, spot, col[:, 2:3] * m + col[:, 3:4] * b, pack_ref, new_ref)

    fixed = lambda x: pl.BlockSpec(x.shape, lambda l, n: (0,) * x.ndim)
    params = pltpu.CompilerParams(vmem_limit_bytes=48 << 20)
    small = list(grads) + list(smalls) + list(columns)
    term_spec = pl.BlockSpec((1, DB, 128), lambda l, n: (l, 0, 0))
    term_shape = shape((2, DB, 128), F32)
    cost = lambda x: pl.CostEstimate(flops=0, bytes_accessed=x.size * 10, transcendentals=0)
    qkv_out = pl.pallas_call(
        qkv_kernel,
        grid=(2, 3),
        out_shape=[shape(qkv.shape, F32), shape(qkv.shape[1:], F32), term_shape],
        in_specs=[pl.BlockSpec((3, 1, 1, DB, wide), lambda l, n: (0, l, n, 0, 0))]
        + [fixed(x) for x in small],
        out_specs=[
            pl.BlockSpec((3, 1, 1, DB, wide), lambda l, n: (0, l, n, 0, 0)),
            pl.BlockSpec((1, 1, DB, wide), lambda l, n: (l, n, 0, 0)),
            term_spec,
        ],
        compiler_params=params,
        cost_estimate=cost(qkv),
        name="adam_qkv",
    )(qkv, *small)
    up_out = pl.pallas_call(
        up_kernel,
        grid=(2, 2),
        out_shape=[shape(up.shape, F32), shape(up.shape[1:], F32), term_shape],
        in_specs=[pl.BlockSpec((3, 1, DB, F8), lambda l, n: (0, l, 0, n))]
        + [fixed(x) for x in small],
        out_specs=[
            pl.BlockSpec((3, 1, DB, F8), lambda l, n: (0, l, 0, n)),
            pl.BlockSpec((1, DB, F8), lambda l, n: (l, 0, n)),
            term_spec,
        ],
        compiler_params=params,
        cost_estimate=cost(up),
        name="adam_up",
    )(up, *small)
    return qkv_out, up_out


def adam_outer(state, grads, begin, name):
    _, layers, rows, DB = state.shape
    half = rows // 2

    def kernel(s_ref, *refs):
        pack_ref, new_ref = refs[4:]
        l, part = pl.program_id(0), pl.program_id(1)
        turn = (part + lax.axis_index("dp")) % 2
        piece = min(256, half)
        for c in range(0, half, piece):
            at = slice(begin + c, begin + c + piece)
            m = chosen(l == 0, turn, [g[:, at] for g in refs[:4]]).astype(F32).T
            adam_block(s_ref, (slice(c, c + piece), slice(None)), m, pack_ref, new_ref)

    fixed = lambda x: pl.BlockSpec(x.shape, lambda l, n: (0,) * x.ndim)
    return pl.pallas_call(
        kernel,
        grid=(2, 2),
        out_shape=[shape(state.shape, F32), shape(state.shape[1:], F32)],
        in_specs=[pl.BlockSpec((3, 1, half, DB), lambda l, n: (0, l, n, 0))]
        + [fixed(x) for x in grads],
        out_specs=[
            pl.BlockSpec((3, 1, half, DB), lambda l, n: (0, l, n, 0)),
            pl.BlockSpec((1, half, DB), lambda l, n: (l, n, 0)),
        ],
        compiler_params=pltpu.CompilerParams(vmem_limit_bytes=48 << 20),
        cost_estimate=pl.CostEstimate(
            flops=0, bytes_accessed=state.size * 10, transcendentals=0
        ),
        name=name,
    )(state, *grads)


def piece_dot(lhs, w_ref, write):
    D = w_ref.shape[0]
    tile = min(512, D)

    def some(c, carry):
        at = pl.ds(pl.multiple_of(c * tile, tile), tile)
        write(at, dot(lhs, w_ref[at, :], NT))
        return carry

    lax.fori_loop(0, D // tile, some, 0)


def scatter_steps(lines, lhs_of, w_ref, far, came, ready, last, total):
    th, tl, z, y = here()

    def rows_of(half, k):
        return lhs_of((half * 4 + flip(z, k)))

    cross = {}
    for k in (3, 2, 1, 0):
        lhs = rows_of(1 - th, k)

        def keep(at, value, k=k):
            far[k, :, at] = value.astype(BF)

        piece_dot(lhs, w_ref, keep)
        cross[k] = lines.push(far.at[k], came.at[k], (1 - th, tl, z, y))
    yield
    along = {}
    for k in (3, 2, 1):
        lhs = rows_of(th, k)
        cross[k].wait_recv()
        if k == 2:
            along[3].wait_recv()

        def keep(at, value, k=k):
            value = value + came[k, :, at].astype(F32)
            if k == 2:
                value = value + last[2, :, at].astype(F32)
            ready[k - 1, :, at] = value.astype(BF)

        piece_dot(lhs, w_ref, keep)
        goal = flip(z, 2) if k == 2 else flip(z, 1)
        along[k] = lines.push(ready.at[k - 1], last.at[k - 1], (th, tl, goal, y))
        yield
    lhs = rows_of(th, 0)

    def keep(at, value):
        total[:, at] = value

    piece_dot(lhs, w_ref, keep)
    cross[0].wait_recv()
    yield
    value = total[...] + came[0].astype(F32)
    for k in (1, 2):
        along[k].wait_recv()
        value = value + last[k - 1].astype(F32)
    total[...] = value


def gather_steps(lines, src, whole):
    th, tl, z, y = here()
    rows = src.shape[0]
    spot = lambda a, b: whole.at[rows_at((a * 4 + b) * rows, rows), :]
    cross = [lines.push(src, spot(th, z), (1 - th, tl, z, y))]
    near = {k: lines.push(src, spot(th, z), (th, tl, flip(z, k), y)) for k in (1, 2)}
    lines.copy(src, spot(th, z)).wait()
    yield
    for k in (1, 2, 3):
        near[k].wait_recv()
        piece = spot(th, flip(z, k))
        if k == 2:
            near[3] = lines.push(piece, piece, (th, tl, flip(z, 1), y))
        cross.append(lines.push(piece, piece, (1 - th, tl, z, y)))
        yield
    for copy in cross:
        copy.wait_recv()


def forward_task(x, w1, w2, aux, turns, h, bias_out, onward):
    L, D = x.shape
    raw = h is None
    W1C, W2R = w1.shape[1], w2.shape[1]
    HW = turns.shape[2]
    F8 = W1C - 3 * HW
    R = 256 if L % 256 == 0 else L
    steps = L // R
    rows_b = L // 8

    def greets():
        return greet_z() + greet_x()

    def body(lines, ins, outs, scratch):
        x_ref, w1_ref, w2_ref, aux_ref, t_ref, bo_ref = ins[:6]
        q_ref, k_ref, v_ref, act_ref, slope_ref, lse_ref, new_ref = outs[:7]
        w1_in, w2_in, bias_ref, far, came, ready, last, block = scratch
        th, tl, z, y = here()
        load1 = lines.copy(w1_ref, w1_in)
        load2 = lines.copy(w2_ref, w2_in)
        total = aux_ref[0, 0:1, :]
        for n in range(1, aux_ref.shape[0]):
            total = total + aux_ref[n, 0:1, :]
        bias_ref[0:1, :] = total
        load1.wait()

        def some(i, carry):
            rows = pl.ds(pl.multiple_of(i * R, R), R)
            if raw:
                xh = normalized(x_ref[rows, :].astype(F32))[0].astype(BF)
                outs[7][rows, :] = xh
            else:
                xh = x_ref[rows, :]
            table = t_ref.at[:, rows, :]
            for n in range(3):
                at = slice(n * HW, (n + 1) * HW)
                p = dot(xh, w1_in[:, at], NN) + bias_ref[0:1, at]
                if n == 0:
                    q_ref[rows, :] = (turned(p, table, 1.0) * HEAD_DIM ** (-0.5)).astype(BF)
                elif n == 1:
                    k_ref[rows, :] = turned(p, table, 1.0).astype(BF)
                else:
                    v_ref[rows, :] = p.astype(BF)
            piece = min(512, F8)
            for c in range(0, F8, piece):
                at = slice(3 * HW + c, 3 * HW + c + piece)
                u = dot(xh, w1_in[:, at], NN) + bias_ref[0:1, at]
                phi = 0.5 + 0.5 * lax.erf(u * 0.5**0.5)
                act_ref[rows, HW + c : HW + c + piece] = (u * phi).astype(BF)
                slope_ref[rows, c : c + piece] = (
                    phi + u * (jnp.exp(-0.5 * u * u) * 0.3989422804014327)
                ).astype(BF)
            return carry

        lax.fori_loop(0, steps, some, 0)
        for start in range(0, L, R):
            here_rows, seen = pl.ds(start, R), pl.ds(0, start + R)
            scores = dot(q_ref[here_rows, :], k_ref[seen, :], NT)
            scores = jnp.where(causal_block(start, R), scores, -1e30)
            peak = jnp.max(scores, axis=-1, keepdims=True)
            weights = jnp.exp(scores - peak)
            total = jnp.sum(weights, axis=-1, keepdims=True)
            weights = (weights * (1.0 / total)).astype(BF)
            act_ref[here_rows, 0:HW] = dot(weights, v_ref[seen, :], NN).astype(BF)
            lse_ref[here_rows, :] = jnp.broadcast_to(peak + jnp.log(total), (R, 128))
        load2.wait()
        yield
        yield from scatter_steps(
            lines,
            lambda n: act_ref[rows_at(n * rows_b, rows_b), :],
            w2_in,
            far,
            came,
            ready,
            last,
            new_ref,
        )
        if raw:
            before = x_ref[rows_at((th * 4 + z) * rows_b, rows_b), :].astype(F32)
        else:
            before = ins[6][...]
        new = before + new_ref[...] + bo_ref[...]
        new_ref[...] = new
        if onward:
            block[...] = normalized(new)[0].astype(BF)
            yield from gather_steps(lines, block, outs[-1])

    inputs = [(x, VMEM), (w1, ANY), (w2, ANY), (aux, VMEM), (turns, VMEM), (bias_out, VMEM)]
    outs = [
        (shape((L, HW), BF), VMEM),
        (shape((L, HW), BF), VMEM),
        (shape((L, HW), BF), VMEM),
        (shape((L, HW + F8), BF), VMEM),
        (shape((L, F8), BF), VMEM),
        (shape((L, 128), F32), VMEM),
        (shape((rows_b, D), F32), VMEM),
    ]
    if raw:
        outs.append((shape((L, D), BF), VMEM))
    else:
        inputs.append((h, VMEM))
    if onward:
        outs.append((shape((L, D), BF), VMEM))
    return Task(
        inputs,
        outs,
        [
            pltpu.VMEM(w1.shape, BF),
            pltpu.VMEM(w2.shape, BF),
            pltpu.VMEM((8, W1C), F32),
            pltpu.VMEM((4, rows_b, D), BF),
            pltpu.VMEM((4, rows_b, D), BF),
            pltpu.VMEM((3, rows_b, D), BF),
            pltpu.VMEM((3, rows_b, D), BF),
            pltpu.VMEM((rows_b, D), BF),
        ],
        14 if onward else 7,
        greets,
        body,
        3 if onward else 2,
    )


def build(mesh):
    tensor, Z, C = (mesh.shape[name] for name in AXES)
    assert tensor == 4 and Z == 4

    def flat(th, tl, z, y):
        return ((th * 2 + tl) * Z + z) * C + y

    def permute(x, move):
        pairs = []
        for th in range(2):
            for tl in range(2):
                for z in range(Z):
                    for y in range(C):
                        target = move(th, tl, z, y)
                        if target is not None:
                            pairs.append((flat(th, tl, z, y), flat(*target)))
        return lax.ppermute(x, AXES, pairs)

    def give_move(turn):
        def move(th, tl, z, y):
            side = tl ^ (z // 2)
            return (th, z // 2, z ^ (2 - 2 * side if turn == 0 else 1 + 2 * side), y)

        return move

    def over_x(x):
        return permute(x, lambda th, tl, z, y: (1 - th, tl, z, y))

    def over_core(x):
        return permute(x, lambda th, tl, z, y: (th, 1 - tl, z, y))

    def local(
        inputs,
        cotangent,
        qkv_state,
        out_state,
        up_state,
        down_state,
        qkv_bias_state,
        up_bias_state,
        norm_state,
    ):
        layers = qkv_state.shape[1]
        S, part_rows, D = inputs.shape
        L = part_rows * C
        rows_b = L // 8
        DB = D // (Z * C)
        F8 = up_state.shape[3] // 2
        HW = qkv_state.shape[4] // 2
        W1C, W2R = 3 * HW + F8, HW + F8
        th, tl, z, y = here()
        odd = (z % 2) == 1
        place = z * C + y
        qkv_planes = jnp.transpose(qkv_state, (0, 1, 3, 2, 4))

        norm_rows = norm_state[0].astype(BF).astype(F32)
        columns = [jnp.pad(norm_rows[l].T, ((0, 0), (0, 3))) for l in range(layers)]

        def pack(l):
            rows = norm_rows[l]
            bq = qkv_bias_state[0, l].astype(BF).astype(F32)
            bu = up_bias_state[0, l].astype(BF).astype(F32)
            n = bq.shape[1]
            vq = lax.dynamic_update_slice(jnp.zeros((3, 2 * HW), F32), bq, (0, place * n))
            vu = lax.dynamic_update_slice(jnp.zeros((2 * F8,), F32), bu, (place * bu.shape[0],))
            vq = jnp.transpose(vq.reshape(3, 2, HW), (1, 0, 2)).reshape(2, 3 * HW)
            row = jnp.concatenate([vq, vu.reshape(2, F8)], axis=1)
            return pack_block(
                l, columns[l], row, rows[4:5], qkv_planes, up_state, out_state, down_state
            )

        def my_rows(whole):
            return lax.dynamic_slice_in_dim(whole, (th * 4 + z) * rows_b, rows_b, axis=0)

        def halves(act, w, dims):
            half = L // 2
            pick = lambda at: lax.dynamic_slice_in_dim(act, at * half, half, axis=0)
            far = dot(pick(1 - th), w, dims).astype(BF)
            near = dot(pick(th), w, dims).astype(BF)
            return near, far

        near_home = C == 2 and S == 1

        def return_natural(block):
            every = lax.all_gather(block, AXES, axis=0)
            every = every.reshape(2, 2, Z, C, rows_b, D)
            every = jnp.transpose(every, (3, 1, 0, 2, 4, 5)).reshape(2 * C, L, D)
            return lax.dynamic_slice(every, (z * S, y * part_rows, 0), (S, part_rows, D))

        positions = jnp.arange(L, dtype=F32)
        frequency = 10000.0 ** (-2.0 * jnp.arange(ROT // 2, dtype=F32) / ROT)
        angles = positions[:, None] * frequency[None, :]
        cosine, sine = jnp.cos(angles), jnp.sin(angles)
        rest = HEAD_DIM - ROT
        turns = jnp.stack(
            [
                jnp.concatenate([cosine, cosine, jnp.ones((L, rest), F32)], axis=1),
                jnp.concatenate([-sine, sine, jnp.zeros((L, rest), F32)], axis=1),
            ]
        )

        packs = [pack(l) for l in range(layers)]
        one, two, aux = packs[0]
        (whole_in,), (gb,), (w1, aux1), (w2,) = run_tasks(
            [
                spread_task(inputs, C, (0, 1, 1, 3)),
                spread_task(cotangent, C, (1, 2, 1, 3)),
                fetch_task(one, aux, C, (3, 2, 1)),
                fetch_task(two, None, C, (3, 4, 1)),
            ],
            0,
            "start",
            48,
        )
        params, saved = [], []
        x, h = whole_in, None
        number = 1
        for l in range(layers):
            bias_out = aux1[:, 1, :DB].reshape(1, D)
            onward = l + 1 < layers
            task = forward_task(x, w1, w2, aux1, turns, h, bias_out, onward)
            if onward:
                one, two, aux = packs[l + 1]
                tasks = [
                    fetch_task(one, aux, C, (0, 2, 2)),
                    task,
                    fetch_task(two, None, C, (1, 8, 0)),
                ]
            else:
                tasks = [task]
            done = run_tasks(tasks, number, "layer_f%d" % l, 63)
            main = done[1] if onward else done[0]
            q, k, v, act, slope, lse, new = main[:7]
            xh = main[7] if l == 0 else x
            before = my_rows(whole_in).astype(F32) if l == 0 else h
            saved.append((before, xh, q, k, v, act, slope, lse))
            params.append((w1, w2))
            h = new
            number += 1
            if onward:
                w1, aux1 = done[0]
                (w2,) = done[2]
                x = done[1][-1]
        outputs = None if near_home else return_natural(h.astype(BF))

        g = my_rows(gb).astype(F32)
        got = [None] * layers
        for l in reversed(range(layers)):
            h_in, xh, q, k, v, act, slope, lse = saved[l]
            w1, w2 = params[l]
            dy, small = backward_compute(gb, w2, slope, q, k, v, lse, turns)
            near, far = halves(dy, w1, NT)
            m1 = dot(xh, dy, TN).astype(BF)
            m2 = dot(gb, act, TN).astype(BF)
            box = {}
            tasks = [scatter_task(near, far, h_in, g, box)]
            if l > 0:
                tasks.append(gather_task(box, rows_b, D))
            tasks.append(collect_task(m1, m2, small, C, box))
            if l == 0:
                tasks.append(return_task((DB, W1C + W2R), small.shape, box))
            if near_home and l == 0:
                tasks.append(natural_task(rows_b, D, box))
            elif outputs is None:
                tasks.append(natural_task(rows_b, D, box, h.astype(BF), "gathered"))
            if not near_home:
                box["placed"] = True
            done = run_tasks(tasks, number, "layer_b%d" % l, 63)
            number += 1
            (g,) = done[0]
            if l > 0:
                (gb,), (f, fa) = done[1:3]
                gb, f, fa = lax.optimization_barrier((gb, f, fa))
                got[l] = [permute(f[turn], give_move(turn)) for turn in range(2)]
                got[l] += [permute(fa, give_move(turn)) for turn in range(2)]
                if outputs is None:
                    outputs = done[3][0][None]
            else:
                got[l] = list(done[2])
        if near_home:
            input_grad = done[3][0][None].astype(F32)
        else:
            input_grad = return_natural(g.astype(BF)).astype(F32)

        blocks = [x for parts in got for x in parts[:2]]
        smalls = [x for parts in got for x in parts[2:]]
        (qkv_pack, qkv_new, term_q), (up_pack, up_new, term_u) = adam_inner(
            qkv_planes, up_state, blocks, smalls, columns
        )
        terms = jnp.stack(
            [term_q[:, :, 0], term_q[:, :, 1], term_u[:, :, 0], term_u[:, :, 1]], axis=1
        )
        terms = terms + over_core(terms)
        terms = terms + over_x(terms)
        out_pack, out_new = adam_outer(out_state, blocks, W1C, "adam_out")
        down_pack, down_new = adam_outer(down_state, blocks, W1C + HW, "adam_down")
        qkv_pack = jnp.transpose(qkv_pack, (0, 1, 3, 2, 4))
        qkv_new = jnp.transpose(qkv_new, (0, 2, 1, 3))
        small = jnp.stack([jnp.stack(parts[2:]) for parts in got])
        small = jnp.where(odd, small[:, ::-1], small)
        bias_q = jnp.transpose(
            small[:, :, 0, : 3 * HW].reshape(layers, 2, 3, HW), (0, 2, 1, 3)
        ).reshape(layers, 3, 2 * HW)
        bias_u = small[:, :, 0, 3 * HW : W1C].reshape(layers, 2 * F8)
        nq, nu = qkv_bias_state.shape[3], up_bias_state.shape[2]
        bias_q = lax.dynamic_slice_in_dim(bias_q, place * nq, nq, axis=2)
        bias_u = lax.dynamic_slice_in_dim(bias_u, place * nu, nu, axis=1)
        dbo = lax.dynamic_slice_in_dim(small[:, 0, 1], place * DB, DB, axis=1)
        norm_total = jnp.concatenate([terms, dbo[:, None]], axis=1)
        qkv_bias_pack, qkv_bias_new = adam_step(qkv_bias_state, bias_q, rate_vector, 0.0)
        up_bias_pack, up_bias_new = adam_step(up_bias_state, bias_u, rate_vector, 0.0)
        norm_pack, norm_new = adam_step(norm_state, norm_total, rate_vector, 0.0)
        return (
            outputs,
            input_grad,
            qkv_pack,
            qkv_new,
            out_pack,
            out_new,
            up_pack,
            up_new,
            down_pack,
            down_new,
            qkv_bias_pack,
            qkv_bias_new,
            up_bias_pack,
            up_bias_new,
            norm_pack,
            norm_new,
        )

    return local


def solution(mesh):
    return jax.shard_map(
        build(mesh),
        mesh=mesh,
        in_specs=(
            P("dp", "ctx", None),
            P("dp", "ctx", None),
            P(None, None, ("dp", "ctx"), None, "tensor"),
            P(None, None, "tensor", ("dp", "ctx")),
            P(None, None, ("dp", "ctx"), "tensor"),
            P(None, None, "tensor", ("dp", "ctx")),
            P(None, None, None, ("tensor", "dp", "ctx")),
            P(None, None, ("tensor", "dp", "ctx")),
            P(None, None, None, ("dp", "ctx")),
        ),
        out_specs=(
            P("dp", "ctx", None),
            P("dp", "ctx", None),
            P(None, None, ("dp", "ctx"), None, "tensor"),
            P(None, ("dp", "ctx"), None, "tensor"),
            P(None, None, "tensor", ("dp", "ctx")),
            P(None, "tensor", ("dp", "ctx")),
            P(None, None, ("dp", "ctx"), "tensor"),
            P(None, ("dp", "ctx"), "tensor"),
            P(None, None, "tensor", ("dp", "ctx")),
            P(None, "tensor", ("dp", "ctx")),
            P(None, None, None, ("tensor", "dp", "ctx")),
            P(None, None, ("tensor", "dp", "ctx")),
            P(None, None, ("tensor", "dp", "ctx")),
            P(None, ("tensor", "dp", "ctx")),
            P(None, None, None, ("dp", "ctx")),
            P(None, None, ("dp", "ctx")),
        ),
        check_vma=False,
    )
```

```python
import jax
import jax.numpy as jnp
from jax import lax
from jax.experimental import pallas as pl
from jax.experimental.pallas import tpu as pltpu
from jax.sharding import PartitionSpec as P

HEAD_DIM = 256
ROT = 64
STEP = 4

beta_one = 0.9
beta_two = 0.95
adam_eps = 1e-08
norm_eps = 1e-05
rate_matrix = 0.008
rate_vector = 0.2
weight_decay = 0.01

BF = jnp.bfloat16
F32 = jnp.float32
AXES = ("tensor", "dp", "ctx")
MESH = pl.DeviceIdType.MESH
ANY, VMEM = pl.ANY, pltpu.VMEM


NN = ((1,), (0,))
NT = ((1,), (1,))
TN = ((0,), (0,))


def dot(a, b, dims):
    return lax.dot_general(a, b, (dims, ((), ())), preferred_element_type=F32)


def adam_step(packed, gradient, learn_rate, decay_rate):
    moment = beta_one * packed[1] + (1.0 - beta_one) * gradient
    root_second = jnp.sqrt(
        beta_two * packed[2] * packed[2] + (1.0 - beta_two) * gradient * gradient
    )
    update = (
        learn_rate
        * (moment / (1.0 - beta_one**STEP))
        / (root_second / (1.0 - beta_two**STEP) ** 0.5 + adam_eps)
    )
    weight = packed[0] - update - learn_rate * decay_rate * packed[0]
    return (jnp.stack([gradient, moment, root_second]), weight)


def normalized(values):
    centered = values - jnp.mean(values, axis=-1, keepdims=True)
    spread = jnp.mean(centered * centered, axis=-1, keepdims=True)
    inverse = lax.rsqrt(spread + norm_eps)
    return centered * inverse, inverse


def here():
    t = lax.axis_index("tensor")
    return t // 2, t % 2, lax.axis_index("dp"), lax.axis_index("ctx")


def flip(v, k):
    out = v
    for bit in (1, 2, 4, 8):
        if k & bit:
            out = out + bit - 2 * bit * ((v // bit) % 2)
    return out


def device(th, tl, z, y):
    return {"tensor": th * 2 + tl, "dp": z, "ctx": y}


def side_of(tl, z):
    half = z // 2
    return tl + half - 2 * tl * half


def planes(side, z):
    return (
        side * z + (1 - side) * flip(z, 2),
        side * (3 - z) + (1 - side) * flip(z, 1),
    )


def fetch_goal(turn):
    th, tl, z, y = here()
    goal = 2 * tl + (z + turn) % 2
    far = goal // 2 + z // 2 - 2 * (goal // 2) * (z // 2)
    side = 1 - far if turn == 0 else far
    half = goal // 2
    core = side + half - 2 * side * half
    return th, core, goal, y


def fetch_source(turn):
    th, tl, z, y = here()
    return th, z // 2, planes(side_of(tl, z), z)[turn], y


class Task:
    def __init__(self, inputs, outs, scratch, pushes, greets, body, copies=0):
        self.inputs, self.outs, self.scratch = inputs, outs, scratch
        self.pushes, self.greets, self.body, self.copies = pushes, greets, body, copies


class Lines:
    def __init__(self, send, recv, local):
        self.send, self.recv, self.local = send, recv, local
        self.used, self.used_local, self.sent, self.closing = 0, 0, [], []

    def push(self, src, dst, to):
        copy = pltpu.make_async_remote_copy(
            src_ref=src,
            dst_ref=dst,
            send_sem=self.send.at[self.used],
            recv_sem=self.recv.at[self.used],
            device_id=device(*to),
            device_id_type=MESH,
        )
        self.used += 1
        copy.start()
        self.sent.append(copy)
        return copy

    def slots(self, n):
        at = self.used
        self.used += n
        return at

    places = slots

    def made(self, src, dst, send, recv, to):
        return pltpu.make_async_remote_copy(
            src_ref=src,
            dst_ref=dst,
            send_sem=send,
            recv_sem=recv,
            device_id=device(*to),
            device_id_type=MESH,
        )

    def copy(self, src, dst):
        copy = pltpu.make_async_copy(src, dst, self.local.at[self.used_local])
        self.used_local += 1
        copy.start()
        return copy


def run_tasks(tasks, number, name, vmem_mib):
    ins = [x for task in tasks for x, _ in task.inputs]
    in_specs = [pl.BlockSpec(memory_space=s) for task in tasks for _, s in task.inputs]
    outs = [x for task in tasks for x, _ in task.outs]
    out_specs = [pl.BlockSpec(memory_space=s) for task in tasks for _, s in task.outs]
    scratch = [x for task in tasks for x in task.scratch]
    pushes = sum(task.pushes for task in tasks)
    copies = max(1, sum(task.copies for task in tasks))
    n_in, n_out = len(ins), len(outs)

    def kernel(*refs):
        lines = Lines(*refs[-3:])
        greets = [place for task in tasks for place in task.greets()]
        barrier = pltpu.get_barrier_semaphore()
        for place in greets:
            pl.semaphore_signal(barrier, inc=1, device_id=device(*place), device_id_type=MESH)
        pl.semaphore_wait(barrier, len(greets))
        i, o, s = 0, n_in, n_in + n_out
        running = []
        for task in tasks:
            running.append(
                task.body(
                    lines,
                    refs[i : i + len(task.inputs)],
                    refs[o : o + len(task.outs)],
                    refs[s : s + len(task.scratch)],
                )
            )
            i, o, s = i + len(task.inputs), o + len(task.outs), s + len(task.scratch)
        while running:
            for body in list(running):
                try:
                    next(body)
                except StopIteration:
                    running.remove(body)
        assert lines.used == pushes, (lines.used, pushes)
        for copy in lines.sent:
            copy.wait_send()
        for close in lines.closing:
            close()

    out = pl.pallas_call(
        kernel,
        out_shape=outs,
        in_specs=in_specs,
        out_specs=out_specs,
        scratch_shapes=scratch
        + [
            pltpu.SemaphoreType.DMA((pushes,)),
            pltpu.SemaphoreType.DMA((pushes,)),
            pltpu.SemaphoreType.DMA((copies,)),
        ],
        compiler_params=pltpu.CompilerParams(
            collective_id=number, has_side_effects=True, vmem_limit_bytes=vmem_mib << 20
        ),
        name=name,
    )(*ins)
    split, at = [], 0
    for task in tasks:
        split.append(out[at : at + len(task.outs)])
        at += len(task.outs)
    return split


def shape(dims, kind):
    return jax.ShapeDtypeStruct(dims, kind)


def rows_at(start, size):
    return pl.ds(pl.multiple_of(start, size), size)


def greet_z(steps=(1, 2)):
    th, tl, z, y = here()
    return [(th, tl, flip(z, k), y) for k in steps]


def greet_x():
    th, tl, z, y = here()
    return [(1 - th, tl, z, y)]


def spread_task(natural, C, waits=(0, 1, 1, 3)):
    S, part_rows, D = natural.shape
    quarter = part_rows // 4

    def greets():
        th, tl, z, y = here()
        plane = [
            (th, flip(tl, d), z, flip(y, j)) for j in range(C) for d in range(2) if j or d
        ]
        return greet_z() + plane + greet_x()

    def body(lines, ins, outs, scratch):
        (nat,), (whole,), (held,) = ins, outs, scratch
        th, tl, z, y = here()
        t = th * 2 + tl
        own = nat.at[:, rows_at(t * quarter, quarter), :]
        for _ in range(waits[0]):
            yield
        far = [lines.push(own, held.at[z], (th, tl, flip(z, k), y)) for k in (1, 2)]
        lines.copy(own, held.at[z]).wait()
        for _ in range(waits[1]):
            yield
        far[1].wait_recv()
        piece = held.at[flip(z, 2)]
        far.append(lines.push(piece, piece, (th, tl, flip(z, 1), y)))
        yield
        far[0].wait_recv()
        far[2].wait_recv()
        spots, sent = [], []
        for j in range(C):
            for d in range(2):
                yy, cc = flip(y, j), flip(tl, d)
                goal = 2 * yy + cc
                block = held.at[goal // S, goal % S]
                if j or d:
                    spot = whole.at[rows_at(y * part_rows + t * quarter, quarter), :]
                    sent.append(lines.push(block, spot, (th, cc, z, yy)))
                else:
                    spot = whole.at[rows_at(y * part_rows + t * quarter, quarter), :]
                    cross = [lines.push(block, spot, (1 - th, tl, z, y))]
                    lines.copy(block, spot).wait()
                    sent.append(None)
                spots.append(whole.at[rows_at(yy * part_rows + (th * 2 + cc) * quarter, quarter), :])
        for _ in range(waits[2]):
            yield
        for copy, spot in zip(sent, spots):
            if copy is not None:
                copy.wait_recv()
                cross.append(lines.push(spot, spot, (1 - th, tl, z, y)))
        for _ in range(waits[3]):
            yield
        for copy in cross:
            copy.wait_recv()

    pushes = 3 + 2 * (2 * C - 1) + 1
    return Task(
        [(natural, VMEM)],
        [(shape((part_rows * C, D), natural.dtype), VMEM)],
        [pltpu.VMEM((4, S, quarter, D), natural.dtype)],
        pushes,
        greets,
        body,
        2,
    )


def fetch_task(shards, aux, C, waits=(0, 2, 0)):
    _, DB, width = shards.shape

    def greets():
        th, tl, z, y = here()
        across = [(th, tl, z, flip(y, j)) for j in range(1, C)] + [(th, 1 - tl, z, y)]
        return [f(turn) for turn in range(2) for f in (fetch_goal, fetch_source)] + across

    def body(lines, ins, outs, scratch):
        th, tl, z, y = here()
        mine = planes(side_of(tl, z), z)
        whole = outs[0]
        items = [(lambda turn: ins[0].at[turn], lambda a, n: whole.at[rows_at(a * DB, n * DB), :])]
        if aux is not None:
            gathered = outs[1]
            items.append((lambda turn: ins[1].at[turn], lambda a, n: gathered.at[pl.ds(a, n)]))
        for _ in range(waits[0]):
            yield
        first = []
        for turn in range(2):
            for source, spot in items:
                src = source(turn)
                if spot is not items[0][1]:
                    src = ins[1].at[pl.ds(turn, 1)]
                first.append(lines.push(src, spot(z * C + y, 1), fetch_goal(turn)))
        for _ in range(waits[1]):
            yield
        second = []
        n = 0
        for turn in range(2):
            second.append([])
            for _, spot in items:
                first[n].wait_recv()
                n += 1
                piece = spot(mine[turn] * C + y, 1)
                for j in range(1, C):
                    second[turn].append(lines.push(piece, piece, (th, tl, z, flip(y, j))))
            yield
        third = []
        for _ in range(waits[2]):
            yield
        for turn in range(2):
            for copy in second[turn]:
                copy.wait_recv()
            for _, spot in items:
                piece = spot(mine[turn] * C, C)
                third.append(lines.push(piece, piece, (th, 1 - tl, z, y)))
            yield
        for copy in third:
            copy.wait_recv()

    kinds = 1 if aux is None else 2
    inputs = [(shards, ANY)]
    outs = [(shape((4 * C * DB, width), shards.dtype), ANY)]
    if aux is not None:
        inputs.append((aux, ANY))
        outs.append((shape((4 * C,) + aux.shape[1:], aux.dtype), ANY))
    return Task(inputs, outs, [], kinds * (2 + 2 * (C - 1) + 2), greets, body)


def gather_task(box, rows, D):
    def greets():
        return greet_z() + greet_x()

    def body(lines, ins, outs, scratch):
        while "block" not in box:
            yield
        sent = lambda: box.update(gathered=True)
        yield from gather_steps(lines, box["block"], outs[0], sent)

    return Task([], [(shape((8 * rows, D), BF), VMEM)], [], 7, greets, body, 1)


def return_task(f_shape, aux_shape, box):
    def greets():
        return [g(turn) for turn in range(2) for g in (fetch_goal, fetch_source)]

    def body(lines, ins, outs, scratch):
        copies = []
        for turn in range(2):
            while ("turn", turn) not in box:
                yield
            f, aux = box["sums"]
            copies.append(lines.push(f.at[turn], outs[turn], fetch_source(turn)))
            copies.append(lines.push(aux, outs[2 + turn], fetch_source(turn)))
        while "placed" not in box:
            yield
        for copy in copies:
            copy.wait_recv()

    outs = [(shape(f_shape, BF), VMEM)] * 2 + [(shape(aux_shape, F32), VMEM)] * 2
    return Task([], outs, [], 4, greets, body)


def natural_task(rows, D, box, block=None, wait=None):
    def greets():
        th, tl, z, y = here()
        return greet_z((1, 2, 3)) + greet_x() + [(th, 1 - tl, z, y), (th, tl, z, 1 - y)]

    def body(lines, ins, outs, scratch):
        (out,), (stage,) = outs, scratch
        if block is None:
            while "block" not in box:
                yield
            src = box["block"]
        else:
            src = ins[0]
        th, tl, z, y = here()
        home = z == 2 * y + tl
        line = tl == z % 2
        root = jnp.logical_and(line, y == th)
        side = jnp.logical_and(line, y != th)
        leaf = tl != z % 2
        both = jnp.logical_and
        spot = lambda ref, p: ref.at[rows_at(p * rows, rows), :]
        to_home = lines.slots(1)
        at_home = lines.places(4)
        goal = 2 * y + tl
        send = lines.made(
            src, spot(stage, z), lines.send.at[to_home], lines.recv.at[at_home + z], (th, tl, goal, y)
        )
        pl.when(z != goal)(lambda: send.start())
        lines.closing.append(lambda: pl.when(z != goal)(lambda: send.wait_send()))
        base = lines.slots(12)
        own = lines.local.at[lines.used_local]
        lines.used_local += 2
        local = lines.local.at[lines.used_local - 1]
        yield
        for k in range(4):
            p = flip(z, k)
            hop = lines.made(
                spot(stage, p), spot(out, p), lines.send.at[base + k], lines.recv.at[base + k],
                (th, tl, z, 1 - y),
            )
            @pl.when(home)
            def _():
                if k == 0:
                    keep = pltpu.make_async_copy(src, spot(stage, p), own)
                    keep.start()
                    keep.wait()
                else:
                    lines.made(
                        src, spot(stage, p), lines.send.at[to_home],
                        lines.recv.at[at_home + p], (th, tl, goal, y),
                    ).wait_recv()

            @pl.when(both(home, y == th))
            def _():
                keep = pltpu.make_async_copy(spot(stage, p), spot(out, p), local)
                keep.start()
                keep.wait()

            pl.when(both(home, y != th))(lambda: hop.start())
            lines.closing.append(
                lambda hop=hop: pl.when(both(home, y != th))(lambda: hop.wait_send())
            )
            yield
        while wait is not None and wait not in box:
            yield
        for k in range(4):
            p = flip(z, k)
            hop = lines.made(
                spot(stage, p), spot(out, p), lines.send.at[base + k], lines.recv.at[base + k],
                (th, tl, z, 1 - y),
            )
            core = lines.made(
                spot(out, p), spot(out, p), lines.send.at[base + 4 + k],
                lines.recv.at[base + 4 + k], (th, 1 - tl, z, y),
            )
            cross = lines.made(
                spot(out, p), spot(out, p), lines.send.at[base + 8 + k],
                lines.recv.at[base + 8 + k], (1 - th, tl, z, y),
            )
            pl.when(both(root, jnp.logical_not(home)))(lambda: hop.wait_recv())

            @pl.when(root)
            def _():
                core.start()
                cross.start()

            lines.closing.append(
                lambda core=core: pl.when(line)(lambda: core.wait_send())
            )
            lines.closing.append(
                lambda cross=cross: pl.when(root)(lambda: cross.wait_send())
            )
            yield
        for k in range(4):
            p = flip(z, k)
            core = lines.made(
                spot(out, p), spot(out, p), lines.send.at[base + 4 + k],
                lines.recv.at[base + 4 + k], (th, 1 - tl, z, y),
            )
            cross = lines.made(
                spot(out, p), spot(out, p), lines.send.at[base + 8 + k],
                lines.recv.at[base + 8 + k], (1 - th, tl, z, y),
            )

            @pl.when(side)
            def _():
                cross.wait_recv()
                core.start()

            yield
        for k in range(4):
            p = flip(z, k)
            core = lines.made(
                spot(out, p), spot(out, p), lines.send.at[base + 4 + k],
                lines.recv.at[base + 4 + k], (th, 1 - tl, z, y),
            )
            pl.when(leaf)(lambda: core.wait_recv())
        box["placed"] = True

    return Task(
        [] if block is None else [(block, VMEM)],
        [(shape((4 * rows, D), BF), VMEM)],
        [pltpu.VMEM((4 * rows, D), BF)],
        17,
        greets,
        body,
        2,
    )


def pack_block(l, norm_columns, bias_row, out_bias, qkv, up, out, down):
    DB, HW = qkv.shape[3], qkv.shape[4] // 2
    F8 = up.shape[3] // 2
    W1C, W2R = 3 * HW + F8, HW + F8

    def kernel(n_ref, b_ref, o_ref, qkv_ref, up_ref, out_ref, down_ref, one_ref, two_ref, aux_ref):
        z = lax.axis_index("dp")
        g1, s1 = n_ref[:, 0:1], n_ref[:, 1:2]
        g2, s2 = n_ref[:, 2:3], n_ref[:, 3:4]
        for part in range(2):
            turn = (part + z) % 2
            aux_ref[turn] = jnp.zeros(aux_ref.shape[1:], F32)
            for n in range(4):
                if n < 3:
                    w = qkv_ref[0, 0, n, :, part * HW : (part + 1) * HW]
                    at = slice(n * HW, (n + 1) * HW)
                    g, s = g1, s1
                else:
                    w = up_ref[0, 0, :, part * F8 : (part + 1) * F8]
                    at = slice(3 * HW, W1C)
                    g, s = g2, s2
                w = w.astype(BF).astype(F32)
                one_ref[turn, :, at] = (g * w).astype(BF)
                aux_ref[turn, 0:1, at] = (
                    jnp.sum(s * w, axis=0, keepdims=True) + b_ref[part : part + 1, at]
                )
            aux_ref[turn, 1:2, 0:DB] = o_ref[...]
            two_ref[turn, :, 0:HW] = out_ref[0, 0, part * HW : (part + 1) * HW, :].T.astype(BF)
            two_ref[turn, :, HW:W2R] = down_ref[0, 0, part * F8 : (part + 1) * F8, :].T.astype(BF)

    whole = lambda x: pl.BlockSpec(x.shape, lambda i: (0,) * x.ndim)
    layer = lambda x: pl.BlockSpec(
        (1, 1) + x.shape[2:], lambda i: (0, l) + (0,) * (x.ndim - 2)
    )
    return pl.pallas_call(
        kernel,
        grid=(1,),
        out_shape=[
            shape((2, DB, W1C), BF),
            shape((2, DB, W2R), BF),
            shape((2, 8, W1C), F32),
        ],
        in_specs=[whole(norm_columns), whole(bias_row), whole(out_bias)]
        + [layer(x) for x in (qkv, up, out, down)],
        out_specs=[
            pl.BlockSpec((2, DB, W1C), lambda i: (0, 0, 0)),
            pl.BlockSpec((2, DB, W2R), lambda i: (0, 0, 0)),
            pl.BlockSpec((2, 8, W1C), lambda i: (0, 0, 0)),
        ],
        compiler_params=pltpu.CompilerParams(vmem_limit_bytes=40 << 20),
        cost_estimate=pl.CostEstimate(flops=0, bytes_accessed=10 << 20, transcendentals=0),
        name="pack",
    )(norm_columns, bias_row, out_bias, qkv, up, out, down)


def turned(x, turn_ref, sign):
    half = ROT // 2
    lane = lax.broadcasted_iota(jnp.int32, x.shape, 1)
    width = x.shape[1]
    other = jnp.where(lane < half, pltpu.roll(x, width - half, 1), pltpu.roll(x, half, 1))
    return x * turn_ref[0] + other * (turn_ref[1] * sign)


def causal_block(start, width):
    rows = start + lax.broadcasted_iota(jnp.int32, (width, start + width), 0)
    return lax.broadcasted_iota(jnp.int32, (width, start + width), 1) <= rows


def forward_compute(x, w1, aux, turns, raw):
    L, D = x.shape
    W1C = w1.shape[1]
    HW = turns.shape[2]
    F8 = W1C - 3 * HW
    R = 256 if L % 256 == 0 else L
    steps = L // R

    def kernel(x_ref, w_ref, aux_ref, t_ref, *outs):
        if raw:
            xh_ref, outs = outs[0], outs[1:]
        q_ref, k_ref, v_ref, act_ref, slope_ref, lse_ref, bias_ref = outs
        i = pl.program_id(0)

        @pl.when(i == 0)
        def _():
            total = aux_ref[0, 0:1, :]
            for n in range(1, aux_ref.shape[0]):
                total = total + aux_ref[n, 0:1, :]
            bias_ref[0:1, :] = total

        rows = pl.ds(pl.multiple_of(i * R, R), R)
        if raw:
            xh = normalized(x_ref[...].astype(F32))[0].astype(BF)
            xh_ref[...] = xh
        else:
            xh = x_ref[...]
        table = t_ref.at[:, rows, :]
        for n in range(3):
            at = slice(n * HW, (n + 1) * HW)
            p = dot(xh, w_ref[:, at], NN) + bias_ref[0:1, at]
            if n == 0:
                q_ref[rows, :] = (turned(p, table, 1.0) * HEAD_DIM ** (-0.5)).astype(BF)
            elif n == 1:
                k_ref[rows, :] = turned(p, table, 1.0).astype(BF)
            else:
                v_ref[rows, :] = p.astype(BF)
        piece = min(512, F8)
        for c in range(0, F8, piece):
            at = slice(3 * HW + c, 3 * HW + c + piece)
            u = dot(xh, w_ref[:, at], NN) + bias_ref[0:1, at]
            phi = 0.5 + 0.5 * lax.erf(u * 0.5**0.5)
            act_ref[rows, HW + c : HW + c + piece] = (u * phi).astype(BF)
            slope_ref[:, c : c + piece] = (
                phi + u * (jnp.exp(-0.5 * u * u) * 0.3989422804014327)
            ).astype(BF)

        @pl.when(i == steps - 1)
        def _():
            for start in range(0, L, R):
                here_rows, seen = pl.ds(start, R), pl.ds(0, start + R)
                scores = dot(q_ref[here_rows, :], k_ref[seen, :], NT)
                scores = jnp.where(causal_block(start, R), scores, -1e30)
                peak = jnp.max(scores, axis=-1, keepdims=True)
                weights = jnp.exp(scores - peak)
                total = jnp.sum(weights, axis=-1, keepdims=True)
                weights = (weights * (1.0 / total)).astype(BF)
                act_ref[here_rows, 0:HW] = dot(weights, v_ref[seen, :], NN).astype(BF)
                lse_ref[here_rows, :] = jnp.broadcast_to(peak + jnp.log(total), (R, 128))

    fixed = lambda dims: pl.BlockSpec(dims, lambda i: (0,) * len(dims))
    moving = lambda dims: pl.BlockSpec(dims, lambda i: (i, 0))
    out_shape = [
        shape((L, HW), BF),
        shape((L, HW), BF),
        shape((L, HW), BF),
        shape((L, HW + F8), BF),
        shape((L, F8), BF),
        shape((L, 128), F32),
    ]
    out_specs = [
        fixed((L, HW)),
        fixed((L, HW)),
        fixed((L, HW)),
        fixed((L, HW + F8)),
        moving((R, F8)),
        fixed((L, 128)),
    ]
    if raw:
        out_shape.insert(0, shape((L, D), BF))
        out_specs.insert(0, moving((R, D)))
    out = pl.pallas_call(
        kernel,
        grid=(steps,),
        out_shape=out_shape,
        in_specs=[moving((R, D)), fixed(w1.shape), fixed(aux.shape), fixed(turns.shape)],
        out_specs=out_specs,
        scratch_shapes=[pltpu.VMEM((8, W1C), F32)],
        compiler_params=pltpu.CompilerParams(vmem_limit_bytes=56 << 20),
        cost_estimate=pl.CostEstimate(
            flops=2 * L * D * W1C, bytes_accessed=24 << 20, transcendentals=4 << 20
        ),
        name="forward_raw" if raw else "forward",
    )(x, w1, aux, turns)
    return out if raw else [x] + list(out)


def backward_compute(gb, w2, slope, q, k, v, lse, turns):
    L, D = gb.shape
    W2R = w2.shape[1]
    HW = q.shape[1]
    F8 = W2R - HW
    W1C = 3 * HW + F8
    R = 256 if L % 256 == 0 else L
    steps = L // R
    scale = HEAD_DIM ** (-0.5)

    def kernel(
        g_ref, w_ref, s_ref, q_ref, k_ref, v_ref, l_ref, t_ref, dy_ref, small_ref, go, dq, dk, dv
    ):
        i = pl.program_id(0)

        @pl.when(i == 0)
        def _():
            small_ref[...] = jnp.zeros_like(small_ref)
            dk[...] = jnp.zeros_like(dk)
            dv[...] = jnp.zeros_like(dv)

        rows = pl.ds(pl.multiple_of(i * R, R), R)
        g = g_ref[...]
        small_ref[1:2, 0:D] += jnp.sum(g.astype(F32), axis=0, keepdims=True)
        go[rows, :] = dot(g, w_ref[:, 0:HW], NN).astype(BF)
        piece = min(512, F8)
        for c in range(0, F8, piece):
            du = dot(g, w_ref[:, HW + c : HW + c + piece], NN)
            du = (du * s_ref[:, c : c + piece].astype(F32)).astype(BF)
            dy_ref[rows, 3 * HW + c : 3 * HW + c + piece] = du
            small_ref[0:1, 3 * HW + c : 3 * HW + c + piece] += jnp.sum(
                du.astype(F32), axis=0, keepdims=True
            )

        @pl.when(i == steps - 1)
        def _():
            for start in range(0, L, R):
                here_rows, seen = pl.ds(start, R), pl.ds(0, start + R)
                qq, gg = q_ref[here_rows, :], go[here_rows, :]
                scores = dot(qq, k_ref[seen, :], NT)
                weights = jnp.where(
                    causal_block(start, R), jnp.exp(scores - l_ref[here_rows, 0:1]), 0.0
                )
                inner = dot(gg, v_ref[seen, :], NT)
                delta = jnp.sum(weights * inner, axis=-1, keepdims=True)
                ds = (weights * (inner - delta)).astype(BF)
                dq[here_rows, :] = dot(ds, k_ref[seen, :], NN) * scale
                dk[seen, :] += dot(ds, qq, TN)
                dv[seen, :] += dot(weights.astype(BF), gg, TN)
            for n, grad in enumerate((dq, dk, dv)):
                at = slice(n * HW, (n + 1) * HW)
                value = grad[...] if n == 2 else turned(grad[...], t_ref, -1.0)
                value = value.astype(BF)
                dy_ref[:, at] = value
                small_ref[0:1, at] = jnp.sum(value.astype(F32), axis=0, keepdims=True)

    fixed = lambda dims: pl.BlockSpec(dims, lambda i: (0,) * len(dims))
    moving = lambda dims: pl.BlockSpec(dims, lambda i: (i, 0))
    return pl.pallas_call(
        kernel,
        grid=(steps,),
        out_shape=[shape((L, W1C), BF), shape((8, max(W1C, D)), F32)],
        in_specs=[moving((R, D)), fixed(w2.shape), moving((R, F8))]
        + [fixed(x.shape) for x in (q, k, v, lse, turns)],
        out_specs=[fixed((L, W1C)), fixed((8, max(W1C, D)))],
        scratch_shapes=[
            pltpu.VMEM((L, HW), BF),
            pltpu.VMEM((L, HW), F32),
            pltpu.VMEM((L, HW), F32),
            pltpu.VMEM((L, HW), F32),
        ],
        compiler_params=pltpu.CompilerParams(vmem_limit_bytes=56 << 20),
        cost_estimate=pl.CostEstimate(
            flops=2 * L * D * W2R, bytes_accessed=20 << 20, transcendentals=1 << 20
        ),
        name="backward",
    )(gb, w2, slope, q, k, v, lse, turns)


def adam_values(w, m, q, gradient, learn_rate, decay_rate):
    moment = beta_one * m + (1.0 - beta_one) * gradient
    root_second = jnp.sqrt(beta_two * q * q + (1.0 - beta_two) * gradient * gradient)
    update = (
        (learn_rate / (1.0 - beta_one**STEP))
        * moment
        / (root_second * (1.0 / (1.0 - beta_two**STEP) ** 0.5) + adam_eps)
    )
    return moment, root_second, w - update - learn_rate * decay_rate * w


def adam_block(state_ref, at, gradient, pack_ref, new_ref):
    moment, root_second, weight = adam_values(
        state_ref[(0, 0) + at],
        state_ref[(1, 0) + at],
        state_ref[(2, 0) + at],
        gradient,
        rate_matrix,
        weight_decay,
    )
    pack_ref[(0, 0) + at] = gradient
    pack_ref[(1, 0) + at] = moment
    pack_ref[(2, 0) + at] = root_second
    new_ref[(0,) + at] = weight


def chosen(first, turn, values):
    even = turn == 0
    return jnp.where(
        first, jnp.where(even, values[0], values[1]), jnp.where(even, values[2], values[3])
    )


def adam_inner(qkv, up, grads, smalls, columns):
    _, layers, _, DB, wide = qkv.shape
    HW = wide // 2
    F8 = up.shape[3] // 2
    assert layers == 2

    def qkv_kernel(*refs):
        s_ref, grads, smalls, (c0, c1) = refs[0], refs[1:5], refs[5:9], refs[9:11]
        pack_ref, new_ref, term_ref = refs[11:]
        l, n = pl.program_id(0), pl.program_id(1)
        z = lax.axis_index("dp")
        first = l == 0
        col = jnp.where(first, c0[...], c1[...])
        at = pl.ds(pl.multiple_of(n * HW, HW), HW)

        @pl.when(n == 0)
        def _():
            term_ref[...] = jnp.zeros_like(term_ref)

        for part in range(2):
            turn = (part + z) % 2
            m = chosen(first, turn, [g[:, at] for g in grads]).astype(F32)
            b = chosen(first, turn, [g[0:1, at] for g in smalls])
            spot = (0, slice(None), slice(part * HW, (part + 1) * HW))
            w = s_ref[(0, 0) + spot].astype(BF).astype(F32)
            term_ref[0, :, 0:1] += jnp.sum(w * m, axis=1, keepdims=True)
            term_ref[0, :, 1:2] += jnp.sum(w * b, axis=1, keepdims=True)
            adam_block(s_ref, spot, col[:, 0:1] * m + col[:, 1:2] * b, pack_ref, new_ref)

    def up_kernel(*refs):
        s_ref, grads, smalls, (c0, c1) = refs[0], refs[1:5], refs[5:9], refs[9:11]
        pack_ref, new_ref, term_ref = refs[11:]
        l, part = pl.program_id(0), pl.program_id(1)
        turn = (part + lax.axis_index("dp")) % 2
        first = l == 0
        col = jnp.where(first, c0[...], c1[...])

        @pl.when(part == 0)
        def _():
            term_ref[...] = jnp.zeros_like(term_ref)

        piece = min(512, F8)
        for c in range(0, F8, piece):
            at = slice(3 * HW + c, 3 * HW + c + piece)
            m = chosen(first, turn, [g[:, at] for g in grads]).astype(F32)
            b = chosen(first, turn, [g[0:1, at] for g in smalls])
            spot = (slice(None), slice(c, c + piece))
            w = s_ref[(0, 0) + spot].astype(BF).astype(F32)
            term_ref[0, :, 0:1] += jnp.sum(w * m, axis=1, keepdims=True)
            term_ref[0, :, 1:2] += jnp.sum(w * b, axis=1, keepdims=True)
            adam_block(s_ref, spot, col[:, 2:3] * m + col[:, 3:4] * b, pack_ref, new_ref)

    fixed = lambda x: pl.BlockSpec(x.shape, lambda l, n: (0,) * x.ndim)
    params = pltpu.CompilerParams(vmem_limit_bytes=48 << 20)
    small = list(grads) + list(smalls) + list(columns)
    term_spec = pl.BlockSpec((1, DB, 128), lambda l, n: (l, 0, 0))
    term_shape = shape((2, DB, 128), F32)
    cost = lambda x: pl.CostEstimate(flops=0, bytes_accessed=x.size * 10, transcendentals=0)
    qkv_out = pl.pallas_call(
        qkv_kernel,
        grid=(2, 3),
        out_shape=[shape(qkv.shape, F32), shape(qkv.shape[1:], F32), term_shape],
        in_specs=[pl.BlockSpec((3, 1, 1, DB, wide), lambda l, n: (0, l, n, 0, 0))]
        + [fixed(x) for x in small],
        out_specs=[
            pl.BlockSpec((3, 1, 1, DB, wide), lambda l, n: (0, l, n, 0, 0)),
            pl.BlockSpec((1, 1, DB, wide), lambda l, n: (l, n, 0, 0)),
            term_spec,
        ],
        compiler_params=params,
        cost_estimate=cost(qkv),
        name="adam_qkv",
    )(qkv, *small)
    up_out = pl.pallas_call(
        up_kernel,
        grid=(2, 2),
        out_shape=[shape(up.shape, F32), shape(up.shape[1:], F32), term_shape],
        in_specs=[pl.BlockSpec((3, 1, DB, F8), lambda l, n: (0, l, 0, n))]
        + [fixed(x) for x in small],
        out_specs=[
            pl.BlockSpec((3, 1, DB, F8), lambda l, n: (0, l, 0, n)),
            pl.BlockSpec((1, DB, F8), lambda l, n: (l, 0, n)),
            term_spec,
        ],
        compiler_params=params,
        cost_estimate=cost(up),
        name="adam_up",
    )(up, *small)
    return qkv_out, up_out


def adam_outer(state, grads, begin, name):
    _, layers, rows, DB = state.shape
    half = rows // 2

    def kernel(s_ref, *refs):
        pack_ref, new_ref = refs[4:]
        l, part = pl.program_id(0), pl.program_id(1)
        turn = (part + lax.axis_index("dp")) % 2
        piece = min(256, half)
        for c in range(0, half, piece):
            at = slice(begin + c, begin + c + piece)
            m = chosen(l == 0, turn, [g[:, at] for g in refs[:4]]).astype(F32).T
            adam_block(s_ref, (slice(c, c + piece), slice(None)), m, pack_ref, new_ref)

    fixed = lambda x: pl.BlockSpec(x.shape, lambda l, n: (0,) * x.ndim)
    return pl.pallas_call(
        kernel,
        grid=(2, 2),
        out_shape=[shape(state.shape, F32), shape(state.shape[1:], F32)],
        in_specs=[pl.BlockSpec((3, 1, half, DB), lambda l, n: (0, l, n, 0))]
        + [fixed(x) for x in grads],
        out_specs=[
            pl.BlockSpec((3, 1, half, DB), lambda l, n: (0, l, n, 0)),
            pl.BlockSpec((1, half, DB), lambda l, n: (l, n, 0)),
        ],
        compiler_params=pltpu.CompilerParams(vmem_limit_bytes=48 << 20),
        cost_estimate=pl.CostEstimate(
            flops=0, bytes_accessed=state.size * 10, transcendentals=0
        ),
        name=name,
    )(state, *grads)


def piece_dot(lhs, w_ref, write):
    D = w_ref.shape[0]
    tile = min(512, D)

    def some(c, carry):
        at = pl.ds(pl.multiple_of(c * tile, tile), tile)
        write(at, dot(lhs, w_ref[at, :], NT))
        return carry

    lax.fori_loop(0, D // tile, some, 0)


def scatter_steps(lines, lhs_of, w_ref, far, came, ready, last, total):
    th, tl, z, y = here()
    rows = came.shape[1]

    def pair(half, base):
        high = z // 2 if base == 0 else 1 - z // 2
        return lhs_of(half * 4 + high * 2)

    cross, along = {}, {}
    for p, base in enumerate((2, 0)):

        def keep(at, value, p=p):
            far[p, :, at] = value.astype(BF)

        piece_dot(pair(1 - th, base), w_ref, keep)
        for k in (base + 1, base):
            piece = far.at[p, rows_at((flip(z, k) % 2) * rows, rows), :]
            cross[k] = lines.push(piece, came.at[k], (1 - th, tl, z, y))
    yield
    for base in (2, 0):

        def keep(at, value, base=base):
            for r in range(2):
                ready[base + (r + z) % 2, :, at] = value[r * rows : (r + 1) * rows].astype(BF)

        piece_dot(pair(th, base), w_ref, keep)
    for k in (3, 2, 1):
        cross[k].wait_recv()
        value = ready[k].astype(F32) + came[k].astype(F32)
        if k == 2:
            along[3].wait_recv()
            value = value + last[2].astype(F32)
        ready[k] = value.astype(BF)
        goal = flip(z, 2) if k == 2 else flip(z, 1)
        along[k] = lines.push(ready.at[k], last.at[k - 1], (th, tl, goal, y))
        yield
    cross[0].wait_recv()
    yield
    value = ready[0].astype(F32) + came[0].astype(F32)
    for k in (1, 2):
        along[k].wait_recv()
        value = value + last[k - 1].astype(F32)
    total[...] = value


def gather_steps(lines, src, whole, sent=lambda: None):
    th, tl, z, y = here()
    rows = src.shape[0]
    spot = lambda a, b: whole.at[rows_at((a * 4 + b) * rows, rows), :]
    cross = [lines.push(src, spot(th, z), (1 - th, tl, z, y))]
    near = {k: lines.push(src, spot(th, z), (th, tl, flip(z, k), y)) for k in (1, 2)}
    lines.copy(src, spot(th, z)).wait()
    yield
    for k in (1, 2, 3):
        near[k].wait_recv()
        piece = spot(th, flip(z, k))
        if k == 2:
            near[3] = lines.push(piece, piece, (th, tl, flip(z, 1), y))
        cross.append(lines.push(piece, piece, (1 - th, tl, z, y)))
        yield
    sent()
    yield
    for copy in cross:
        copy.wait_recv()


def forward_task(x, w1, w2, aux, turns, h, bias_out, onward):
    L, D = x.shape
    raw = h is None
    W1C, W2R = w1.shape[1], w2.shape[1]
    HW = turns.shape[2]
    F8 = W1C - 3 * HW
    R = 256 if L % 256 == 0 else L
    steps = L // R
    rows_b = L // 8

    def greets():
        return greet_z() + greet_x()

    def body(lines, ins, outs, scratch):
        x_ref, w1_ref, w2_ref, aux_ref, t_ref, bo_ref = ins[:6]
        q_ref, k_ref, v_ref, act_ref, slope_ref, lse_ref, new_ref = outs[:7]
        w1_in, w2_in, bias_ref, far, came, ready, last, block = scratch
        th, tl, z, y = here()
        load1 = lines.copy(w1_ref, w1_in)
        load2 = lines.copy(w2_ref, w2_in)
        total = aux_ref[0, 0:1, :]
        for n in range(1, aux_ref.shape[0]):
            total = total + aux_ref[n, 0:1, :]
        bias_ref[0:1, :] = total
        load1.wait()

        def some(i, carry):
            rows = pl.ds(pl.multiple_of(i * R, R), R)
            if raw:
                xh = normalized(x_ref[rows, :].astype(F32))[0].astype(BF)
                outs[7][rows, :] = xh
            else:
                xh = x_ref[rows, :]
            table = t_ref.at[:, rows, :]
            for n in range(3):
                at = slice(n * HW, (n + 1) * HW)
                p = dot(xh, w1_in[:, at], NN) + bias_ref[0:1, at]
                if n == 0:
                    q_ref[rows, :] = (turned(p, table, 1.0) * HEAD_DIM ** (-0.5)).astype(BF)
                elif n == 1:
                    k_ref[rows, :] = turned(p, table, 1.0).astype(BF)
                else:
                    v_ref[rows, :] = p.astype(BF)
            piece = min(512, F8)
            for c in range(0, F8, piece):
                at = slice(3 * HW + c, 3 * HW + c + piece)
                u = dot(xh, w1_in[:, at], NN) + bias_ref[0:1, at]
                phi = 0.5 + 0.5 * lax.erf(u * 0.5**0.5)
                act_ref[rows, HW + c : HW + c + piece] = (u * phi).astype(BF)
                slope_ref[rows, c : c + piece] = (
                    phi + u * (jnp.exp(-0.5 * u * u) * 0.3989422804014327)
                ).astype(BF)
            return carry

        lax.fori_loop(0, steps, some, 0)
        for start in range(0, L, R):
            here_rows, seen = pl.ds(start, R), pl.ds(0, start + R)
            scores = dot(q_ref[here_rows, :], k_ref[seen, :], NT)
            scores = jnp.where(causal_block(start, R), scores, -1e30)
            peak = jnp.max(scores, axis=-1, keepdims=True)
            weights = jnp.exp(scores - peak)
            total = jnp.sum(weights, axis=-1, keepdims=True)
            weights = (weights * (1.0 / total)).astype(BF)
            act_ref[here_rows, 0:HW] = dot(weights, v_ref[seen, :], NN).astype(BF)
            lse_ref[here_rows, :] = jnp.broadcast_to(peak + jnp.log(total), (R, 128))
        load2.wait()
        yield
        yield from scatter_steps(
            lines,
            lambda n: act_ref[pl.ds(pl.multiple_of(n * rows_b, 2 * rows_b), 2 * rows_b), :],
            w2_in,
            far,
            came,
            ready,
            last,
            new_ref,
        )
        if raw:
            before = x_ref[rows_at((th * 4 + z) * rows_b, rows_b), :].astype(F32)
        else:
            before = ins[6][...]
        new = before + new_ref[...] + bo_ref[...]
        new_ref[...] = new
        if onward:
            block[...] = normalized(new)[0].astype(BF)
            yield from gather_steps(lines, block, outs[-1])

    inputs = [(x, VMEM), (w1, ANY), (w2, ANY), (aux, VMEM), (turns, VMEM), (bias_out, VMEM)]
    outs = [
        (shape((L, HW), BF), VMEM),
        (shape((L, HW), BF), VMEM),
        (shape((L, HW), BF), VMEM),
        (shape((L, HW + F8), BF), VMEM),
        (shape((L, F8), BF), VMEM),
        (shape((L, 128), F32), VMEM),
        (shape((rows_b, D), F32), VMEM),
    ]
    if raw:
        outs.append((shape((L, D), BF), VMEM))
    else:
        inputs.append((h, VMEM))
    if onward:
        outs.append((shape((L, D), BF), VMEM))
    return Task(
        inputs,
        outs,
        [
            pltpu.VMEM(w1.shape, BF),
            pltpu.VMEM(w2.shape, BF),
            pltpu.VMEM((8, W1C), F32),
            pltpu.VMEM((2, 2 * rows_b, D), BF),
            pltpu.VMEM((4, rows_b, D), BF),
            pltpu.VMEM((4, rows_b, D), BF),
            pltpu.VMEM((3, rows_b, D), BF),
            pltpu.VMEM((rows_b, D), BF),
        ],
        14 if onward else 7,
        greets,
        body,
        3 if onward else 2,
    )


def slope_task(dy, w1, act, gb, h, g, box):
    L, W1C = dy.shape
    D = gb.shape[1]
    rows = L // 8

    def greets():
        return greet_z() + greet_x()

    def body(lines, ins, outs, scratch):
        dy_ref, w1_ref, act_ref, gb_ref, h_ref, g_ref = ins
        (out,) = outs
        w1_in, far, came, ready, last, block = scratch
        load = lines.copy(w1_ref, w1_in)
        box["factors"] = (dy_ref, act_ref, gb_ref)
        load.wait()
        yield from scatter_steps(
            lines,
            lambda n: dy_ref[pl.ds(pl.multiple_of(n * rows, 2 * rows), 2 * rows), :],
            w1_in,
            far,
            came,
            ready,
            last,
            out,
        )
        total = out[...]
        xn, inverse = normalized(h_ref[...])
        value = g_ref[...] + inverse * (
            total
            - jnp.mean(total, axis=-1, keepdims=True)
            - xn * jnp.mean(total * xn, axis=-1, keepdims=True)
        )
        out[...] = value
        block[...] = value.astype(BF)
        box["block"] = block

    return Task(
        [(dy, VMEM), (w1, ANY), (act, VMEM), (gb, VMEM), (h, VMEM), (g, VMEM)],
        [(shape((rows, D), F32), VMEM)],
        [
            pltpu.VMEM(w1.shape, BF),
            pltpu.VMEM((2, 2 * rows, D), BF),
            pltpu.VMEM((4, rows, D), BF),
            pltpu.VMEM((4, rows, D), BF),
            pltpu.VMEM((3, rows, D), BF),
            pltpu.VMEM((rows, D), BF),
        ],
        7,
        greets,
        body,
        1,
    )


def collect_task(xh, wide, deep, aux, C, box):
    L, D = xh.shape
    DB = D // (4 * C)
    CB = C * DB
    both = wide + deep
    tall = aux.shape
    step = min(256, CB)

    def greets():
        th, tl, z, y = here()
        return [(th, 1 - tl, z, y)] + [(th, tl, z, flip(y, j)) for j in range(1, C)]

    def body(lines, ins, outs, scratch):
        xh_ref, aux_ref = ins
        f_ref, fa_ref = outs
        send, came, came_y, columns, small_own, small_came, small_y = scratch
        th, tl, z, y = here()
        side = side_of(tl, z)
        mine, other = planes(side, z), planes(1 - side, z)
        over = (th, 1 - tl, z, y)
        sites = [other[0], mine[0], other[1], mine[1]]

        def load(n):
            return lines.copy(xh_ref.at[:, rows_at(sites[n] * CB, CB)], columns.at[n % 2])

        loads = [load(0)]
        sent_small = lines.push(aux_ref, small_came, over)
        while "factors" not in box:
            yield
        dy_ref, act_ref, gb_ref = box["factors"]
        sent, across = [], []
        for n in range(4):
            turn, own = n // 2, n % 2 == 1
            if n < 3:
                loads.append(load(n + 1))
            loads[n].wait()
            if own:
                sent[turn].wait_recv()
            target = came if own else send

            def some(i, carry, n=n, turn=turn, own=own, target=target):
                at = pl.ds(pl.multiple_of(i * step, step), step)
                begin = pl.ds(pl.multiple_of(sites[n] * CB + i * step, step), step)
                one = dot(columns[n % 2, :, at], dy_ref[...], TN)
                if own:
                    one = one + came[turn, at, 0:wide].astype(F32)
                target[turn, at, 0:wide] = one.astype(BF)
                two = dot(gb_ref[:, begin], act_ref[...], TN)
                if own:
                    two = two + came[turn, at, wide:].astype(F32)
                target[turn, at, wide:] = two.astype(BF)
                return carry

            lax.fori_loop(0, CB // step, some, 0)
            if not own:
                sent.append(lines.push(send.at[turn], came.at[turn], over))
            else:
                for j in range(1, C):
                    at = rows_at(flip(y, j) * DB, DB)
                    across.append(
                        (
                            turn,
                            j,
                            lines.push(
                                came.at[turn, at, :],
                                came_y.at[j - 1, turn],
                                (th, tl, z, flip(y, j)),
                            ),
                        )
                    )
            if n == 1:
                sent_small.wait_recv()
                small_own[...] = aux_ref[...] + small_came[...]
                small = [
                    lines.push(small_own, small_y.at[j - 1], (th, tl, z, flip(y, j)))
                    for j in range(1, C)
                ]
            yield
        while "block" not in box:
            yield
        for copy in small:
            copy.wait_recv()
        total = small_own[...]
        for j in range(1, C):
            total = total + small_y[j - 1]
        fa_ref[...] = total
        box["sums"] = outs
        yield
        yield
        some_rows = min(64, DB)
        for turn in range(2):
            for t, j, copy in across:
                if t == turn:
                    copy.wait_recv()

            def add(i, carry, turn=turn):
                at = pl.ds(pl.multiple_of(i * some_rows, some_rows), some_rows)
                from_at = pl.ds(
                    pl.multiple_of(y * DB + i * some_rows, some_rows), some_rows
                )
                value = came[turn, from_at, :].astype(F32)
                for j in range(1, C):
                    value = value + came_y[j - 1, turn, at, :].astype(F32)
                f_ref[turn, at, :] = value.astype(BF)
                return carry

            lax.fori_loop(0, DB // some_rows, add, 0)
            box["turn", turn] = True
            yield

    return Task(
        [(xh, ANY), (aux, VMEM)],
        [(shape((2, DB, both), BF), VMEM), (shape(tall, F32), VMEM)],
        [
            pltpu.VMEM((2, CB, both), BF),
            pltpu.VMEM((2, CB, both), BF),
            pltpu.VMEM((C - 1, 2, DB, both), BF),
            pltpu.VMEM((2, L, CB), BF),
            pltpu.VMEM(tall, F32),
            pltpu.VMEM(tall, F32),
            pltpu.VMEM((C - 1,) + tall, F32),
        ],
        3 + (C - 1) * 3,
        greets,
        body,
        4,
    )


def build(mesh):
    tensor, Z, C = (mesh.shape[name] for name in AXES)
    assert tensor == 4 and Z == 4

    def flat(th, tl, z, y):
        return ((th * 2 + tl) * Z + z) * C + y

    def permute(x, move):
        pairs = []
        for th in range(2):
            for tl in range(2):
                for z in range(Z):
                    for y in range(C):
                        target = move(th, tl, z, y)
                        if target is not None:
                            pairs.append((flat(th, tl, z, y), flat(*target)))
        return lax.ppermute(x, AXES, pairs)

    def give_move(turn):
        def move(th, tl, z, y):
            side = tl ^ (z // 2)
            return (th, z // 2, z ^ (2 - 2 * side if turn == 0 else 1 + 2 * side), y)

        return move

    def over_x(x):
        return permute(x, lambda th, tl, z, y: (1 - th, tl, z, y))

    def over_core(x):
        return permute(x, lambda th, tl, z, y: (th, 1 - tl, z, y))

    def local(
        inputs,
        cotangent,
        qkv_state,
        out_state,
        up_state,
        down_state,
        qkv_bias_state,
        up_bias_state,
        norm_state,
    ):
        layers = qkv_state.shape[1]
        S, part_rows, D = inputs.shape
        L = part_rows * C
        rows_b = L // 8
        DB = D // (Z * C)
        F8 = up_state.shape[3] // 2
        HW = qkv_state.shape[4] // 2
        W1C, W2R = 3 * HW + F8, HW + F8
        th, tl, z, y = here()
        odd = (z % 2) == 1
        place = z * C + y
        qkv_planes = jnp.transpose(qkv_state, (0, 1, 3, 2, 4))

        norm_rows = norm_state[0].astype(BF).astype(F32)
        columns = [jnp.pad(norm_rows[l].T, ((0, 0), (0, 3))) for l in range(layers)]

        def pack(l):
            rows = norm_rows[l]
            bq = qkv_bias_state[0, l].astype(BF).astype(F32)
            bu = up_bias_state[0, l].astype(BF).astype(F32)
            n = bq.shape[1]
            vq = lax.dynamic_update_slice(jnp.zeros((3, 2 * HW), F32), bq, (0, place * n))
            vu = lax.dynamic_update_slice(jnp.zeros((2 * F8,), F32), bu, (place * bu.shape[0],))
            vq = jnp.transpose(vq.reshape(3, 2, HW), (1, 0, 2)).reshape(2, 3 * HW)
            row = jnp.concatenate([vq, vu.reshape(2, F8)], axis=1)
            return pack_block(
                l, columns[l], row, rows[4:5], qkv_planes, up_state, out_state, down_state
            )

        def my_rows(whole):
            return lax.dynamic_slice_in_dim(whole, (th * 4 + z) * rows_b, rows_b, axis=0)

        near_home = C == 2 and S == 1

        def return_natural(block):
            every = lax.all_gather(block, AXES, axis=0)
            every = every.reshape(2, 2, Z, C, rows_b, D)
            every = jnp.transpose(every, (3, 1, 0, 2, 4, 5)).reshape(2 * C, L, D)
            return lax.dynamic_slice(every, (z * S, y * part_rows, 0), (S, part_rows, D))

        positions = jnp.arange(L, dtype=F32)
        frequency = 10000.0 ** (-2.0 * jnp.arange(ROT // 2, dtype=F32) / ROT)
        angles = positions[:, None] * frequency[None, :]
        cosine, sine = jnp.cos(angles), jnp.sin(angles)
        rest = HEAD_DIM - ROT
        turns = jnp.stack(
            [
                jnp.concatenate([cosine, cosine, jnp.ones((L, rest), F32)], axis=1),
                jnp.concatenate([-sine, sine, jnp.zeros((L, rest), F32)], axis=1),
            ]
        )

        packs = [pack(l) for l in range(layers)]
        one, two, aux = packs[0]
        (whole_in,), (w1, aux1), (w2,) = run_tasks(
            [
                spread_task(inputs, C, (0, 1, 1, 3)),
                fetch_task(one, aux, C, (1, 2, 1)),
                fetch_task(two, None, C, (1, 4, 1)),
            ],
            0,
            "start",
            48,
        )
        params, saved = [], []
        x, h = whole_in, None
        number = 1
        for l in range(layers):
            bias_out = aux1[:, 1, :DB].reshape(1, D)
            onward = l + 1 < layers
            task = forward_task(x, w1, w2, aux1, turns, h, bias_out, onward)
            if onward:
                one, two, aux = packs[l + 1]
                tasks = [
                    fetch_task(one, aux, C, (0, 3, 2)),
                    fetch_task(two, None, C, (0, 7, 1)),
                    task,
                ]
            else:
                tasks = [spread_task(cotangent, C, (0, 1, 3, 2)), task]
            done = run_tasks(tasks, number, "layer_f%d" % l, 63)
            q, k, v, act, slope, lse, new = done[-1][:7]
            xh = done[-1][7] if l == 0 else x
            before = my_rows(whole_in).astype(F32) if l == 0 else h
            saved.append((before, xh, q, k, v, act, slope, lse))
            params.append((w1, w2))
            h = new
            number += 1
            if onward:
                w1, aux1 = done[0]
                (w2,) = done[1]
                x = done[2][-1]
            else:
                (gb,) = done[0]
        outputs = None if near_home else return_natural(h.astype(BF))

        g = my_rows(gb).astype(F32)
        got = [None] * layers
        for l in reversed(range(layers)):
            h_in, xh, q, k, v, act, slope, lse = saved[l]
            w1, w2 = params[l]
            dy, small = backward_compute(gb, w2, slope, q, k, v, lse, turns)
            box = {}
            tasks = [slope_task(dy, w1, act, gb, h_in, g, box)]
            if l > 0:
                tasks.append(gather_task(box, rows_b, D))
            tasks.append(collect_task(xh, W1C, W2R, small, C, box))
            if l == 0:
                tasks.append(return_task((DB, W1C + W2R), small.shape, box))
            if near_home and l == 0:
                tasks.append(natural_task(rows_b, D, box))
            elif outputs is None:
                tasks.append(natural_task(rows_b, D, box, h.astype(BF), "gathered"))
            if not near_home:
                box["placed"] = True
            done = run_tasks(tasks, number, "layer_b%d" % l, 63)
            number += 1
            (g,) = done[0]
            if l > 0:
                (gb,), (f, fa) = done[1:3]
                gb, f, fa = lax.optimization_barrier((gb, f, fa))
                got[l] = [permute(f[turn], give_move(turn)) for turn in range(2)]
                got[l] += [permute(fa, give_move(turn)) for turn in range(2)]
                if outputs is None:
                    outputs = done[3][0][None]
            else:
                got[l] = list(done[2])
        if near_home:
            input_grad = done[3][0][None].astype(F32)
        else:
            input_grad = return_natural(g.astype(BF)).astype(F32)

        blocks = [x for parts in got for x in parts[:2]]
        smalls = [x for parts in got for x in parts[2:]]
        (qkv_pack, qkv_new, term_q), (up_pack, up_new, term_u) = adam_inner(
            qkv_planes, up_state, blocks, smalls, columns
        )
        terms = jnp.stack(
            [term_q[:, :, 0], term_q[:, :, 1], term_u[:, :, 0], term_u[:, :, 1]], axis=1
        )
        terms = terms + over_core(terms)
        terms = terms + over_x(terms)
        out_pack, out_new = adam_outer(out_state, blocks, W1C, "adam_out")
        down_pack, down_new = adam_outer(down_state, blocks, W1C + HW, "adam_down")
        qkv_pack = jnp.transpose(qkv_pack, (0, 1, 3, 2, 4))
        qkv_new = jnp.transpose(qkv_new, (0, 2, 1, 3))
        small = jnp.stack([jnp.stack(parts[2:]) for parts in got])
        small = jnp.where(odd, small[:, ::-1], small)
        bias_q = jnp.transpose(
            small[:, :, 0, : 3 * HW].reshape(layers, 2, 3, HW), (0, 2, 1, 3)
        ).reshape(layers, 3, 2 * HW)
        bias_u = small[:, :, 0, 3 * HW : W1C].reshape(layers, 2 * F8)
        nq, nu = qkv_bias_state.shape[3], up_bias_state.shape[2]
        bias_q = lax.dynamic_slice_in_dim(bias_q, place * nq, nq, axis=2)
        bias_u = lax.dynamic_slice_in_dim(bias_u, place * nu, nu, axis=1)
        dbo = lax.dynamic_slice_in_dim(small[:, 0, 1], place * DB, DB, axis=1)
        norm_total = jnp.concatenate([terms, dbo[:, None]], axis=1)
        qkv_bias_pack, qkv_bias_new = adam_step(qkv_bias_state, bias_q, rate_vector, 0.0)
        up_bias_pack, up_bias_new = adam_step(up_bias_state, bias_u, rate_vector, 0.0)
        norm_pack, norm_new = adam_step(norm_state, norm_total, rate_vector, 0.0)
        return (
            outputs,
            input_grad,
            qkv_pack,
            qkv_new,
            out_pack,
            out_new,
            up_pack,
            up_new,
            down_pack,
            down_new,
            qkv_bias_pack,
            qkv_bias_new,
            up_bias_pack,
            up_bias_new,
            norm_pack,
            norm_new,
        )

    return local


def solution(mesh):
    return jax.shard_map(
        build(mesh),
        mesh=mesh,
        in_specs=(
            P("dp", "ctx", None),
            P("dp", "ctx", None),
            P(None, None, ("dp", "ctx"), None, "tensor"),
            P(None, None, "tensor", ("dp", "ctx")),
            P(None, None, ("dp", "ctx"), "tensor"),
            P(None, None, "tensor", ("dp", "ctx")),
            P(None, None, None, ("tensor", "dp", "ctx")),
            P(None, None, ("tensor", "dp", "ctx")),
            P(None, None, None, ("dp", "ctx")),
        ),
        out_specs=(
            P("dp", "ctx", None),
            P("dp", "ctx", None),
            P(None, None, ("dp", "ctx"), None, "tensor"),
            P(None, ("dp", "ctx"), None, "tensor"),
            P(None, None, "tensor", ("dp", "ctx")),
            P(None, "tensor", ("dp", "ctx")),
            P(None, None, ("dp", "ctx"), "tensor"),
            P(None, ("dp", "ctx"), "tensor"),
            P(None, None, "tensor", ("dp", "ctx")),
            P(None, "tensor", ("dp", "ctx")),
            P(None, None, None, ("tensor", "dp", "ctx")),
            P(None, None, ("tensor", "dp", "ctx")),
            P(None, None, ("tensor", "dp", "ctx")),
            P(None, ("tensor", "dp", "ctx")),
            P(None, None, None, ("dp", "ctx")),
            P(None, None, ("dp", "ctx")),
        ),
        check_vma=False,
    )
```

```python
import jax
import jax.numpy as jnp
from jax import lax
from jax.experimental import pallas as pl
from jax.experimental.pallas import tpu as pltpu
from jax.sharding import PartitionSpec as P

HEAD_DIM = 256
ROT = 64
STEP = 4

beta_one = 0.9
beta_two = 0.95
adam_eps = 1e-08
norm_eps = 1e-05
rate_matrix = 0.008
rate_vector = 0.2
weight_decay = 0.01

BF = jnp.bfloat16
F32 = jnp.float32
AXES = ("tensor", "dp", "ctx")
MESH = pl.DeviceIdType.MESH
ANY, VMEM = pl.ANY, pltpu.VMEM


NN = ((1,), (0,))
NT = ((1,), (1,))
TN = ((0,), (0,))


def dot(a, b, dims):
    return lax.dot_general(a, b, (dims, ((), ())), preferred_element_type=F32)


def adam_step(packed, gradient, learn_rate, decay_rate):
    moment = beta_one * packed[1] + (1.0 - beta_one) * gradient
    root_second = jnp.sqrt(
        beta_two * packed[2] * packed[2] + (1.0 - beta_two) * gradient * gradient
    )
    update = (
        learn_rate
        * (moment / (1.0 - beta_one**STEP))
        / (root_second / (1.0 - beta_two**STEP) ** 0.5 + adam_eps)
    )
    weight = packed[0] - update - learn_rate * decay_rate * packed[0]
    return (jnp.stack([gradient, moment, root_second]), weight)


def normalized(values):
    centered = values - jnp.mean(values, axis=-1, keepdims=True)
    spread = jnp.mean(centered * centered, axis=-1, keepdims=True)
    inverse = lax.rsqrt(spread + norm_eps)
    return centered * inverse, inverse


def here():
    t = lax.axis_index("tensor")
    return t // 2, t % 2, lax.axis_index("dp"), lax.axis_index("ctx")


def flip(v, k):
    out = v
    for bit in (1, 2, 4, 8):
        if k & bit:
            out = out + bit - 2 * bit * ((v // bit) % 2)
    return out


def device(th, tl, z, y):
    return {"tensor": th * 2 + tl, "dp": z, "ctx": y}


def side_of(tl, z):
    half = z // 2
    return tl + half - 2 * tl * half


def planes(side, z):
    return (
        side * z + (1 - side) * flip(z, 2),
        side * (3 - z) + (1 - side) * flip(z, 1),
    )


def fetch_goal(turn):
    th, tl, z, y = here()
    goal = 2 * tl + (z + turn) % 2
    far = goal // 2 + z // 2 - 2 * (goal // 2) * (z // 2)
    side = 1 - far if turn == 0 else far
    half = goal // 2
    core = side + half - 2 * side * half
    return th, core, goal, y


def fetch_source(turn):
    th, tl, z, y = here()
    return th, z // 2, planes(side_of(tl, z), z)[turn], y


class Task:
    def __init__(self, inputs, outs, scratch, pushes, greets, body, copies=0):
        self.inputs, self.outs, self.scratch = inputs, outs, scratch
        self.pushes, self.greets, self.body, self.copies = pushes, greets, body, copies


class Lines:
    def __init__(self, send, recv, local):
        self.send, self.recv, self.local = send, recv, local
        self.used, self.used_local, self.sent, self.closing = 0, 0, [], []

    def push(self, src, dst, to):
        copy = pltpu.make_async_remote_copy(
            src_ref=src,
            dst_ref=dst,
            send_sem=self.send.at[self.used],
            recv_sem=self.recv.at[self.used],
            device_id=device(*to),
            device_id_type=MESH,
        )
        self.used += 1
        copy.start()
        self.sent.append(copy)
        return copy

    def slots(self, n):
        at = self.used
        self.used += n
        return at

    places = slots

    def made(self, src, dst, send, recv, to):
        return pltpu.make_async_remote_copy(
            src_ref=src,
            dst_ref=dst,
            send_sem=send,
            recv_sem=recv,
            device_id=device(*to),
            device_id_type=MESH,
        )

    def copy(self, src, dst):
        copy = pltpu.make_async_copy(src, dst, self.local.at[self.used_local])
        self.used_local += 1
        copy.start()
        return copy


def run_tasks(tasks, number, name, vmem_mib):
    ins = [x for task in tasks for x, _ in task.inputs]
    in_specs = [pl.BlockSpec(memory_space=s) for task in tasks for _, s in task.inputs]
    outs = [x for task in tasks for x, _ in task.outs]
    out_specs = [pl.BlockSpec(memory_space=s) for task in tasks for _, s in task.outs]
    scratch = [x for task in tasks for x in task.scratch]
    pushes = sum(task.pushes for task in tasks)
    copies = max(1, sum(task.copies for task in tasks))
    n_in, n_out = len(ins), len(outs)

    def kernel(*refs):
        lines = Lines(*refs[-3:])
        greets = [place for task in tasks for place in task.greets()]
        barrier = pltpu.get_barrier_semaphore()
        for place in greets:
            pl.semaphore_signal(barrier, inc=1, device_id=device(*place), device_id_type=MESH)
        pl.semaphore_wait(barrier, len(greets))
        i, o, s = 0, n_in, n_in + n_out
        running = []
        for task in tasks:
            running.append(
                task.body(
                    lines,
                    refs[i : i + len(task.inputs)],
                    refs[o : o + len(task.outs)],
                    refs[s : s + len(task.scratch)],
                )
            )
            i, o, s = i + len(task.inputs), o + len(task.outs), s + len(task.scratch)
        while running:
            for body in list(running):
                try:
                    next(body)
                except StopIteration:
                    running.remove(body)
        assert lines.used == pushes, (lines.used, pushes)
        for copy in lines.sent:
            copy.wait_send()
        for close in lines.closing:
            close()

    out = pl.pallas_call(
        kernel,
        out_shape=outs,
        in_specs=in_specs,
        out_specs=out_specs,
        scratch_shapes=scratch
        + [
            pltpu.SemaphoreType.DMA((pushes,)),
            pltpu.SemaphoreType.DMA((pushes,)),
            pltpu.SemaphoreType.DMA((copies,)),
        ],
        compiler_params=pltpu.CompilerParams(
            collective_id=number, has_side_effects=True, vmem_limit_bytes=vmem_mib << 20
        ),
        name=name,
    )(*ins)
    split, at = [], 0
    for task in tasks:
        split.append(out[at : at + len(task.outs)])
        at += len(task.outs)
    return split


def shape(dims, kind):
    return jax.ShapeDtypeStruct(dims, kind)


def rows_at(start, size):
    return pl.ds(pl.multiple_of(start, size), size)


def greet_z(steps=(1, 2)):
    th, tl, z, y = here()
    return [(th, tl, flip(z, k), y) for k in steps]


def greet_x():
    th, tl, z, y = here()
    return [(1 - th, tl, z, y)]


def spread_task(natural, C, waits=(0, 1, 1, 3)):
    S, part_rows, D = natural.shape
    quarter = part_rows // 4

    def greets():
        th, tl, z, y = here()
        plane = [
            (th, flip(tl, d), z, flip(y, j)) for j in range(C) for d in range(2) if j or d
        ]
        return greet_z() + plane + greet_x()

    def body(lines, ins, outs, scratch):
        (nat,), (whole,), (held,) = ins, outs, scratch
        th, tl, z, y = here()
        t = th * 2 + tl
        own = nat.at[:, rows_at(t * quarter, quarter), :]
        for _ in range(waits[0]):
            yield
        far = [lines.push(own, held.at[z], (th, tl, flip(z, k), y)) for k in (1, 2)]
        lines.copy(own, held.at[z]).wait()
        for _ in range(waits[1]):
            yield
        far[1].wait_recv()
        piece = held.at[flip(z, 2)]
        far.append(lines.push(piece, piece, (th, tl, flip(z, 1), y)))
        yield
        far[0].wait_recv()
        far[2].wait_recv()
        spots, sent = [], []
        for j in range(C):
            for d in range(2):
                yy, cc = flip(y, j), flip(tl, d)
                goal = 2 * yy + cc
                block = held.at[goal // S, goal % S]
                if j or d:
                    spot = whole.at[rows_at(y * part_rows + t * quarter, quarter), :]
                    sent.append(lines.push(block, spot, (th, cc, z, yy)))
                else:
                    spot = whole.at[rows_at(y * part_rows + t * quarter, quarter), :]
                    cross = [lines.push(block, spot, (1 - th, tl, z, y))]
                    lines.copy(block, spot).wait()
                    sent.append(None)
                spots.append(whole.at[rows_at(yy * part_rows + (th * 2 + cc) * quarter, quarter), :])
        for _ in range(waits[2]):
            yield
        for copy, spot in zip(sent, spots):
            if copy is not None:
                copy.wait_recv()
                cross.append(lines.push(spot, spot, (1 - th, tl, z, y)))
        for _ in range(waits[3]):
            yield
        for copy in cross:
            copy.wait_recv()

    pushes = 3 + 2 * (2 * C - 1) + 1
    return Task(
        [(natural, VMEM)],
        [(shape((part_rows * C, D), natural.dtype), VMEM)],
        [pltpu.VMEM((4, S, quarter, D), natural.dtype)],
        pushes,
        greets,
        body,
        2,
    )


def fetch_task(shards, aux, C, waits=(0, 2, 0)):
    _, DB, width = shards.shape

    def greets():
        th, tl, z, y = here()
        across = [(th, tl, z, flip(y, j)) for j in range(1, C)] + [(th, 1 - tl, z, y)]
        return [f(turn) for turn in range(2) for f in (fetch_goal, fetch_source)] + across

    def body(lines, ins, outs, scratch):
        th, tl, z, y = here()
        mine = planes(side_of(tl, z), z)
        whole = outs[0]
        items = [(lambda turn: ins[0].at[turn], lambda a, n: whole.at[rows_at(a * DB, n * DB), :])]
        if aux is not None:
            gathered = outs[1]
            items.append((lambda turn: ins[1].at[turn], lambda a, n: gathered.at[pl.ds(a, n)]))
        for _ in range(waits[0]):
            yield
        first = []
        for turn in range(2):
            for source, spot in items:
                src = source(turn)
                if spot is not items[0][1]:
                    src = ins[1].at[pl.ds(turn, 1)]
                first.append(lines.push(src, spot(z * C + y, 1), fetch_goal(turn)))
        for _ in range(waits[1]):
            yield
        second = []
        n = 0
        for turn in range(2):
            second.append([])
            for _, spot in items:
                first[n].wait_recv()
                n += 1
                piece = spot(mine[turn] * C + y, 1)
                for j in range(1, C):
                    second[turn].append(lines.push(piece, piece, (th, tl, z, flip(y, j))))
            yield
        third = []
        for _ in range(waits[2]):
            yield
        for turn in range(2):
            for copy in second[turn]:
                copy.wait_recv()
            for _, spot in items:
                piece = spot(mine[turn] * C, C)
                third.append(lines.push(piece, piece, (th, 1 - tl, z, y)))
            yield
        for copy in third:
            copy.wait_recv()

    kinds = 1 if aux is None else 2
    inputs = [(shards, ANY)]
    outs = [(shape((4 * C * DB, width), shards.dtype), ANY)]
    if aux is not None:
        inputs.append((aux, ANY))
        outs.append((shape((4 * C,) + aux.shape[1:], aux.dtype), ANY))
    return Task(inputs, outs, [], kinds * (2 + 2 * (C - 1) + 2), greets, body)


def gather_task(box, rows, D):
    def greets():
        return greet_z() + greet_x()

    def body(lines, ins, outs, scratch):
        while "block" not in box:
            yield
        sent = lambda: box.update(gathered=True)
        yield from gather_steps(lines, box["block"], outs[0], sent)

    return Task([], [(shape((8 * rows, D), BF), VMEM)], [], 7, greets, body, 1)


def return_task(f_shape, aux_shape, box):
    def greets():
        return [g(turn) for turn in range(2) for g in (fetch_goal, fetch_source)]

    def body(lines, ins, outs, scratch):
        copies = []
        for turn in range(2):
            while ("turn", turn) not in box:
                yield
            f, aux = box["sums"]
            copies.append(lines.push(f.at[turn], outs[turn], fetch_source(turn)))
            copies.append(lines.push(aux, outs[2 + turn], fetch_source(turn)))
        while "placed" not in box:
            yield
        for copy in copies:
            copy.wait_recv()

    outs = [(shape(f_shape, BF), VMEM)] * 2 + [(shape(aux_shape, F32), VMEM)] * 2
    return Task([], outs, [], 4, greets, body)


def natural_task(rows, D, box, block=None, wait=None):
    def greets():
        th, tl, z, y = here()
        return greet_z((1, 2, 3)) + greet_x() + [(th, 1 - tl, z, y), (th, tl, z, 1 - y)]

    def body(lines, ins, outs, scratch):
        (out,), (stage,) = outs, scratch
        if block is None:
            while "block" not in box:
                yield
            src = box["block"]
        else:
            src = ins[0]
        th, tl, z, y = here()
        home = z == 2 * y + tl
        line = tl == z % 2
        root = jnp.logical_and(line, y == th)
        side = jnp.logical_and(line, y != th)
        leaf = tl != z % 2
        both = jnp.logical_and
        spot = lambda ref, p: ref.at[rows_at(p * rows, rows), :]
        to_home = lines.slots(1)
        at_home = lines.places(4)
        goal = 2 * y + tl
        send = lines.made(
            src, spot(stage, z), lines.send.at[to_home], lines.recv.at[at_home + z], (th, tl, goal, y)
        )
        pl.when(z != goal)(lambda: send.start())
        lines.closing.append(lambda: pl.when(z != goal)(lambda: send.wait_send()))
        base = lines.slots(12)
        own = lines.local.at[lines.used_local]
        lines.used_local += 2
        local = lines.local.at[lines.used_local - 1]
        yield
        for k in range(4):
            p = flip(z, k)
            hop = lines.made(
                spot(stage, p), spot(out, p), lines.send.at[base + k], lines.recv.at[base + k],
                (th, tl, z, 1 - y),
            )
            @pl.when(home)
            def _():
                if k == 0:
                    keep = pltpu.make_async_copy(src, spot(stage, p), own)
                    keep.start()
                    keep.wait()
                else:
                    lines.made(
                        src, spot(stage, p), lines.send.at[to_home],
                        lines.recv.at[at_home + p], (th, tl, goal, y),
                    ).wait_recv()

            @pl.when(both(home, y == th))
            def _():
                keep = pltpu.make_async_copy(spot(stage, p), spot(out, p), local)
                keep.start()
                keep.wait()

            pl.when(both(home, y != th))(lambda: hop.start())
            lines.closing.append(
                lambda hop=hop: pl.when(both(home, y != th))(lambda: hop.wait_send())
            )
            if block is None:
                yield
        if block is not None:
            yield
            yield
        for k in range(4):
            p = flip(z, k)
            hop = lines.made(
                spot(stage, p), spot(out, p), lines.send.at[base + k], lines.recv.at[base + k],
                (th, tl, z, 1 - y),
            )
            core = lines.made(
                spot(out, p), spot(out, p), lines.send.at[base + 4 + k],
                lines.recv.at[base + 4 + k], (th, 1 - tl, z, y),
            )
            cross = lines.made(
                spot(out, p), spot(out, p), lines.send.at[base + 8 + k],
                lines.recv.at[base + 8 + k], (1 - th, tl, z, y),
            )
            pl.when(both(root, jnp.logical_not(home)))(lambda: hop.wait_recv())

            @pl.when(root)
            def _():
                core.start()
                cross.start()

            lines.closing.append(
                lambda core=core: pl.when(line)(lambda: core.wait_send())
            )
            lines.closing.append(
                lambda cross=cross: pl.when(root)(lambda: cross.wait_send())
            )
            if block is None:
                yield
        while wait is not None and wait not in box:
            yield
        for k in range(4):
            p = flip(z, k)
            core = lines.made(
                spot(out, p), spot(out, p), lines.send.at[base + 4 + k],
                lines.recv.at[base + 4 + k], (th, 1 - tl, z, y),
            )
            cross = lines.made(
                spot(out, p), spot(out, p), lines.send.at[base + 8 + k],
                lines.recv.at[base + 8 + k], (1 - th, tl, z, y),
            )

            @pl.when(side)
            def _():
                cross.wait_recv()
                core.start()

            yield
        for k in range(4):
            p = flip(z, k)
            core = lines.made(
                spot(out, p), spot(out, p), lines.send.at[base + 4 + k],
                lines.recv.at[base + 4 + k], (th, 1 - tl, z, y),
            )
            pl.when(leaf)(lambda: core.wait_recv())
        box["placed"] = True

    return Task(
        [] if block is None else [(block, VMEM)],
        [(shape((4 * rows, D), BF), VMEM)],
        [pltpu.VMEM((4 * rows, D), BF)],
        17,
        greets,
        body,
        2,
    )


def pack_block(l, norm_columns, bias_row, out_bias, qkv, up, out, down):
    DB, HW = qkv.shape[3], qkv.shape[4] // 2
    F8 = up.shape[3] // 2
    W1C, W2R = 3 * HW + F8, HW + F8

    def kernel(n_ref, b_ref, o_ref, qkv_ref, up_ref, out_ref, down_ref, one_ref, two_ref, aux_ref):
        z = lax.axis_index("dp")
        g1, s1 = n_ref[:, 0:1], n_ref[:, 1:2]
        g2, s2 = n_ref[:, 2:3], n_ref[:, 3:4]
        for part in range(2):
            turn = (part + z) % 2
            aux_ref[turn] = jnp.zeros(aux_ref.shape[1:], F32)
            for n in range(4):
                if n < 3:
                    w = qkv_ref[0, 0, n, :, part * HW : (part + 1) * HW]
                    at = slice(n * HW, (n + 1) * HW)
                    g, s = g1, s1
                else:
                    w = up_ref[0, 0, :, part * F8 : (part + 1) * F8]
                    at = slice(3 * HW, W1C)
                    g, s = g2, s2
                w = w.astype(BF).astype(F32)
                one_ref[turn, :, at] = (g * w).astype(BF)
                aux_ref[turn, 0:1, at] = (
                    jnp.sum(s * w, axis=0, keepdims=True) + b_ref[part : part + 1, at]
                )
            aux_ref[turn, 1:2, 0:DB] = o_ref[...]
            two_ref[turn, :, 0:HW] = out_ref[0, 0, part * HW : (part + 1) * HW, :].T.astype(BF)
            two_ref[turn, :, HW:W2R] = down_ref[0, 0, part * F8 : (part + 1) * F8, :].T.astype(BF)

    whole = lambda x: pl.BlockSpec(x.shape, lambda i: (0,) * x.ndim)
    layer = lambda x: pl.BlockSpec(
        (1, 1) + x.shape[2:], lambda i: (0, l) + (0,) * (x.ndim - 2)
    )
    return pl.pallas_call(
        kernel,
        grid=(1,),
        out_shape=[
            shape((2, DB, W1C), BF),
            shape((2, DB, W2R), BF),
            shape((2, 8, W1C), F32),
        ],
        in_specs=[whole(norm_columns), whole(bias_row), whole(out_bias)]
        + [layer(x) for x in (qkv, up, out, down)],
        out_specs=[
            pl.BlockSpec((2, DB, W1C), lambda i: (0, 0, 0)),
            pl.BlockSpec((2, DB, W2R), lambda i: (0, 0, 0)),
            pl.BlockSpec((2, 8, W1C), lambda i: (0, 0, 0)),
        ],
        compiler_params=pltpu.CompilerParams(vmem_limit_bytes=40 << 20),
        cost_estimate=pl.CostEstimate(flops=0, bytes_accessed=10 << 20, transcendentals=0),
        name="pack",
    )(norm_columns, bias_row, out_bias, qkv, up, out, down)


def turned(x, turn_ref, sign):
    half = ROT // 2
    lane = lax.broadcasted_iota(jnp.int32, x.shape, 1)
    width = x.shape[1]
    other = jnp.where(lane < half, pltpu.roll(x, width - half, 1), pltpu.roll(x, half, 1))
    return x * turn_ref[0] + other * (turn_ref[1] * sign)


def causal_block(start, width):
    rows = start + lax.broadcasted_iota(jnp.int32, (width, start + width), 0)
    return lax.broadcasted_iota(jnp.int32, (width, start + width), 1) <= rows


def forward_compute(x, w1, aux, turns, raw):
    L, D = x.shape
    W1C = w1.shape[1]
    HW = turns.shape[2]
    F8 = W1C - 3 * HW
    R = 256 if L % 256 == 0 else L
    steps = L // R

    def kernel(x_ref, w_ref, aux_ref, t_ref, *outs):
        if raw:
            xh_ref, outs = outs[0], outs[1:]
        q_ref, k_ref, v_ref, act_ref, slope_ref, lse_ref, bias_ref = outs
        i = pl.program_id(0)

        @pl.when(i == 0)
        def _():
            total = aux_ref[0, 0:1, :]
            for n in range(1, aux_ref.shape[0]):
                total = total + aux_ref[n, 0:1, :]
            bias_ref[0:1, :] = total

        rows = pl.ds(pl.multiple_of(i * R, R), R)
        if raw:
            xh = normalized(x_ref[...].astype(F32))[0].astype(BF)
            xh_ref[...] = xh
        else:
            xh = x_ref[...]
        table = t_ref.at[:, rows, :]
        for n in range(3):
            at = slice(n * HW, (n + 1) * HW)
            p = dot(xh, w_ref[:, at], NN) + bias_ref[0:1, at]
            if n == 0:
                q_ref[rows, :] = (turned(p, table, 1.0) * HEAD_DIM ** (-0.5)).astype(BF)
            elif n == 1:
                k_ref[rows, :] = turned(p, table, 1.0).astype(BF)
            else:
                v_ref[rows, :] = p.astype(BF)
        piece = min(512, F8)
        for c in range(0, F8, piece):
            at = slice(3 * HW + c, 3 * HW + c + piece)
            u = dot(xh, w_ref[:, at], NN) + bias_ref[0:1, at]
            phi = 0.5 + 0.5 * lax.erf(u * 0.5**0.5)
            act_ref[rows, HW + c : HW + c + piece] = (u * phi).astype(BF)
            slope_ref[:, c : c + piece] = (
                phi + u * (jnp.exp(-0.5 * u * u) * 0.3989422804014327)
            ).astype(BF)

        @pl.when(i == steps - 1)
        def _():
            for start in range(0, L, R):
                here_rows, seen = pl.ds(start, R), pl.ds(0, start + R)
                scores = dot(q_ref[here_rows, :], k_ref[seen, :], NT)
                scores = jnp.where(causal_block(start, R), scores, -1e30)
                peak = jnp.max(scores, axis=-1, keepdims=True)
                weights = jnp.exp(scores - peak)
                total = jnp.sum(weights, axis=-1, keepdims=True)
                weights = (weights * (1.0 / total)).astype(BF)
                act_ref[here_rows, 0:HW] = dot(weights, v_ref[seen, :], NN).astype(BF)
                lse_ref[here_rows, :] = jnp.broadcast_to(peak + jnp.log(total), (R, 128))

    fixed = lambda dims: pl.BlockSpec(dims, lambda i: (0,) * len(dims))
    moving = lambda dims: pl.BlockSpec(dims, lambda i: (i, 0))
    out_shape = [
        shape((L, HW), BF),
        shape((L, HW), BF),
        shape((L, HW), BF),
        shape((L, HW + F8), BF),
        shape((L, F8), BF),
        shape((L, 128), F32),
    ]
    out_specs = [
        fixed((L, HW)),
        fixed((L, HW)),
        fixed((L, HW)),
        fixed((L, HW + F8)),
        moving((R, F8)),
        fixed((L, 128)),
    ]
    if raw:
        out_shape.insert(0, shape((L, D), BF))
        out_specs.insert(0, moving((R, D)))
    out = pl.pallas_call(
        kernel,
        grid=(steps,),
        out_shape=out_shape,
        in_specs=[moving((R, D)), fixed(w1.shape), fixed(aux.shape), fixed(turns.shape)],
        out_specs=out_specs,
        scratch_shapes=[pltpu.VMEM((8, W1C), F32)],
        compiler_params=pltpu.CompilerParams(vmem_limit_bytes=56 << 20),
        cost_estimate=pl.CostEstimate(
            flops=2 * L * D * W1C, bytes_accessed=24 << 20, transcendentals=4 << 20
        ),
        name="forward_raw" if raw else "forward",
    )(x, w1, aux, turns)
    return out if raw else [x] + list(out)


def backward_compute(gb, w2, slope, q, k, v, lse, turns):
    L, D = gb.shape
    W2R = w2.shape[1]
    HW = q.shape[1]
    F8 = W2R - HW
    W1C = 3 * HW + F8
    R = 256 if L % 256 == 0 else L
    steps = L // R
    scale = HEAD_DIM ** (-0.5)

    def kernel(
        g_ref, w_ref, s_ref, q_ref, k_ref, v_ref, l_ref, t_ref, dy_ref, small_ref, go, dq, dk, dv
    ):
        i = pl.program_id(0)

        @pl.when(i == 0)
        def _():
            small_ref[...] = jnp.zeros_like(small_ref)
            dk[...] = jnp.zeros_like(dk)
            dv[...] = jnp.zeros_like(dv)

        rows = pl.ds(pl.multiple_of(i * R, R), R)
        g = g_ref[...]
        small_ref[1:2, 0:D] += jnp.sum(g.astype(F32), axis=0, keepdims=True)
        go[rows, :] = dot(g, w_ref[:, 0:HW], NN).astype(BF)
        piece = min(512, F8)
        for c in range(0, F8, piece):
            du = dot(g, w_ref[:, HW + c : HW + c + piece], NN)
            du = (du * s_ref[:, c : c + piece].astype(F32)).astype(BF)
            dy_ref[rows, 3 * HW + c : 3 * HW + c + piece] = du
            small_ref[0:1, 3 * HW + c : 3 * HW + c + piece] += jnp.sum(
                du.astype(F32), axis=0, keepdims=True
            )

        @pl.when(i == steps - 1)
        def _():
            for start in range(0, L, R):
                here_rows, seen = pl.ds(start, R), pl.ds(0, start + R)
                qq, gg = q_ref[here_rows, :], go[here_rows, :]
                scores = dot(qq, k_ref[seen, :], NT)
                weights = jnp.where(
                    causal_block(start, R), jnp.exp(scores - l_ref[here_rows, 0:1]), 0.0
                )
                inner = dot(gg, v_ref[seen, :], NT)
                delta = jnp.sum(weights * inner, axis=-1, keepdims=True)
                ds = (weights * (inner - delta)).astype(BF)
                dq[here_rows, :] = dot(ds, k_ref[seen, :], NN) * scale
                dk[seen, :] += dot(ds, qq, TN)
                dv[seen, :] += dot(weights.astype(BF), gg, TN)
            for n, grad in enumerate((dq, dk, dv)):
                at = slice(n * HW, (n + 1) * HW)
                value = grad[...] if n == 2 else turned(grad[...], t_ref, -1.0)
                value = value.astype(BF)
                dy_ref[:, at] = value
                small_ref[0:1, at] = jnp.sum(value.astype(F32), axis=0, keepdims=True)

    fixed = lambda dims: pl.BlockSpec(dims, lambda i: (0,) * len(dims))
    moving = lambda dims: pl.BlockSpec(dims, lambda i: (i, 0))
    return pl.pallas_call(
        kernel,
        grid=(steps,),
        out_shape=[shape((L, W1C), BF), shape((8, max(W1C, D)), F32)],
        in_specs=[moving((R, D)), fixed(w2.shape), moving((R, F8))]
        + [fixed(x.shape) for x in (q, k, v, lse, turns)],
        out_specs=[fixed((L, W1C)), fixed((8, max(W1C, D)))],
        scratch_shapes=[
            pltpu.VMEM((L, HW), BF),
            pltpu.VMEM((L, HW), F32),
            pltpu.VMEM((L, HW), F32),
            pltpu.VMEM((L, HW), F32),
        ],
        compiler_params=pltpu.CompilerParams(vmem_limit_bytes=56 << 20),
        cost_estimate=pl.CostEstimate(
            flops=2 * L * D * W2R, bytes_accessed=20 << 20, transcendentals=1 << 20
        ),
        name="backward",
    )(gb, w2, slope, q, k, v, lse, turns)


def adam_values(w, m, q, gradient, learn_rate, decay_rate):
    moment = beta_one * m + (1.0 - beta_one) * gradient
    root_second = jnp.sqrt(beta_two * q * q + (1.0 - beta_two) * gradient * gradient)
    update = (
        (learn_rate / (1.0 - beta_one**STEP))
        * moment
        / (root_second * (1.0 / (1.0 - beta_two**STEP) ** 0.5) + adam_eps)
    )
    return moment, root_second, w - update - learn_rate * decay_rate * w


def adam_block(state_ref, at, gradient, pack_ref, new_ref):
    moment, root_second, weight = adam_values(
        state_ref[(0, 0) + at],
        state_ref[(1, 0) + at],
        state_ref[(2, 0) + at],
        gradient,
        rate_matrix,
        weight_decay,
    )
    pack_ref[(0, 0) + at] = gradient
    pack_ref[(1, 0) + at] = moment
    pack_ref[(2, 0) + at] = root_second
    new_ref[(0,) + at] = weight


def chosen(first, turn, values):
    even = turn == 0
    return jnp.where(
        first, jnp.where(even, values[0], values[1]), jnp.where(even, values[2], values[3])
    )


def adam_inner(qkv, up, grads, smalls, columns):
    _, layers, _, DB, wide = qkv.shape
    HW = wide // 2
    F8 = up.shape[3] // 2
    assert layers == 2

    def qkv_kernel(*refs):
        s_ref, grads, smalls, (c0, c1) = refs[0], refs[1:5], refs[5:9], refs[9:11]
        pack_ref, new_ref, term_ref = refs[11:]
        l, n = pl.program_id(0), pl.program_id(1)
        z = lax.axis_index("dp")
        first = l == 0
        col = jnp.where(first, c0[...], c1[...])
        at = pl.ds(pl.multiple_of(n * HW, HW), HW)

        @pl.when(n == 0)
        def _():
            term_ref[...] = jnp.zeros_like(term_ref)

        for part in range(2):
            turn = (part + z) % 2
            m = chosen(first, turn, [g[:, at] for g in grads]).astype(F32)
            b = chosen(first, turn, [g[0:1, at] for g in smalls])
            spot = (0, slice(None), slice(part * HW, (part + 1) * HW))
            w = s_ref[(0, 0) + spot].astype(BF).astype(F32)
            term_ref[0, :, 0:1] += jnp.sum(w * m, axis=1, keepdims=True)
            term_ref[0, :, 1:2] += jnp.sum(w * b, axis=1, keepdims=True)
            adam_block(s_ref, spot, col[:, 0:1] * m + col[:, 1:2] * b, pack_ref, new_ref)

    def up_kernel(*refs):
        s_ref, grads, smalls, (c0, c1) = refs[0], refs[1:5], refs[5:9], refs[9:11]
        pack_ref, new_ref, term_ref = refs[11:]
        l, part = pl.program_id(0), pl.program_id(1)
        turn = (part + lax.axis_index("dp")) % 2
        first = l == 0
        col = jnp.where(first, c0[...], c1[...])

        @pl.when(part == 0)
        def _():
            term_ref[...] = jnp.zeros_like(term_ref)

        piece = min(512, F8)
        for c in range(0, F8, piece):
            at = slice(3 * HW + c, 3 * HW + c + piece)
            m = chosen(first, turn, [g[:, at] for g in grads]).astype(F32)
            b = chosen(first, turn, [g[0:1, at] for g in smalls])
            spot = (slice(None), slice(c, c + piece))
            w = s_ref[(0, 0) + spot].astype(BF).astype(F32)
            term_ref[0, :, 0:1] += jnp.sum(w * m, axis=1, keepdims=True)
            term_ref[0, :, 1:2] += jnp.sum(w * b, axis=1, keepdims=True)
            adam_block(s_ref, spot, col[:, 2:3] * m + col[:, 3:4] * b, pack_ref, new_ref)

    fixed = lambda x: pl.BlockSpec(x.shape, lambda l, n: (0,) * x.ndim)
    params = pltpu.CompilerParams(vmem_limit_bytes=48 << 20)
    small = list(grads) + list(smalls) + list(columns)
    term_spec = pl.BlockSpec((1, DB, 128), lambda l, n: (l, 0, 0))
    term_shape = shape((2, DB, 128), F32)
    cost = lambda x: pl.CostEstimate(flops=0, bytes_accessed=x.size * 10, transcendentals=0)
    qkv_out = pl.pallas_call(
        qkv_kernel,
        grid=(2, 3),
        out_shape=[shape(qkv.shape, F32), shape(qkv.shape[1:], F32), term_shape],
        in_specs=[pl.BlockSpec((3, 1, 1, DB, wide), lambda l, n: (0, l, n, 0, 0))]
        + [fixed(x) for x in small],
        out_specs=[
            pl.BlockSpec((3, 1, 1, DB, wide), lambda l, n: (0, l, n, 0, 0)),
            pl.BlockSpec((1, 1, DB, wide), lambda l, n: (l, n, 0, 0)),
            term_spec,
        ],
        compiler_params=params,
        cost_estimate=cost(qkv),
        name="adam_qkv",
    )(qkv, *small)
    up_out = pl.pallas_call(
        up_kernel,
        grid=(2, 2),
        out_shape=[shape(up.shape, F32), shape(up.shape[1:], F32), term_shape],
        in_specs=[pl.BlockSpec((3, 1, DB, F8), lambda l, n: (0, l, 0, n))]
        + [fixed(x) for x in small],
        out_specs=[
            pl.BlockSpec((3, 1, DB, F8), lambda l, n: (0, l, 0, n)),
            pl.BlockSpec((1, DB, F8), lambda l, n: (l, 0, n)),
            term_spec,
        ],
        compiler_params=params,
        cost_estimate=cost(up),
        name="adam_up",
    )(up, *small)
    return qkv_out, up_out


def adam_outer(state, grads, begin, name):
    _, layers, rows, DB = state.shape
    half = rows // 2

    def kernel(s_ref, *refs):
        pack_ref, new_ref = refs[4:]
        l, part = pl.program_id(0), pl.program_id(1)
        turn = (part + lax.axis_index("dp")) % 2
        piece = min(256, half)
        for c in range(0, half, piece):
            at = slice(begin + c, begin + c + piece)
            m = chosen(l == 0, turn, [g[:, at] for g in refs[:4]]).astype(F32).T
            adam_block(s_ref, (slice(c, c + piece), slice(None)), m, pack_ref, new_ref)

    fixed = lambda x: pl.BlockSpec(x.shape, lambda l, n: (0,) * x.ndim)
    return pl.pallas_call(
        kernel,
        grid=(2, 2),
        out_shape=[shape(state.shape, F32), shape(state.shape[1:], F32)],
        in_specs=[pl.BlockSpec((3, 1, half, DB), lambda l, n: (0, l, n, 0))]
        + [fixed(x) for x in grads],
        out_specs=[
            pl.BlockSpec((3, 1, half, DB), lambda l, n: (0, l, n, 0)),
            pl.BlockSpec((1, half, DB), lambda l, n: (l, n, 0)),
        ],
        compiler_params=pltpu.CompilerParams(vmem_limit_bytes=48 << 20),
        cost_estimate=pl.CostEstimate(
            flops=0, bytes_accessed=state.size * 10, transcendentals=0
        ),
        name=name,
    )(state, *grads)


def piece_dot(lhs, w_ref, write):
    D = w_ref.shape[0]
    tile = min(512, D)

    def some(c, carry):
        at = pl.ds(pl.multiple_of(c * tile, tile), tile)
        write(at, dot(lhs, w_ref[at, :], NT))
        return carry

    lax.fori_loop(0, D // tile, some, 0)


def scatter_steps(lines, lhs_of, w_ref, far, came, ready, last, total):
    th, tl, z, y = here()
    rows = came.shape[1]

    def pair(half, base):
        high = z // 2 if base == 0 else 1 - z // 2
        return lhs_of(half * 4 + high * 2)

    cross, along = {}, {}
    for p, base in enumerate((2, 0)):

        def keep(at, value, p=p):
            far[p, :, at] = value.astype(BF)

        piece_dot(pair(1 - th, base), w_ref, keep)
        for k in (base + 1, base):
            piece = far.at[p, rows_at((flip(z, k) % 2) * rows, rows), :]
            cross[k] = lines.push(piece, came.at[k], (1 - th, tl, z, y))
    yield
    for base in (2, 0):

        def keep(at, value, base=base):
            for r in range(2):
                ready[base + (r + z) % 2, :, at] = value[r * rows : (r + 1) * rows].astype(BF)

        piece_dot(pair(th, base), w_ref, keep)
    for k in (3, 2, 1):
        cross[k].wait_recv()
        value = ready[k].astype(F32) + came[k].astype(F32)
        if k == 2:
            along[3].wait_recv()
            value = value + last[2].astype(F32)
        ready[k] = value.astype(BF)
        goal = flip(z, 2) if k == 2 else flip(z, 1)
        along[k] = lines.push(ready.at[k], last.at[k - 1], (th, tl, goal, y))
        yield
    cross[0].wait_recv()
    yield
    value = ready[0].astype(F32) + came[0].astype(F32)
    for k in (1, 2):
        along[k].wait_recv()
        value = value + last[k - 1].astype(F32)
    total[...] = value


def gather_steps(lines, src, whole, sent=lambda: None):
    th, tl, z, y = here()
    rows = src.shape[0]
    spot = lambda a, b: whole.at[rows_at((a * 4 + b) * rows, rows), :]
    cross = [lines.push(src, spot(th, z), (1 - th, tl, z, y))]
    near = {k: lines.push(src, spot(th, z), (th, tl, flip(z, k), y)) for k in (1, 2)}
    lines.copy(src, spot(th, z)).wait()
    yield
    for k in (1, 2, 3):
        near[k].wait_recv()
        piece = spot(th, flip(z, k))
        if k == 2:
            near[3] = lines.push(piece, piece, (th, tl, flip(z, 1), y))
        cross.append(lines.push(piece, piece, (1 - th, tl, z, y)))
        yield
    sent()
    yield
    for copy in cross:
        copy.wait_recv()


def forward_task(x, w1, w2, aux, turns, h, bias_out, onward):
    L, D = x.shape
    raw = h is None
    W1C, W2R = w1.shape[1], w2.shape[1]
    HW = turns.shape[2]
    F8 = W1C - 3 * HW
    R = 256 if L % 256 == 0 else L
    steps = L // R
    rows_b = L // 8

    def greets():
        return greet_z() + greet_x()

    def body(lines, ins, outs, scratch):
        x_ref, w1_ref, w2_ref, aux_ref, t_ref, bo_ref = ins[:6]
        q_ref, k_ref, v_ref, act_ref, slope_ref, lse_ref, new_ref = outs[:7]
        w1_in, w2_in, bias_ref, far, came, ready, last, block = scratch
        th, tl, z, y = here()
        load1 = lines.copy(w1_ref, w1_in)
        load2 = lines.copy(w2_ref, w2_in)
        total = aux_ref[0, 0:1, :]
        for n in range(1, aux_ref.shape[0]):
            total = total + aux_ref[n, 0:1, :]
        bias_ref[0:1, :] = total
        load1.wait()

        def some(i, carry):
            rows = pl.ds(pl.multiple_of(i * R, R), R)
            if raw:
                xh = normalized(x_ref[rows, :].astype(F32))[0].astype(BF)
                outs[7][rows, :] = xh
            else:
                xh = x_ref[rows, :]
            table = t_ref.at[:, rows, :]
            for n in range(3):
                at = slice(n * HW, (n + 1) * HW)
                p = dot(xh, w1_in[:, at], NN) + bias_ref[0:1, at]
                if n == 0:
                    q_ref[rows, :] = (turned(p, table, 1.0) * HEAD_DIM ** (-0.5)).astype(BF)
                elif n == 1:
                    k_ref[rows, :] = turned(p, table, 1.0).astype(BF)
                else:
                    v_ref[rows, :] = p.astype(BF)
            piece = min(512, F8)
            for c in range(0, F8, piece):
                at = slice(3 * HW + c, 3 * HW + c + piece)
                u = dot(xh, w1_in[:, at], NN) + bias_ref[0:1, at]
                phi = 0.5 + 0.5 * lax.erf(u * 0.5**0.5)
                act_ref[rows, HW + c : HW + c + piece] = (u * phi).astype(BF)
                slope_ref[rows, c : c + piece] = (
                    phi + u * (jnp.exp(-0.5 * u * u) * 0.3989422804014327)
                ).astype(BF)
            return carry

        lax.fori_loop(0, steps, some, 0)
        for start in range(0, L, R):
            here_rows, seen = pl.ds(start, R), pl.ds(0, start + R)
            scores = dot(q_ref[here_rows, :], k_ref[seen, :], NT)
            scores = jnp.where(causal_block(start, R), scores, -1e30)
            peak = jnp.max(scores, axis=-1, keepdims=True)
            weights = jnp.exp(scores - peak)
            total = jnp.sum(weights, axis=-1, keepdims=True)
            weights = (weights * (1.0 / total)).astype(BF)
            act_ref[here_rows, 0:HW] = dot(weights, v_ref[seen, :], NN).astype(BF)
            lse_ref[here_rows, :] = jnp.broadcast_to(peak + jnp.log(total), (R, 128))
        load2.wait()
        yield
        yield from scatter_steps(
            lines,
            lambda n: act_ref[pl.ds(pl.multiple_of(n * rows_b, 2 * rows_b), 2 * rows_b), :],
            w2_in,
            far,
            came,
            ready,
            last,
            new_ref,
        )
        if raw:
            before = x_ref[rows_at((th * 4 + z) * rows_b, rows_b), :].astype(F32)
        else:
            before = ins[6][...]
        new = before + new_ref[...] + bo_ref[...]
        new_ref[...] = new
        if onward:
            block[...] = normalized(new)[0].astype(BF)
            yield from gather_steps(lines, block, outs[-1])

    inputs = [(x, VMEM), (w1, ANY), (w2, ANY), (aux, VMEM), (turns, VMEM), (bias_out, VMEM)]
    outs = [
        (shape((L, HW), BF), VMEM),
        (shape((L, HW), BF), VMEM),
        (shape((L, HW), BF), VMEM),
        (shape((L, HW + F8), BF), VMEM),
        (shape((L, F8), BF), VMEM),
        (shape((L, 128), F32), VMEM),
        (shape((rows_b, D), F32), VMEM),
    ]
    if raw:
        outs.append((shape((L, D), BF), VMEM))
    else:
        inputs.append((h, VMEM))
    if onward:
        outs.append((shape((L, D), BF), VMEM))
    return Task(
        inputs,
        outs,
        [
            pltpu.VMEM(w1.shape, BF),
            pltpu.VMEM(w2.shape, BF),
            pltpu.VMEM((8, W1C), F32),
            pltpu.VMEM((2, 2 * rows_b, D), BF),
            pltpu.VMEM((4, rows_b, D), BF),
            pltpu.VMEM((4, rows_b, D), BF),
            pltpu.VMEM((3, rows_b, D), BF),
            pltpu.VMEM((rows_b, D), BF),
        ],
        14 if onward else 7,
        greets,
        body,
        3 if onward else 2,
    )


def slope_task(dy, w1, act, gb, h, g, box):
    L, W1C = dy.shape
    D = gb.shape[1]
    rows = L // 8

    def greets():
        return greet_z() + greet_x()

    def body(lines, ins, outs, scratch):
        dy_ref, w1_ref, act_ref, gb_ref, h_ref, g_ref = ins
        (out,) = outs
        w1_in, far, came, ready, last, block = scratch
        load = lines.copy(w1_ref, w1_in)
        box["factors"] = (dy_ref, act_ref, gb_ref)
        load.wait()
        yield from scatter_steps(
            lines,
            lambda n: dy_ref[pl.ds(pl.multiple_of(n * rows, 2 * rows), 2 * rows), :],
            w1_in,
            far,
            came,
            ready,
            last,
            out,
        )
        total = out[...]
        xn, inverse = normalized(h_ref[...])
        value = g_ref[...] + inverse * (
            total
            - jnp.mean(total, axis=-1, keepdims=True)
            - xn * jnp.mean(total * xn, axis=-1, keepdims=True)
        )
        out[...] = value
        block[...] = value.astype(BF)
        box["block"] = block

    return Task(
        [(dy, VMEM), (w1, ANY), (act, VMEM), (gb, VMEM), (h, VMEM), (g, VMEM)],
        [(shape((rows, D), F32), VMEM)],
        [
            pltpu.VMEM(w1.shape, BF),
            pltpu.VMEM((2, 2 * rows, D), BF),
            pltpu.VMEM((4, rows, D), BF),
            pltpu.VMEM((4, rows, D), BF),
            pltpu.VMEM((3, rows, D), BF),
            pltpu.VMEM((rows, D), BF),
        ],
        7,
        greets,
        body,
        1,
    )


def collect_task(xh, wide, deep, aux, C, box):
    L, D = xh.shape
    DB = D // (4 * C)
    CB = C * DB
    both = wide + deep
    tall = aux.shape
    step = min(256, CB)

    def greets():
        th, tl, z, y = here()
        return [(th, 1 - tl, z, y)] + [(th, tl, z, flip(y, j)) for j in range(1, C)]

    def body(lines, ins, outs, scratch):
        xh_ref, aux_ref = ins
        f_ref, fa_ref = outs
        send, came, came_y, columns, small_own, small_came, small_y = scratch
        th, tl, z, y = here()
        side = side_of(tl, z)
        mine, other = planes(side, z), planes(1 - side, z)
        over = (th, 1 - tl, z, y)
        sites = [other[0], mine[0], other[1], mine[1]]

        def load(n):
            return lines.copy(xh_ref.at[:, rows_at(sites[n] * CB, CB)], columns.at[n % 2])

        loads = [load(0)]
        sent_small = lines.push(aux_ref, small_came, over)
        while "factors" not in box:
            yield
        dy_ref, act_ref, gb_ref = box["factors"]
        sent, across = [], []
        for n in range(4):
            turn, own = n // 2, n % 2 == 1
            if n < 3:
                loads.append(load(n + 1))
            loads[n].wait()
            if own:
                sent[turn].wait_recv()
            target = came if own else send

            def some(i, carry, n=n, turn=turn, own=own, target=target):
                at = pl.ds(pl.multiple_of(i * step, step), step)
                begin = pl.ds(pl.multiple_of(sites[n] * CB + i * step, step), step)
                one = dot(columns[n % 2, :, at], dy_ref[...], TN)
                if own:
                    one = one + came[turn, at, 0:wide].astype(F32)
                target[turn, at, 0:wide] = one.astype(BF)
                two = dot(gb_ref[:, begin], act_ref[...], TN)
                if own:
                    two = two + came[turn, at, wide:].astype(F32)
                target[turn, at, wide:] = two.astype(BF)
                return carry

            lax.fori_loop(0, CB // step, some, 0)
            if not own:
                sent.append(lines.push(send.at[turn], came.at[turn], over))
            else:
                for j in range(1, C):
                    at = rows_at(flip(y, j) * DB, DB)
                    across.append(
                        (
                            turn,
                            j,
                            lines.push(
                                came.at[turn, at, :],
                                came_y.at[j - 1, turn],
                                (th, tl, z, flip(y, j)),
                            ),
                        )
                    )
            if n == 1:
                sent_small.wait_recv()
                small_own[...] = aux_ref[...] + small_came[...]
                small = [
                    lines.push(small_own, small_y.at[j - 1], (th, tl, z, flip(y, j)))
                    for j in range(1, C)
                ]
            yield
        while "block" not in box:
            yield
        for copy in small:
            copy.wait_recv()
        total = small_own[...]
        for j in range(1, C):
            total = total + small_y[j - 1]
        fa_ref[...] = total
        box["sums"] = outs
        yield
        yield
        some_rows = min(64, DB)
        for turn in range(2):
            for t, j, copy in across:
                if t == turn:
                    copy.wait_recv()

            def add(i, carry, turn=turn):
                at = pl.ds(pl.multiple_of(i * some_rows, some_rows), some_rows)
                from_at = pl.ds(
                    pl.multiple_of(y * DB + i * some_rows, some_rows), some_rows
                )
                value = came[turn, from_at, :].astype(F32)
                for j in range(1, C):
                    value = value + came_y[j - 1, turn, at, :].astype(F32)
                f_ref[turn, at, :] = value.astype(BF)
                return carry

            lax.fori_loop(0, DB // some_rows, add, 0)
            box["turn", turn] = True
            yield

    return Task(
        [(xh, ANY), (aux, VMEM)],
        [(shape((2, DB, both), BF), VMEM), (shape(tall, F32), VMEM)],
        [
            pltpu.VMEM((2, CB, both), BF),
            pltpu.VMEM((2, CB, both), BF),
            pltpu.VMEM((C - 1, 2, DB, both), BF),
            pltpu.VMEM((2, L, CB), BF),
            pltpu.VMEM(tall, F32),
            pltpu.VMEM(tall, F32),
            pltpu.VMEM((C - 1,) + tall, F32),
        ],
        3 + (C - 1) * 3,
        greets,
        body,
        4,
    )


def build(mesh):
    tensor, Z, C = (mesh.shape[name] for name in AXES)
    assert tensor == 4 and Z == 4

    def flat(th, tl, z, y):
        return ((th * 2 + tl) * Z + z) * C + y

    def permute(x, move):
        pairs = []
        for th in range(2):
            for tl in range(2):
                for z in range(Z):
                    for y in range(C):
                        target = move(th, tl, z, y)
                        if target is not None:
                            pairs.append((flat(th, tl, z, y), flat(*target)))
        return lax.ppermute(x, AXES, pairs)

    def give_move(turn):
        def move(th, tl, z, y):
            side = tl ^ (z // 2)
            return (th, z // 2, z ^ (2 - 2 * side if turn == 0 else 1 + 2 * side), y)

        return move

    def over_x(x):
        return permute(x, lambda th, tl, z, y: (1 - th, tl, z, y))

    def over_core(x):
        return permute(x, lambda th, tl, z, y: (th, 1 - tl, z, y))

    def local(
        inputs,
        cotangent,
        qkv_state,
        out_state,
        up_state,
        down_state,
        qkv_bias_state,
        up_bias_state,
        norm_state,
    ):
        layers = qkv_state.shape[1]
        S, part_rows, D = inputs.shape
        L = part_rows * C
        rows_b = L // 8
        DB = D // (Z * C)
        F8 = up_state.shape[3] // 2
        HW = qkv_state.shape[4] // 2
        W1C, W2R = 3 * HW + F8, HW + F8
        th, tl, z, y = here()
        odd = (z % 2) == 1
        place = z * C + y
        qkv_planes = jnp.transpose(qkv_state, (0, 1, 3, 2, 4))

        norm_rows = norm_state[0].astype(BF).astype(F32)
        columns = [jnp.pad(norm_rows[l].T, ((0, 0), (0, 3))) for l in range(layers)]

        def pack(l):
            rows = norm_rows[l]
            bq = qkv_bias_state[0, l].astype(BF).astype(F32)
            bu = up_bias_state[0, l].astype(BF).astype(F32)
            n = bq.shape[1]
            vq = lax.dynamic_update_slice(jnp.zeros((3, 2 * HW), F32), bq, (0, place * n))
            vu = lax.dynamic_update_slice(jnp.zeros((2 * F8,), F32), bu, (place * bu.shape[0],))
            vq = jnp.transpose(vq.reshape(3, 2, HW), (1, 0, 2)).reshape(2, 3 * HW)
            row = jnp.concatenate([vq, vu.reshape(2, F8)], axis=1)
            return pack_block(
                l, columns[l], row, rows[4:5], qkv_planes, up_state, out_state, down_state
            )

        def my_rows(whole):
            return lax.dynamic_slice_in_dim(whole, (th * 4 + z) * rows_b, rows_b, axis=0)

        near_home = C == 2 and S == 1

        def return_natural(block):
            every = lax.all_gather(block, AXES, axis=0)
            every = every.reshape(2, 2, Z, C, rows_b, D)
            every = jnp.transpose(every, (3, 1, 0, 2, 4, 5)).reshape(2 * C, L, D)
            return lax.dynamic_slice(every, (z * S, y * part_rows, 0), (S, part_rows, D))

        positions = jnp.arange(L, dtype=F32)
        frequency = 10000.0 ** (-2.0 * jnp.arange(ROT // 2, dtype=F32) / ROT)
        angles = positions[:, None] * frequency[None, :]
        cosine, sine = jnp.cos(angles), jnp.sin(angles)
        rest = HEAD_DIM - ROT
        turns = jnp.stack(
            [
                jnp.concatenate([cosine, cosine, jnp.ones((L, rest), F32)], axis=1),
                jnp.concatenate([-sine, sine, jnp.zeros((L, rest), F32)], axis=1),
            ]
        )

        packs = [pack(l) for l in range(layers)]
        one, two, aux = packs[0]
        (whole_in,), (w1, aux1), (w2,) = run_tasks(
            [
                spread_task(inputs, C, (0, 1, 1, 3)),
                fetch_task(one, aux, C, (1, 2, 1)),
                fetch_task(two, None, C, (1, 4, 1)),
            ],
            0,
            "start",
            48,
        )
        params, saved = [], []
        x, h = whole_in, None
        number = 1
        for l in range(layers):
            bias_out = aux1[:, 1, :DB].reshape(1, D)
            onward = l + 1 < layers
            task = forward_task(x, w1, w2, aux1, turns, h, bias_out, onward)
            if onward:
                one, two, aux = packs[l + 1]
                tasks = [
                    fetch_task(one, aux, C, (0, 3, 2)),
                    fetch_task(two, None, C, (0, 7, 1)),
                    task,
                ]
            else:
                tasks = [spread_task(cotangent, C, (0, 1, 3, 2)), task]
            done = run_tasks(tasks, number, "layer_f%d" % l, 63)
            q, k, v, act, slope, lse, new = done[-1][:7]
            xh = done[-1][7] if l == 0 else x
            before = my_rows(whole_in).astype(F32) if l == 0 else h
            saved.append((before, xh, q, k, v, act, slope, lse))
            params.append((w1, w2))
            h = new
            number += 1
            if onward:
                w1, aux1 = done[0]
                (w2,) = done[1]
                x = done[2][-1]
            else:
                (gb,) = done[0]
        outputs = None if near_home else return_natural(h.astype(BF))

        g = my_rows(gb).astype(F32)
        got = [None] * layers
        for l in reversed(range(layers)):
            h_in, xh, q, k, v, act, slope, lse = saved[l]
            w1, w2 = params[l]
            dy, small = backward_compute(gb, w2, slope, q, k, v, lse, turns)
            box = {}
            tasks = [slope_task(dy, w1, act, gb, h_in, g, box)]
            if l > 0:
                tasks.append(gather_task(box, rows_b, D))
            tasks.append(collect_task(xh, W1C, W2R, small, C, box))
            if l == 0:
                tasks.append(return_task((DB, W1C + W2R), small.shape, box))
            if near_home and l == 0:
                tasks.append(natural_task(rows_b, D, box))
            elif outputs is None:
                tasks.insert(1, natural_task(rows_b, D, box, h.astype(BF), "gathered"))
            if not near_home:
                box["placed"] = True
            done = run_tasks(tasks, number, "layer_b%d" % l, 63)
            number += 1
            if outputs is None:
                outputs = done.pop(1)[0][None]
            (g,) = done[0]
            if l > 0:
                (gb,), (f, fa) = done[1:3]
                gb, f, fa = lax.optimization_barrier((gb, f, fa))
                got[l] = [permute(f[turn], give_move(turn)) for turn in range(2)]
                got[l] += [permute(fa, give_move(turn)) for turn in range(2)]
            else:
                got[l] = list(done[2])
        if near_home:
            input_grad = done[3][0][None].astype(F32)
        else:
            input_grad = return_natural(g.astype(BF)).astype(F32)

        blocks = [x for parts in got for x in parts[:2]]
        smalls = [x for parts in got for x in parts[2:]]
        (qkv_pack, qkv_new, term_q), (up_pack, up_new, term_u) = adam_inner(
            qkv_planes, up_state, blocks, smalls, columns
        )
        terms = jnp.stack(
            [term_q[:, :, 0], term_q[:, :, 1], term_u[:, :, 0], term_u[:, :, 1]], axis=1
        )
        terms = terms + over_core(terms)
        terms = terms + over_x(terms)
        out_pack, out_new = adam_outer(out_state, blocks, W1C, "adam_out")
        down_pack, down_new = adam_outer(down_state, blocks, W1C + HW, "adam_down")
        qkv_pack = jnp.transpose(qkv_pack, (0, 1, 3, 2, 4))
        qkv_new = jnp.transpose(qkv_new, (0, 2, 1, 3))
        small = jnp.stack([jnp.stack(parts[2:]) for parts in got])
        small = jnp.where(odd, small[:, ::-1], small)
        bias_q = jnp.transpose(
            small[:, :, 0, : 3 * HW].reshape(layers, 2, 3, HW), (0, 2, 1, 3)
        ).reshape(layers, 3, 2 * HW)
        bias_u = small[:, :, 0, 3 * HW : W1C].reshape(layers, 2 * F8)
        nq, nu = qkv_bias_state.shape[3], up_bias_state.shape[2]
        bias_q = lax.dynamic_slice_in_dim(bias_q, place * nq, nq, axis=2)
        bias_u = lax.dynamic_slice_in_dim(bias_u, place * nu, nu, axis=1)
        dbo = lax.dynamic_slice_in_dim(small[:, 0, 1], place * DB, DB, axis=1)
        norm_total = jnp.concatenate([terms, dbo[:, None]], axis=1)
        qkv_bias_pack, qkv_bias_new = adam_step(qkv_bias_state, bias_q, rate_vector, 0.0)
        up_bias_pack, up_bias_new = adam_step(up_bias_state, bias_u, rate_vector, 0.0)
        norm_pack, norm_new = adam_step(norm_state, norm_total, rate_vector, 0.0)
        return (
            outputs,
            input_grad,
            qkv_pack,
            qkv_new,
            out_pack,
            out_new,
            up_pack,
            up_new,
            down_pack,
            down_new,
            qkv_bias_pack,
            qkv_bias_new,
            up_bias_pack,
            up_bias_new,
            norm_pack,
            norm_new,
        )

    return local


def solution(mesh):
    return jax.shard_map(
        build(mesh),
        mesh=mesh,
        in_specs=(
            P("dp", "ctx", None),
            P("dp", "ctx", None),
            P(None, None, ("dp", "ctx"), None, "tensor"),
            P(None, None, "tensor", ("dp", "ctx")),
            P(None, None, ("dp", "ctx"), "tensor"),
            P(None, None, "tensor", ("dp", "ctx")),
            P(None, None, None, ("tensor", "dp", "ctx")),
            P(None, None, ("tensor", "dp", "ctx")),
            P(None, None, None, ("dp", "ctx")),
        ),
        out_specs=(
            P("dp", "ctx", None),
            P("dp", "ctx", None),
            P(None, None, ("dp", "ctx"), None, "tensor"),
            P(None, ("dp", "ctx"), None, "tensor"),
            P(None, None, "tensor", ("dp", "ctx")),
            P(None, "tensor", ("dp", "ctx")),
            P(None, None, ("dp", "ctx"), "tensor"),
            P(None, ("dp", "ctx"), "tensor"),
            P(None, None, "tensor", ("dp", "ctx")),
            P(None, "tensor", ("dp", "ctx")),
            P(None, None, None, ("tensor", "dp", "ctx")),
            P(None, None, ("tensor", "dp", "ctx")),
            P(None, None, ("tensor", "dp", "ctx")),
            P(None, ("tensor", "dp", "ctx")),
            P(None, None, None, ("dp", "ctx")),
            P(None, None, ("dp", "ctx")),
        ),
        check_vma=False,
    )
```
